128 devices in a mesh: row: 16 (over x, y), col: 8 (over z, core).
Axes of the slice: x: 4, y: 4, z: 4, core: 2. Of those that a mesh axis runs over, the one named last changes fastest.
Arguments:
- counts: int32 [8192, 8192], P('row', 'col'), may hold values from 1 to 5
- sample_weights: float32 [8192, 8192], P('row', 'col'), may hold values from 0.045 to 54
- classes: int32 [8192, 8192], P('row', 'col'), may hold values from 0 to 3
- class_radius: int32 [4], replicated, may hold values from 8 to 64, as said below
Outputs:
- density_first: float32 [8192, 8192], P('row', 'col')
- density_second: float32 [8192, 8192], P('row', 'col')
The draws below stay inside these ranges and needn't reach their ends.
Inputs may be any that keep to these rules, and one draw needn't show every extreme that they name: `class_radius`: the radii rise strictly from class 0 to class 3, and class 3's radius is 64.
All inputs are finite; a program needn't handle non-finite values.
Results may differ from the reference program's by a relative error of at most 0.0001.
Values sent between devices are 32-bit elements; how exact they have to be, the bound alone decides.
No kernel may reach another device: no remote copies, remote signals or barrier semaphores. Data moves between devices by JAX's collectives and lax.ppermute only.
A program may use at most 128 MiB of HBM per device.

```python
import math
import jax
import jax.numpy as jnp
from jax import lax

CR = 512
CC = 1024
RMAX = 64
PR = 32
CLASSES = 4
NX = 8192
NY = 8192


def draw_counts(key, part):
    rows = jnp.arange(NX)[:, None]
    columns = jnp.arange(NY)[None, :]
    ceiling = jnp.broadcast_to(2 + 3 * rows // NX + 3 * columns // NY, (NX, NY))
    return jax.random.randint(jax.random.fold_in(key, 3), (NX, NY), 1, ceiling).astype(jnp.int32)


def draw_classes(key, part):
    first_key, second_key = jax.random.split(jax.random.fold_in(key, 7))
    block_rows = max(CR // 2, 1)
    block_columns = max(CC // 2, 1)
    blocks = jax.random.randint(first_key, (NX // block_rows, NY // block_columns), 0, 4)
    spread_grid = jnp.repeat(jnp.repeat(blocks, block_rows, axis=0), block_columns, axis=1)
    bumped = (jax.random.randint(second_key, (NX, NY), 0, 4) == 3).astype(jnp.int32)
    return jnp.minimum(spread_grid + bumped, 3).astype(jnp.int32)


def draw_class_radius(key, part):
    keys = jax.random.split(jax.random.fold_in(key, 11), 3)
    lowest = max(RMAX // 8, 1)
    middle = max(RMAX // 4, lowest)
    first_radius = jax.random.randint(keys[0], (1,), lowest, middle + 1)
    second_radius = jax.random.randint(keys[1], (1,), middle + 1, RMAX // 2 + 1)
    third_radius = jax.random.randint(keys[2], (1,), RMAX // 2 + 1, RMAX)
    widest = jnp.full((1,), RMAX, jnp.int32)
    return jnp.concatenate([first_radius, second_radius, third_radius, widest]).astype(jnp.int32)


def draw_sample_weights(key, part):
    keys = jax.random.split(jax.random.fold_in(key, 5), 3)
    row_scale = jnp.exp(jax.random.uniform(keys[0], (NX, 1), jnp.float32, math.log(0.3), math.log(3.0)))
    column_scale = jnp.exp(jax.random.uniform(keys[1], (1, NY), jnp.float32, math.log(0.3), math.log(3.0)))
    cell_scale = jnp.exp(jax.random.uniform(keys[2], (NX, NY), jnp.float32, math.log(0.5), math.log(2.0)))
    return (row_scale * column_scale * cell_scale).astype(jnp.float32)


def setup_inputs(seed: int = 0) -> dict:
    key_of = jax.random.split(jax.random.key(seed), 5)
    counts = draw_counts(jax.random.fold_in(key_of[4], 71), 0)
    sample_weights = draw_sample_weights(jax.random.fold_in(key_of[4], 71), 0)
    classes = draw_classes(jax.random.fold_in(key_of[4], 71), 0)
    class_radius = draw_class_radius(jax.random.fold_in(key_of[4], 71), 0)
    return dict(counts=counts, sample_weights=sample_weights, classes=classes, class_radius=class_radius)


BACKGROUND = 0.5
HIGHEST_PRECISION = lax.Precision.HIGHEST


def band_pair(radius, reach):
    spread = 0.5 * radius
    offsets = jnp.arange(-reach, reach + 1).astype(jnp.float32)
    inside = (jnp.abs(offsets) <= radius).astype(jnp.float32)
    norm_sum = jnp.sum(jnp.exp(-offsets * offsets / (2.0 * spread * spread)) * inside)
    source = jnp.arange(4 * reach)[:, None]
    target = jnp.arange(2 * reach)[None, :]
    shifts = (source - target - reach).astype(jnp.float32)
    weight = jnp.exp(-shifts * shifts / (2.0 * spread * spread)) * (jnp.abs(shifts) <= radius).astype(jnp.float32) / norm_sum
    return weight[: 2 * reach], weight[2 * reach:]


def along_columns(field, band_upper, band_lower):
    block_width = band_upper.shape[0]
    blocks = field.reshape(field.shape[0], field.shape[1] // block_width, block_width)
    result = jnp.einsum("mjk,ko->mjo", blocks[:, :-1], band_upper, precision=HIGHEST_PRECISION)
    result = result + jnp.einsum("mjk,ko->mjo", blocks[:, 1:], band_lower, precision=HIGHEST_PRECISION)
    return result.reshape(field.shape[0], -1)


def along_rows(field, band_upper, band_lower):
    block_width = band_upper.shape[0]
    blocks = field.reshape(field.shape[0] // block_width, block_width, field.shape[1])
    result = jnp.einsum("jkn,ko->jon", blocks[:-1], band_upper, precision=HIGHEST_PRECISION)
    result = result + jnp.einsum("jkn,ko->jon", blocks[1:], band_lower, precision=HIGHEST_PRECISION)
    return result.reshape(-1, field.shape[1])


def smooth(field, band_upper, band_lower, reach):
    padded = jnp.pad(field, ((0, 0), (reach, reach)))
    partial_field = along_columns(padded, band_upper, band_lower)
    padded = jnp.pad(partial_field, ((reach, reach), (0, 0)))
    return along_rows(padded, band_upper, band_lower)


def reference(counts, sample_weights, classes, class_radius):
    cell_mass = counts.astype(jnp.float32) * sample_weights
    pilot_upper, pilot_lower = band_pair(jnp.float32(PR), PR)
    pilot_field = smooth(cell_mass, pilot_upper, pilot_lower, PR) + BACKGROUND
    mass_sum = jnp.sum(cell_mass)
    radii = class_radius.astype(jnp.float32)
    results = []
    for iteration in range(2):
        mean_log = jnp.sum(cell_mass * jnp.log(pilot_field)) / mass_sum
        adapted = cell_mass * pilot_field / jnp.exp(mean_log)
        density = jnp.zeros_like(adapted)
        for class_index in range(CLASSES):
            band_upper, band_lower = band_pair(radii[class_index], RMAX)
            masked = jnp.where(classes == class_index, adapted, jnp.float32(0.0))
            density = density + smooth(masked, band_upper, band_lower, RMAX)
        results.append(density)
        pilot_field = density + BACKGROUND
    return results[0], results[1]
```

```python
import functools

import jax
import jax.numpy as jnp
from jax import lax
from jax.experimental import pallas as pl
from jax.experimental.pallas import tpu as pltpu
from jax.sharding import PartitionSpec as P

REACH = 64
PILOT_RADIUS = 32
CLASSES = 4
BACKGROUND = 0.5
TILE = 256
BAND = TILE + 2 * REACH
F32 = jnp.float32
BF16 = jnp.bfloat16
MIB = 1 << 20


def call(kernel, outs, args, smem=(), limit=24):
    vmem = pl.BlockSpec(memory_space=pltpu.VMEM)
    scalar = pl.BlockSpec(memory_space=pltpu.SMEM)
    return pl.pallas_call(
        kernel,
        out_shape=[jax.ShapeDtypeStruct(s, d) for s, d in outs],
        in_specs=[scalar if i in smem else vmem for i in range(len(args))],
        out_specs=[vmem] * len(outs),
        compiler_params=pltpu.CompilerParams(vmem_limit_bytes=limit * MIB),
    )(*args)


def split(value):
    high = value.astype(BF16)
    return high, (value - high.astype(F32)).astype(BF16)


def dot(a, b):
    return jnp.dot(a, b, preferred_element_type=F32)


def bands_kernel(radius_ref, high_ref, low_ref, stack_ref, rim_ref):
    def iota(shape, dim):
        return lax.broadcasted_iota(jnp.int32, shape, dim)

    lane = iota((8, 128), 1).astype(F32)
    tap = jnp.where(iota((8, 128), 0) == 0, jnp.where(lane == 0, 1.0, 2.0), 0.0)
    shift = (iota((BAND, TILE), 0) - REACH - iota((BAND, TILE), 1)).astype(F32)
    row, column = iota((128, 128), 0), iota((128, 128), 1)
    upper = row < 64
    same = upper == (column < 64)
    rim_shift = (row - column + jnp.where(upper, REACH, -REACH)).astype(F32)
    for c in range(CLASSES + 1):
        radius = F32(PILOT_RADIUS) if c == CLASSES else radius_ref[c].astype(F32)
        radius = jnp.full((1, 1), radius, F32)
        inverse = 1.0 / (2.0 * (0.5 * radius) * (0.5 * radius))

        def shape_of(d):
            return jnp.where(jnp.abs(d) <= radius, jnp.exp(-(d * d) * inverse), 0.0)

        total = jnp.sum(shape_of(lane) * tap, axis=(0, 1), keepdims=True)
        high, low = split(shape_of(shift) / total)
        high_ref[c * BAND : (c + 1) * BAND, :] = high
        low_ref[c * BAND : (c + 1) * BAND, :] = low
        stack_ref[c, :, 0:TILE] = high
        stack_ref[c, :, TILE : 2 * TILE] = low
        stack_ref[c, :, 2 * TILE :] = high
        high, low = split(jnp.where(same, shape_of(rim_shift) / total, 0.0))
        rim_ref[c, :, 0:128] = high
        rim_ref[c, :, 128:256] = high
        rim_ref[c, :, 256:384] = low


def masked(pieces, labels, c):
    if labels is None:
        return pieces
    keep = labels == c
    return [jnp.where(keep, piece, jnp.zeros_like(piece)) for piece in pieces]


def rows_kernel(*refs, bands, labelled):
    field_ref, refs = refs[0], refs[1:]
    label_ref, refs = (refs[0], refs[1:]) if labelled else (None, refs)
    stack_ref, high_ref, low_ref, edge_ref = refs
    rows, columns = field_ref.shape
    for n in range(columns // TILE):
        at = slice(n * TILE, (n + 1) * TILE)
        pieces = split(field_ref[:, at])
        labels = label_ref[:, at] if labelled else None
        for slot, c in enumerate(bands):
            high, low = masked(pieces, labels, c)

            def part(t, start):
                own = slice(t * TILE, (t + 1) * TILE)
                right = jnp.concatenate([high[own], high[own], low[own]], axis=0)
                return dot(stack_ref[c, start : start + TILE + REACH, :], right)

            first, second = part(0, REACH), part(1, 0)
            edge_ref[slot, 0:REACH, at] = first[0:REACH]
            edge_ref[slot, REACH:, at] = second[TILE:]
            cut = TILE - REACH
            for target, value in (
                (0, first[REACH:cut]),
                (cut - REACH, first[cut:] + second[: 2 * REACH]),
                (cut + REACH, second[2 * REACH : TILE]),
            ):
                value_high, value_low = split(value)
                high_ref[slot, target : target + value.shape[0], at] = value_high
                low_ref[slot, target : target + value.shape[0], at] = value_low


def swept(parts, bands, high_ref, low_ref, inputs, taps, outputs):
    stacked = [
        jnp.concatenate([ref[c * BAND + taps.start : c * BAND + taps.stop, outputs] for c in bands])
        for ref in (high_ref, low_ref)
    ]
    results = []
    for high_part, low_part in parts:
        high, low = (
            jnp.concatenate([ref[slot, :, inputs] for slot in range(len(bands))], axis=1)
            for ref in (high_part, low_part)
        )
        results.append(dot(high, stacked[0]) + dot(high, stacked[1]) + dot(low, stacked[0]))
    return results


def place(target_ref, at, inner, edge):
    rows = target_ref.shape[0]
    target_ref[0:REACH, at] = edge[0:REACH]
    target_ref[REACH : rows - REACH, at] = inner
    target_ref[rows - REACH :, at] = edge[REACH:]


def edges_kernel(*refs, bands, labelled):
    partial_ref, top_ref, bottom_ref, refs = refs[0], refs[1], refs[2], refs[3:]
    if labelled:
        top_label_ref, bottom_label_ref, refs = refs[0], refs[1], refs[2:]
    inner_high, inner_low, rim_ref, band_high, band_low, refs = *refs[:5], refs[5:]
    edge_high, edge_low, left_ref, right_ref, send_left, send_right = refs
    columns = top_ref.shape[1]
    for n in range(columns // TILE):
        at = slice(n * TILE, (n + 1) * TILE)
        pieces = split(jnp.concatenate([top_ref[:, at], bottom_ref[:, at]]))
        labels = None
        if labelled:
            labels = jnp.concatenate([top_label_ref[:, at], bottom_label_ref[:, at]])
            labels = labels.astype(F32).astype(BF16)
        for slot, c in enumerate(bands):
            high, low = masked(pieces, labels, c)
            right = jnp.concatenate([high, low, high], axis=0)
            value = partial_ref[slot, :, at] + dot(rim_ref[c], right)
            edge_high[slot, :, at], edge_low[slot, :, at] = split(value)
    parts = ((inner_high, inner_low), (edge_high, edge_low))
    sides = (
        (left_ref, slice(0, TILE), slice(128, BAND), slice(0, TILE)),
        (right_ref, slice(columns - 128, columns), slice(0, 128), slice(0, 128)),
    )
    for target, inputs, taps, outputs in sides:
        inner, edge = swept(parts, bands, band_high, band_low, inputs, taps, outputs)
        place(target, slice(None), inner, edge)
    half = left_ref.shape[0] // 2
    lower = lax.broadcasted_iota(jnp.int32, (half, 128), 1) < REACH
    left = left_ref[:, 0:128]
    send_left[...] = jnp.where(lower, left[:half], pltpu.roll(left[half:], REACH, 1))
    right = right_ref[...]
    send_right[...] = jnp.where(lower, pltpu.roll(right[:half], REACH, 1), right[half:])


def middle_kernel(inner_high, inner_low, edge_high, edge_low, band_high, band_low, out_ref, *, bands):
    parts = ((inner_high, inner_low), (edge_high, edge_low))
    for j in range(out_ref.shape[1] // TILE):
        inputs = slice(j * TILE + 128, j * TILE + 128 + BAND)
        inner, edge = swept(
            parts, bands, band_high, band_low, inputs, slice(0, BAND), slice(0, TILE)
        )
        place(out_ref, slice(j * TILE, (j + 1) * TILE), inner, edge)


def gathered(left_ref, middle_ref, right_ref, from_left, from_right, at):
    half = left_ref.shape[0] // 2
    lane = lax.broadcasted_iota(jnp.int32, (at.stop - at.start, 128), 1)
    local = slice(at.start % half, at.start % half + at.stop - at.start)
    come_left, come_right = from_left[local], from_right[local]
    if at.start < half:
        come_left = pltpu.roll(come_left, REACH, 1)
    else:
        come_right = pltpu.roll(come_right, REACH, 1)
    first = left_ref[at, 0:128] + jnp.where(lane >= REACH, come_left, 0.0)
    last = right_ref[at, :] + jnp.where(lane < REACH, come_right, 0.0)
    blocks = [first, left_ref[at, 128:256]]
    blocks += [middle_ref[at, k : k + 128] for k in range(0, middle_ref.shape[1], 128)]
    blocks += [last]
    turned = [pltpu.roll(block, REACH, 1) for block in blocks]
    return [jnp.where(lane < REACH, a, b) for a, b in zip(turned[:-1], turned[1:])]


def finish_kernel(*refs, scaled, density, following, totals):
    left_ref, middle_ref, right_ref, from_left, from_right, refs = *refs[:5], refs[5:]
    if scaled:
        log_ref, mass_total_ref, refs = refs[0], refs[1], refs[2:]
        inverse = jnp.exp(-(log_ref[0:1, :] / mass_total_ref[1:2, :]))
    if following:
        mass_ref, refs = refs[0], refs[1:]
    if density:
        density_ref, refs = refs[0], refs[1:]
    if following:
        adapted_ref, top_ref, bottom_ref, stat_ref = refs
    rows = left_ref.shape[0]
    step = 64
    log_sum = jnp.zeros((8, 128), F32)
    mass_sum = jnp.zeros((8, 128), F32)
    for start in range(0, rows, step):
        at = slice(start, start + step)
        blocks = gathered(left_ref, middle_ref, right_ref, from_left, from_right, at)
        for k, block in enumerate(blocks):
            lanes = slice(k * 128, (k + 1) * 128)
            if scaled:
                block = block * inverse
            if density:
                density_ref[at, lanes] = block
            if following:
                pilot = block + BACKGROUND
                mass = mass_ref[at, lanes]
                value = mass * pilot
                adapted_ref[at, lanes] = value
                if start == 0:
                    top_ref[:, lanes] = value
                if start == rows - step:
                    bottom_ref[:, lanes] = value
                terms = mass * jnp.log(pilot)
                log_sum += jnp.sum(terms.reshape(step // 8, 8, 128), axis=0)
                if totals:
                    mass_sum += jnp.sum(mass.reshape(step // 8, 8, 128), axis=0)
    if following:
        log_sum = jnp.sum(log_sum, axis=(0, 1), keepdims=True)
        mass_sum = jnp.sum(mass_sum, axis=(0, 1), keepdims=True)
        row = lax.broadcasted_iota(jnp.int32, (8, 128), 0)
        stat_ref[...] = jnp.where(row == 0, log_sum, jnp.where(row == 1, mass_sum, 0.0))


def shift_pair(up, down, axis):
    count = lax.axis_size(axis)
    forward = [(i, i + 1) for i in range(count - 1)]
    backward = [(i + 1, i) for i in range(count - 1)]
    return lax.ppermute(down, axis, forward), lax.ppermute(up, axis, backward)


def total_over(stat):
    for axis in ("row", "col"):
        distance = 1
        while distance < lax.axis_size(axis):
            pairs = [(i, i ^ distance) for i in range(lax.axis_size(axis))]
            stat = stat + lax.ppermute(stat, axis, pairs)
            distance *= 2
    return stat


def smooth(field, halo, labels, label_halo, tables, bands):
    high, low, stack, rim = tables
    rows, columns = field.shape
    count = len(bands)
    labelled = labels is not None
    inner = (count, rows - 2 * REACH, columns)
    edge = (count, 2 * REACH, columns)
    args = [field] + ([labels] if labelled else []) + [stack]
    inner_high, inner_low, partial = call(
        functools.partial(rows_kernel, bands=bands, labelled=labelled),
        [(inner, BF16), (inner, BF16), (edge, F32)],
        args,
    )
    args = [partial, *halo, *(label_halo if labelled else ()), inner_high, inner_low]
    args += [rim, high, low]
    edge_high, edge_low, left, right, send_left, send_right = call(
        functools.partial(edges_kernel, bands=bands, labelled=labelled),
        [(edge, BF16), (edge, BF16), ((rows, TILE), F32), ((rows, 128), F32)]
        + [((rows // 2, 128), F32)] * 2,
        args,
    )
    from_left, from_right = shift_pair(send_left, send_right, "col")
    (middle,) = call(
        functools.partial(middle_kernel, bands=bands),
        [((rows, columns - TILE), F32)],
        [inner_high, inner_low, edge_high, edge_low, high, low],
    )
    return left, middle, right, from_left, from_right


def body(counts, sample_weights, classes, class_radius):
    rows, columns = counts.shape
    top = counts[:REACH].astype(F32) * sample_weights[:REACH]
    bottom = counts[rows - REACH :].astype(F32) * sample_weights[rows - REACH :]
    mass_halo = shift_pair(top, bottom, "row")
    label_halo = shift_pair(classes[:REACH], classes[rows - REACH :], "row")
    mass = counts.astype(F32) * sample_weights
    labels = classes.astype(F32).astype(BF16)
    wide = (CLASSES + 1) * BAND
    tables = call(
        bands_kernel,
        [
            ((wide, TILE), BF16),
            ((wide, TILE), BF16),
            ((CLASSES + 1, BAND, 3 * TILE), BF16),
            ((CLASSES + 1, 128, 384), BF16),
        ],
        [class_radius],
        smem=(0,),
    )
    plane = ((rows, columns), F32)
    rim = ((REACH, columns), F32)
    stat = ((8, 128), F32)
    every = tuple(range(CLASSES))

    pieces = smooth(mass, mass_halo, None, None, tables, (CLASSES,))
    adapted, top, bottom, first_stat = call(
        functools.partial(finish_kernel, scaled=False, density=False, following=True, totals=True),
        [plane, rim, rim, stat],
        [*pieces, mass],
    )
    halo = shift_pair(top, bottom, "row")
    first_total = total_over(first_stat)
    pieces = smooth(adapted, halo, labels, label_halo, tables, every)
    density_first, adapted, top, bottom, second_stat = call(
        functools.partial(finish_kernel, scaled=True, density=True, following=True, totals=False),
        [plane, plane, rim, rim, stat],
        [*pieces, first_total, first_total, mass],
    )
    halo = shift_pair(top, bottom, "row")
    second_total = total_over(second_stat)
    pieces = smooth(adapted, halo, labels, label_halo, tables, every)
    (density_second,) = call(
        functools.partial(finish_kernel, scaled=True, density=True, following=False, totals=False),
        [plane],
        [*pieces, second_total, first_total],
    )
    return density_first, density_second


def solution(mesh):
    spec = P("row", "col")
    return jax.shard_map(
        body,
        mesh=mesh,
        in_specs=(spec, spec, spec, P()),
        out_specs=(spec, spec),
        check_vma=False,
    )
```

```python
import functools

import jax
import jax.numpy as jnp
from jax import lax
from jax.experimental import pallas as pl
from jax.experimental.pallas import tpu as pltpu
from jax.sharding import PartitionSpec as P


REACH = 64
PILOT_RADIUS = 32
CLASSES = 4
BACKGROUND = 0.5
TILE = 256
BAND = TILE + 2 * REACH
F32 = jnp.float32
BF16 = jnp.bfloat16
MIB = 1 << 20


def call(kernel, outs, args, smem=(), limit=24, flops=100_000_000):
    vmem = pl.BlockSpec(memory_space=pltpu.VMEM)
    scalar = pl.BlockSpec(memory_space=pltpu.SMEM)
    return pl.pallas_call(
        kernel,
        out_shape=[jax.ShapeDtypeStruct(s, d) for s, d in outs],
        in_specs=[scalar if i in smem else vmem for i in range(len(args))],
        out_specs=[vmem] * len(outs),
        compiler_params=pltpu.CompilerParams(vmem_limit_bytes=limit * MIB),
        cost_estimate=pl.CostEstimate(flops=flops, transcendentals=0, bytes_accessed=4 * MIB),
    )(*args)


def split(value):
    high = value.astype(BF16)
    return high, (value - high.astype(F32)).astype(BF16)


def dot(a, b):
    return jnp.dot(a, b, preferred_element_type=F32)


def bands_kernel(radius_ref, high_ref, low_ref, stack_ref, rim_ref):
    def iota(shape, dim):
        return lax.broadcasted_iota(jnp.int32, shape, dim)

    lane = iota((8, 128), 1).astype(F32)
    tap = jnp.where(iota((8, 128), 0) == 0, jnp.where(lane == 0, 1.0, 2.0), 0.0)
    shift = (iota((BAND, TILE), 0) - REACH - iota((BAND, TILE), 1)).astype(F32)
    row, column = iota((128, 128), 0), iota((128, 128), 1)
    upper = row < 64
    same = upper == (column < 64)
    rim_shift = (row - column + jnp.where(upper, REACH, -REACH)).astype(F32)
    for c in range(CLASSES + 1):
        radius = F32(PILOT_RADIUS) if c == CLASSES else radius_ref[c].astype(F32)
        radius = jnp.full((1, 1), radius, F32)
        inverse = 1.0 / (2.0 * (0.5 * radius) * (0.5 * radius))

        def shape_of(d):
            return jnp.where(jnp.abs(d) <= radius, jnp.exp(-(d * d) * inverse), 0.0)

        total = jnp.sum(shape_of(lane) * tap, axis=(0, 1), keepdims=True)
        high, low = split(shape_of(shift) / total)
        high_ref[c * BAND : (c + 1) * BAND, :] = high
        low_ref[c * BAND : (c + 1) * BAND, :] = low
        stack_ref[c, :, 0:TILE] = high
        stack_ref[c, :, TILE : 2 * TILE] = low
        stack_ref[c, :, 2 * TILE :] = high
        high, low = split(jnp.where(same, shape_of(rim_shift) / total, 0.0))
        rim_ref[c, :, 0:128] = high
        rim_ref[c, :, 128:256] = high
        rim_ref[c, :, 256:384] = low


def masked(pieces, labels, c):
    if labels is None:
        return pieces
    keep = labels == c
    return [jnp.where(keep, piece, jnp.zeros_like(piece)) for piece in pieces]


def rows_kernel(*refs, bands, labelled):
    field_ref, refs = refs[0], refs[1:]
    label_ref, refs = (refs[0], refs[1:]) if labelled else (None, refs)
    stack_ref, high_ref, low_ref, edge_ref = refs
    _, columns = field_ref.shape
    for n in range(columns // TILE):
        at = slice(n * TILE, (n + 1) * TILE)
        pieces = split(field_ref[:, at])
        labels = label_ref[:, at] if labelled else None
        for slot, c in enumerate(bands):
            high, low = masked(pieces, labels, c)

            def part(t, start):
                own = slice(t * TILE, (t + 1) * TILE)
                right = jnp.concatenate([high[own], high[own], low[own]], axis=0)
                return dot(stack_ref[c, start : start + TILE + REACH, :], right)

            first, second = part(0, REACH), part(1, 0)
            edge_ref[slot, 0:REACH, at] = first[0:REACH]
            edge_ref[slot, REACH:, at] = second[TILE:]
            cut = TILE - REACH
            for target, value in (
                (0, first[REACH:cut]),
                (cut - REACH, first[cut:] + second[: 2 * REACH]),
                (cut + REACH, second[2 * REACH : TILE]),
            ):
                value_high, value_low = split(value)
                high_ref[slot, target : target + value.shape[0], at] = value_high
                low_ref[slot, target : target + value.shape[0], at] = value_low


def swept(parts, bands, high_ref, low_ref, inputs, taps, outputs):
    stacked = [
        jnp.concatenate([ref[c * BAND + taps.start : c * BAND + taps.stop, outputs] for c in bands])
        for ref in (high_ref, low_ref)
    ]
    results = []
    for part in parts:
        high, low = (
            jnp.concatenate([ref[slot, :, inputs] for ref, slot in side], axis=1) for side in part
        )
        results.append(dot(high, stacked[0]) + dot(high, stacked[1]) + dot(low, stacked[0]))
    return results


def place(target_ref, at, inner, edge):
    rows = target_ref.shape[0]
    target_ref[0:REACH, at] = edge[0:REACH]
    target_ref[REACH : rows - REACH, at] = inner
    target_ref[rows - REACH :, at] = edge[REACH:]


def take(refs, *counts):
    groups = []
    for count in counts:
        groups.append(list(refs[:count]))
        refs = refs[count:]
    return *groups, list(refs)


def slots_of(refs, groups):
    return [(ref, slot) for ref, group in zip(refs, groups) for slot in range(len(group))]


def chosen(odd_ref, when_odd, when_even):
    return jnp.where(odd_ref[0:1, 0:1] > 0.5, when_odd, when_even)


def edges_kernel(*refs, groups, labelled):
    count = len(groups)
    refs, (odd_row, odd_column), halo, labels_in, partials, highs, lows, tables, outs = (
        None,
        *take(refs, 2, 2, 2 * labelled, count, count, count, 3),
    )
    rim_ref, band_high, band_low = tables
    edge_high, edge_low, left_ref, right_ref, send_a, send_b = outs
    bands = [c for group in groups for c in group]
    partial_slots = slots_of(partials, groups)
    columns = halo[0].shape[1]
    for n in range(columns // TILE):
        at = slice(n * TILE, (n + 1) * TILE)

        def joined(pair):
            first, second = pair[0][:, at].astype(F32), pair[1][:, at].astype(F32)
            top = chosen(odd_row, first, second)
            bottom = chosen(odd_row, second, first)
            missing = REACH - first.shape[0]
            if missing:
                zeros = jnp.zeros((missing, TILE), F32)
                return jnp.concatenate([zeros, top, bottom, zeros])
            return jnp.concatenate([top, bottom])

        pieces = split(joined(halo))
        labels = joined(labels_in).astype(BF16) if labelled else None
        for slot, c in enumerate(bands):
            high, low = masked(pieces, labels, c)
            right = jnp.concatenate([high, low, high], axis=0)
            source, at_slot = partial_slots[slot]
            value = source[at_slot, :, at] + dot(rim_ref[c], right)
            edge_high[slot, :, at], edge_low[slot, :, at] = split(value)
    parts = parts_of(highs, lows, edge_high, edge_low, groups)
    sides = (
        (left_ref, slice(0, TILE), slice(128, BAND), slice(0, TILE)),
        (right_ref, slice(columns - 128, columns), slice(0, 128), slice(0, 128)),
    )
    for target, inputs, taps, outputs in sides:
        inner, edge = swept(parts, bands, band_high, band_low, inputs, taps, outputs)
        place(target, slice(None), inner, edge)
    half = left_ref.shape[0] // 2
    lower = lax.broadcasted_iota(jnp.int32, (half, 128), 1) < REACH
    left = left_ref[:, 0:128]
    left = jnp.where(lower, left[:half], pltpu.roll(left[half:], REACH, 1))
    right = right_ref[...]
    right = jnp.where(lower, pltpu.roll(right[:half], REACH, 1), right[half:])
    send_a[...] = chosen(odd_column, left, right)
    send_b[...] = chosen(odd_column, right, left)


def parts_of(highs, lows, edge_high, edge_low, groups):
    whole = [[c for group in groups for c in group]]
    return (
        (slots_of(highs, groups), slots_of(lows, groups)),
        (slots_of([edge_high], whole), slots_of([edge_low], whole)),
    )


def middle_kernel(*refs, groups, blocks):
    count = len(groups)
    highs, lows, (edge_high, edge_low, band_high, band_low), (out_ref,) = take(refs, count, count, 4)
    bands = [c for group in groups for c in group]
    parts = parts_of(highs, lows, edge_high, edge_low, groups)
    for slot, j in enumerate(blocks):
        inputs = slice(j * TILE + 128, j * TILE + 128 + BAND)
        inner, edge = swept(
            parts, bands, band_high, band_low, inputs, slice(0, BAND), slice(0, TILE)
        )
        place(out_ref, slice(slot * TILE, (slot + 1) * TILE), inner, edge)


def gathered(pieces, come, odd, at):
    left_ref, middles, right_ref = pieces
    half = left_ref.shape[0] // 2
    lane = lax.broadcasted_iota(jnp.int32, (at.stop - at.start, 128), 1)
    local = slice(at.start % half, at.start % half + at.stop - at.start)
    come_left = chosen(odd, come[0][local], come[1][local])
    come_right = chosen(odd, come[1][local], come[0][local])
    if at.start < half:
        come_left = pltpu.roll(come_left, REACH, 1)
    else:
        come_right = pltpu.roll(come_right, REACH, 1)
    first = left_ref[at, 0:128] + jnp.where(lane >= REACH, come_left, 0.0)
    last = right_ref[at, :] + jnp.where(lane < REACH, come_right, 0.0)
    blocks = [first, left_ref[at, 128:256]]
    for middle_ref in middles:
        blocks += [middle_ref[at, k : k + 128] for k in range(0, middle_ref.shape[1], 128)]
    blocks += [last]
    turned = [pltpu.roll(block, REACH, 1) for block in blocks]
    return [jnp.where(lane < REACH, a, b) for a, b in zip(turned[:-1], turned[1:])]


def finish_kernel(*refs, middles, scaled, density, following, totals):
    (odd_row, odd_column), (left_ref,), middle_refs, (right_ref,), come, refs = take(
        refs, 2, 1, middles, 1, 2
    )
    pieces = (left_ref, middle_refs, right_ref)
    if scaled:
        (log_ref, mass_total_ref), refs = take(refs, 2)
        inverse = jnp.exp(-(log_ref[0:1, :] / mass_total_ref[1:2, :]))
    if following:
        (mass_ref,), refs = take(refs, 1)
    if density:
        (density_ref,), refs = take(refs, 1)
    if following:
        adapted_ref, send_a, send_b, stat_ref = refs
    rows = left_ref.shape[0]
    step = 64
    log_sum = jnp.zeros((8, 128), F32)
    mass_sum = jnp.zeros((8, 128), F32)
    for start in range(0, rows, step):
        at = slice(start, start + step)
        for k, block in enumerate(gathered(pieces, come, odd_column, at)):
            lanes = slice(k * 128, (k + 1) * 128)
            if scaled:
                block = block * inverse
            if density:
                density_ref[at, lanes] = block
            if following:
                pilot = block + BACKGROUND
                mass = mass_ref[at, lanes]
                adapted_ref[at, lanes] = mass * pilot
                terms = mass * jnp.log(pilot)
                log_sum += jnp.sum(terms.reshape(step // 8, 8, 128), axis=0)
                if totals:
                    mass_sum += jnp.sum(mass.reshape(step // 8, 8, 128), axis=0)
    if following:
        top, bottom = adapted_ref[0:REACH], adapted_ref[rows - REACH :]
        send_a[...] = chosen(odd_row, top, bottom)
        send_b[...] = chosen(odd_row, bottom, top)
        log_sum = jnp.sum(log_sum, axis=(0, 1), keepdims=True)
        mass_sum = jnp.sum(mass_sum, axis=(0, 1), keepdims=True)
        row = lax.broadcasted_iota(jnp.int32, (8, 128), 0)
        stat_ref[...] = jnp.where(row == 0, log_sum, jnp.where(row == 1, mass_sum, 0.0))


def exchange(first, second, axis):
    results = []
    for offset, value in ((0, first), (1, second)):
        pairs = []
        for i in range(offset, lax.axis_size(axis) - 1, 2):
            pairs += [(i, i + 1), (i + 1, i)]
        results.append(lax.ppermute(value, axis, pairs))
    return results


HOPS = {1: (), 2: (1,), 4: (1, 3), 8: (1, 2, 6), 16: (4, 12, 1, 3)}


def total_over(stat):
    for axis in ("col", "row"):
        for hop in HOPS[lax.axis_size(axis)]:
            pairs = [(i, i ^ hop) for i in range(lax.axis_size(axis))]
            stat = stat + lax.ppermute(stat, axis, pairs)
    return stat


def smooth(field, halo, labels, label_halo, tables, odd, groups, blocks):
    high, low, stack, rim = tables
    rows, columns = field.shape
    labelled = labels is not None
    bands = [c for group in groups for c in group]
    highs, lows, partials = [], [], []
    for group in groups:
        inner = (len(group), rows - 2 * REACH, columns)
        edge = (len(group), 2 * REACH, columns)
        results = call(
            functools.partial(rows_kernel, bands=group, labelled=labelled),
            [(inner, BF16), (inner, BF16), (edge, F32)],
            [field] + ([labels] if labelled else []) + [stack],
            flops=len(group) * 1_000_000_000,
        )
        for results_of, result in zip((highs, lows, partials), results):
            results_of.append(result)
    edge = (len(bands), 2 * REACH, columns)
    edge_high, edge_low, left, right, send_a, send_b = call(
        functools.partial(edges_kernel, groups=groups, labelled=labelled),
        [(edge, BF16), (edge, BF16), ((rows, TILE), F32), ((rows, 128), F32)]
        + [((rows // 2, 128), F32)] * 2,
        [*odd, *halo, *(label_halo if labelled else ()), *partials, *highs, *lows]
        + [rim, high, low],
        flops=len(bands) * 500_000_000,
    )
    come = exchange(send_a, send_b, "col")
    middles = []
    for part in blocks:
        middles += call(
            functools.partial(middle_kernel, groups=groups, blocks=part),
            [((rows, len(part) * TILE), F32)],
            [*highs, *lows, edge_high, edge_low, high, low],
            flops=len(bands) * len(part) * 250_000_000,
        )
    return [*odd, left, *middles, right, *come]


def finish(pieces, extra, outs, **flags):
    return call(
        functools.partial(finish_kernel, middles=len(pieces) - 6, **flags),
        outs,
        [*pieces, *extra],
        flops=500_000_000,
    )


def body(counts, sample_weights, classes, class_radius):
    rows, columns = counts.shape
    is_odd = [(lax.axis_index(axis) & 1).astype(F32) for axis in ("row", "col")]
    odd = [jnp.full((8, 128), value, F32) for value in is_odd]
    plane = ((rows, columns), F32)
    rim = ((REACH, columns), F32)
    stat = ((8, 128), F32)
    groups = ((0,), (1, 2), (3,))
    blocks = tuple((j,) for j in range(columns // TILE - 1))

    def ends(array, width):
        top, bottom = array[:width], array[rows - width :]
        return [jnp.where(is_odd[0] > 0.5, *pair) for pair in ((top, bottom), (bottom, top))]

    sends = [
        number.astype(F32) * weight
        for number, weight in zip(ends(counts, PILOT_RADIUS), ends(sample_weights, PILOT_RADIUS))
    ]
    mass_halo = exchange(*sends, "row")
    label_halo = exchange(*ends(classes, REACH), "row")
    mass = counts.astype(F32) * sample_weights
    labels = classes.astype(F32).astype(BF16)
    wide = (CLASSES + 1) * BAND
    tables = call(
        bands_kernel,
        [
            ((wide, TILE), BF16),
            ((wide, TILE), BF16),
            ((CLASSES + 1, BAND, 3 * TILE), BF16),
            ((CLASSES + 1, 128, 384), BF16),
        ],
        [class_radius],
        smem=(0,),
        flops=500_000_000,
    )
    pieces = smooth(
        mass, mass_halo, None, None, tables, odd, ((CLASSES,),), (sum(blocks, ()),)
    )
    adapted, *sends, first_stat = finish(
        pieces,
        [mass],
        [plane, rim, rim, stat],
        scaled=False,
        density=False,
        following=True,
        totals=True,
    )
    halo = exchange(*sends, "row")
    first_total = total_over(first_stat)
    pieces = smooth(adapted, halo, labels, label_halo, tables, odd, groups, blocks)
    density_first, adapted, *sends, second_stat = finish(
        pieces,
        [first_total, first_total, mass],
        [plane, plane, rim, rim, stat],
        scaled=True,
        density=True,
        following=True,
        totals=False,
    )
    halo = exchange(*sends, "row")
    second_total = total_over(second_stat)
    pieces = smooth(adapted, halo, labels, label_halo, tables, odd, groups, blocks)
    (density_second,) = finish(
        pieces,
        [second_total, first_total],
        [plane],
        scaled=True,
        density=True,
        following=False,
        totals=False,
    )
    return density_first, density_second


def solution(mesh):
    spec = P("row", "col")
    return jax.shard_map(
        body,
        mesh=mesh,
        in_specs=(spec, spec, spec, P()),
        out_specs=(spec, spec),
        check_vma=False,
    )
```

```python
import functools

import jax
import jax.numpy as jnp
from jax import lax
from jax.experimental import pallas as pl
from jax.experimental.pallas import tpu as pltpu
from jax.sharding import PartitionSpec as P


REACH = 64
PILOT_RADIUS = 32
CLASSES = 4
BACKGROUND = 0.5
TILE = 256
BAND = TILE + 2 * REACH
STEP = 64
F32 = jnp.float32
BF16 = jnp.bfloat16
MIB = 1 << 20
HBM = pl.BlockSpec(memory_space=pltpu.HBM)
VMEM = pl.BlockSpec(memory_space=pltpu.VMEM)
SMEM = pl.BlockSpec(memory_space=pltpu.SMEM)


def call(kernel, outs, args, ins=None, out_specs=None, scratch=(), limit=24, flops=100_000_000):
    return pl.pallas_call(
        kernel,
        out_shape=[jax.ShapeDtypeStruct(s, d) for s, d in outs],
        in_specs=ins or [VMEM] * len(args),
        out_specs=out_specs or [VMEM] * len(outs),
        scratch_shapes=scratch,
        compiler_params=pltpu.CompilerParams(vmem_limit_bytes=limit * MIB),
        cost_estimate=pl.CostEstimate(flops=flops, transcendentals=0, bytes_accessed=4 * MIB),
    )(*args)


def iota(shape, dim):
    return lax.broadcasted_iota(jnp.int32, shape, dim)


def split(value):
    high = value.astype(BF16)
    return high, (value - high.astype(F32)).astype(BF16)


def dot(a, b):
    return jnp.dot(a, b, preferred_element_type=F32)


def take(refs, *counts):
    groups = []
    for count in counts:
        groups.append(list(refs[:count]))
        refs = refs[count:]
    return *groups, list(refs)


def chosen(flag, when_set, when_clear):
    return jnp.where(flag > 0.5, when_set, when_clear)


def flags_of(axis):
    index = lax.axis_index(axis)
    last = lax.axis_size(axis) - 1
    values = (index & 1, jnp.minimum(index, 1), jnp.minimum(last - index, 1))
    return [jnp.full((1, 1), value.astype(F32), F32) for value in values]


def fill_bands(radius_ref, high_ref, low_ref, stack_ref, rim_ref):
    lane = iota((8, 128), 1).astype(F32)
    tap = jnp.where(iota((8, 128), 0) == 0, jnp.where(lane == 0, 1.0, 2.0), 0.0)
    shift = (iota((BAND, TILE), 0) - REACH - iota((BAND, TILE), 1)).astype(F32)
    row, column = iota((128, 128), 0), iota((128, 128), 1)
    upper = row < 64
    same = upper == (column < 64)
    rim_shift = (row - column + jnp.where(upper, REACH, -REACH)).astype(F32)
    for c in range(CLASSES + 1):
        radius = F32(PILOT_RADIUS) if c == CLASSES else radius_ref[c].astype(F32)
        radius = jnp.full((1, 1), radius, F32)
        inverse = 1.0 / (2.0 * (0.5 * radius) * (0.5 * radius))

        def shape_of(d):
            return jnp.where(jnp.abs(d) <= radius, jnp.exp(-(d * d) * inverse), 0.0)

        total = jnp.sum(shape_of(lane) * tap, axis=(0, 1), keepdims=True)
        high, low = split(shape_of(shift) / total)
        high_ref[c * BAND : (c + 1) * BAND, :] = high
        low_ref[c * BAND : (c + 1) * BAND, :] = low
        stack_ref[c, :, 0:TILE] = high
        stack_ref[c, :, TILE : 2 * TILE] = low
        stack_ref[c, :, 2 * TILE :] = high
        high, low = split(jnp.where(same, shape_of(rim_shift) / total, 0.0))
        rim_ref[c, :, 0:128] = high
        rim_ref[c, :, 128:256] = high
        rim_ref[c, :, 256:384] = low


def prepare_kernel(*refs):
    (radius_ref, *fields), tables, outs, scratch = take(refs, 4, 4, 4)
    mass_ref, label_ref, send_a, send_b = outs
    *local, arrived = scratch
    copies = [
        pltpu.make_async_copy(field, kept, arrived.at[n])
        for n, (field, kept) in enumerate(zip(fields, local))
    ]
    for copy in copies:
        copy.start()
    fill_bands(radius_ref, *tables)
    counts, weights, classes = local
    copies[0].wait()
    copies[1].wait()
    rows = counts.shape[0]
    for start in range(0, rows, STEP):
        at = slice(start, start + STEP)
        mass_ref[at] = counts[at].astype(F32) * weights[at]
    copies[2].wait()
    for start in range(0, rows, STEP):
        at = slice(start, start + STEP)
        label_ref[at] = classes[at].astype(F32).astype(BF16)
    odd = flags_of("row")[0]
    top, bottom = classes[0:REACH], classes[rows - REACH :]
    send_a[...] = chosen(odd, top, bottom)
    send_b[...] = chosen(odd, bottom, top)


def masked(pieces, labels, c):
    if labels is None:
        return pieces
    keep = labels == c
    return [jnp.where(keep, piece, jnp.zeros_like(piece)) for piece in pieces]


def rows_kernel(*refs, bands, labelled):
    (field_ref,), label_refs, (stack_ref, high_ref, low_ref, edge_ref) = take(refs, 1, labelled)
    _, columns = field_ref.shape
    for n in range(columns // TILE):
        at = slice(n * TILE, (n + 1) * TILE)
        pieces = split(field_ref[:, at])
        labels = label_refs[0][:, at] if labelled else None
        for slot, c in enumerate(bands):
            high, low = masked(pieces, labels, c)

            def part(t, start):
                own = slice(t * TILE, (t + 1) * TILE)
                right = jnp.concatenate([high[own], high[own], low[own]], axis=0)
                return dot(stack_ref[c, start : start + TILE + REACH, :], right)

            first, second = part(0, REACH), part(1, 0)
            edge_ref[slot, 0:REACH, at] = first[0:REACH]
            edge_ref[slot, REACH:, at] = second[TILE:]
            cut = TILE - REACH
            for target, value in (
                (0, first[REACH:cut]),
                (cut - REACH, first[cut:] + second[: 2 * REACH]),
                (cut + REACH, second[2 * REACH : TILE]),
            ):
                value_high, value_low = split(value)
                high_ref[slot, target : target + value.shape[0], at] = value_high
                low_ref[slot, target : target + value.shape[0], at] = value_low


def kept_row(start, rows):
    if start < REACH:
        return rows - 2 * REACH + start
    return start if start >= rows - REACH else start - REACH


def stacked_left(sides, inputs, start, stop, inner):
    refs, edge_ref = sides
    pieces = []
    slot = 0
    for ref in refs:
        for own in range(ref.shape[0]):
            rows = []
            if start < inner:
                rows.append(ref[own, start : min(stop, inner), inputs])
            if stop > inner:
                rows.append(edge_ref[slot, max(start, inner) - inner : stop - inner, inputs])
            pieces.append(rows[0] if len(rows) == 1 else jnp.concatenate(rows))
            slot += 1
    return jnp.concatenate(pieces, axis=1)


def swept(highs, lows, bands, band_refs, inputs, taps, outputs, start, stop, inner):
    right_high, right_low = (
        jnp.concatenate([ref[c * BAND + taps.start : c * BAND + taps.stop, outputs] for c in bands])
        for ref in band_refs
    )
    high = stacked_left(highs, inputs, start, stop, inner)
    low = stacked_left(lows, inputs, start, stop, inner)
    return dot(high, right_high) + dot(high, right_low) + dot(low, right_high)


def edges_kernel(*refs, groups, labelled):
    count = len(groups)
    halo, labels_in, partials, highs, lows, (rim_ref, *band_refs), outs = take(
        refs, 2, 2 * labelled, count, count, count, 3
    )
    edge_high, edge_low, left_ref, right_ref, send_a, send_b = outs
    bands = [c for group in groups for c in group]
    sources = [(ref, own) for ref in partials for own in range(ref.shape[0])]
    columns = halo[0].shape[1]
    odd_row, has_top, has_bottom = flags_of("row")
    odd_column = flags_of("col")[0]
    for n in range(columns // TILE):
        at = slice(n * TILE, (n + 1) * TILE)

        def joined(pair):
            first, second = pair[0][:, at].astype(F32), pair[1][:, at].astype(F32)
            top = chosen(has_top, chosen(odd_row, first, second), 0.0)
            bottom = chosen(has_bottom, chosen(odd_row, second, first), 0.0)
            missing = REACH - first.shape[0]
            if missing:
                zeros = jnp.zeros((missing, TILE), F32)
                return jnp.concatenate([zeros, top, bottom, zeros])
            return jnp.concatenate([top, bottom])

        pieces = split(joined(halo))
        labels = joined(labels_in).astype(BF16) if labelled else None
        for slot, c in enumerate(bands):
            high, low = masked(pieces, labels, c)
            right = jnp.concatenate([high, low, high], axis=0)
            source, own = sources[slot]
            value = source[own, :, at] + dot(rim_ref[c], right)
            edge_high[slot, :, at], edge_low[slot, :, at] = split(value)
    rows = left_ref.shape[0]
    inner = rows - 2 * REACH
    sides = (
        (left_ref, slice(0, TILE), slice(128, BAND), slice(0, TILE)),
        (right_ref, slice(columns - 128, columns), slice(0, 128), slice(0, 128)),
    )
    for target, *window in sides:
        target[...] = swept(
            (highs, edge_high), (lows, edge_low), bands, band_refs, *window, 0, rows, inner
        )
    half = rows // 2
    lower = iota((half, 128), 1) < REACH
    left = left_ref[:, 0:128]
    left = jnp.where(lower, left[:half], pltpu.roll(left[half:], REACH, 1))
    right = right_ref[...]
    right = jnp.where(lower, pltpu.roll(right[:half], REACH, 1), right[half:])
    send_a[...] = chosen(odd_column, left, right)
    send_b[...] = chosen(odd_column, right, left)


def middle_kernel(*refs, groups, start):
    count = len(groups)
    highs, lows, (edge_high, edge_low), band_refs, (out_ref,) = take(refs, count, count, 2, 2)
    bands = [c for group in groups for c in group]
    inner = highs[0].shape[1]
    stop = start + out_ref.shape[0]
    for j in range(out_ref.shape[1] // TILE):
        inputs = slice(j * TILE + 128, j * TILE + 128 + BAND)
        out_ref[:, j * TILE : (j + 1) * TILE] = swept(
            (highs, edge_high),
            (lows, edge_low),
            bands,
            band_refs,
            inputs,
            slice(0, BAND),
            slice(0, TILE),
            start,
            stop,
            inner,
        )


def gathered(pieces, come, flags, start):
    left_ref, middles, right_ref = pieces
    odd, has_left, has_right = flags
    rows = left_ref.shape[0]
    half = rows // 2
    kept = kept_row(start, rows)
    at = slice(kept, kept + STEP)
    lane = iota((STEP, 128), 1)
    local = slice(kept % half, kept % half + STEP)
    come_left = chosen(has_left, chosen(odd, come[0][local], come[1][local]), 0.0)
    come_right = chosen(has_right, chosen(odd, come[1][local], come[0][local]), 0.0)
    if kept < half:
        come_left = pltpu.roll(come_left, REACH, 1)
    else:
        come_right = pltpu.roll(come_right, REACH, 1)
    first = left_ref[at, 0:128] + jnp.where(lane >= REACH, come_left, 0.0)
    last = right_ref[at, :] + jnp.where(lane < REACH, come_right, 0.0)
    each = middles[0].shape[0]
    middle_ref = middles[kept // each]
    own = slice(kept % each, kept % each + STEP)
    blocks = [first, left_ref[at, 128:256]]
    blocks += [middle_ref[own, k : k + 128] for k in range(0, middle_ref.shape[1], 128)]
    blocks += [last]
    turned = [pltpu.roll(block, REACH, 1) for block in blocks]
    return [jnp.where(lane < REACH, a, b) for a, b in zip(turned[:-1], turned[1:])]


def finish_kernel(*refs, middles, scaled, following, totals):
    (left_ref,), middle_refs, (right_ref,), come, refs = take(refs, 1, middles, 1, 2)
    pieces = (left_ref, middle_refs, right_ref)
    totals_in, mass_in, density_out, refs = take(refs, 2 * scaled, following, scaled)
    adapted_out, refs = take(refs, 4 * following)
    if scaled:
        inverse = jnp.exp(-(totals_in[0][0:1, :] / totals_in[1][1:2, :]))
        staged, done = refs
    rows = left_ref.shape[0]
    column_flags = flags_of("col")
    log_sum = jnp.zeros((8, 128), F32)
    mass_sum = jnp.zeros((8, 128), F32)
    copies = []
    for number, start in enumerate(range(0, rows, STEP)):
        at = slice(start, start + STEP)
        for k, block in enumerate(gathered(pieces, come, column_flags, start)):
            lanes = slice(k * 128, (k + 1) * 128)
            if scaled:
                block = block * inverse
                staged[at, lanes] = block
            if following:
                pilot = block + BACKGROUND
                mass = mass_in[0][at, lanes]
                adapted_out[0][at, lanes] = mass * pilot
                terms = mass * jnp.log(pilot)
                log_sum += jnp.sum(terms.reshape(STEP // 8, 8, 128), axis=0)
                if totals:
                    mass_sum += jnp.sum(mass.reshape(STEP // 8, 8, 128), axis=0)
        if scaled:
            copy = pltpu.make_async_copy(staged.at[at], density_out[0].at[at], done.at[number])
            copy.start()
            copies.append(copy)
    if following:
        adapted_ref, send_a, send_b, stat_ref = adapted_out
        odd_row = flags_of("row")[0]
        top, bottom = adapted_ref[0:REACH], adapted_ref[rows - REACH :]
        send_a[...] = chosen(odd_row, top, bottom)
        send_b[...] = chosen(odd_row, bottom, top)
        log_sum = jnp.sum(log_sum, axis=(0, 1), keepdims=True)
        mass_sum = jnp.sum(mass_sum, axis=(0, 1), keepdims=True)
        row = iota((8, 128), 0)
        stat_ref[...] = jnp.where(row == 0, log_sum, jnp.where(row == 1, mass_sum, 0.0))
    for copy in copies:
        copy.wait()


def exchange(first, second, axis):
    results = []
    count = lax.axis_size(axis)
    for offset, value in ((0, first), (1, second)):
        pairs = []
        for i in range(offset, count, 2):
            pairs += [(i, (i + 1) % count), ((i + 1) % count, i)]
        results.append(lax.ppermute(value, axis, pairs))
    return results


HOPS = {1: (), 2: (1,), 4: (1, 3), 8: (1, 2, 6), 16: (4, 12, 1, 3)}


def total_over(stat):
    for axis in ("col", "row"):
        for hop in HOPS[lax.axis_size(axis)]:
            pairs = [(i, i ^ hop) for i in range(lax.axis_size(axis))]
            stat = stat + lax.ppermute(stat, axis, pairs)
    return stat


def smooth(field, halo, labels, label_halo, tables, groups, cuts):
    high, low, stack, rim = tables
    rows, columns = field.shape
    labelled = labels is not None
    bands = [c for group in groups for c in group]
    highs, lows, partials = [], [], []
    for group in groups:
        inner = (len(group), rows - 2 * REACH, columns)
        edge = (len(group), 2 * REACH, columns)
        results = call(
            functools.partial(rows_kernel, bands=group, labelled=labelled),
            [(inner, BF16), (inner, BF16), (edge, F32)],
            [field] + ([labels] if labelled else []) + [stack],
            flops=len(group) * 1_000_000_000,
        )
        for results_of, result in zip((highs, lows, partials), results):
            results_of.append(result)
    edge = (len(bands), 2 * REACH, columns)
    edge_high, edge_low, left, right, send_a, send_b = call(
        functools.partial(edges_kernel, groups=groups, labelled=labelled),
        [(edge, BF16), (edge, BF16), ((rows, TILE), F32), ((rows, 128), F32)]
        + [((rows // 2, 128), F32)] * 2,
        [*halo, *(label_halo if labelled else ()), *partials, *highs, *lows]
        + [rim, high, low],
        flops=len(bands) * 500_000_000,
    )
    come = exchange(send_a, send_b, "col")
    middles = []
    for number in range(cuts):
        middles += call(
            functools.partial(middle_kernel, groups=groups, start=number * (rows // cuts)),
            [((rows // cuts, columns - TILE), F32)],
            [*highs, *lows, edge_high, edge_low, high, low],
            flops=len(bands) * 750_000_000 // cuts,
        )
    return [left, *middles, right, *come]


def finish(pieces, extra, scaled, following, totals, shape):
    plane, rim, stat = (shape, F32), ((REACH, shape[1]), F32), ((8, 128), F32)
    outs = [plane] * scaled + [plane, rim, rim, stat] * following
    scratch = []
    if scaled:
        scratch = [pltpu.VMEM(shape, F32), pltpu.SemaphoreType.DMA((shape[0] // STEP,))]
    return call(
        functools.partial(
            finish_kernel,
            middles=len(pieces) - 4,
            scaled=scaled,
            following=following,
            totals=totals,
        ),
        outs,
        [*pieces, *extra],
        out_specs=[HBM] * scaled + [VMEM] * (4 * following),
        scratch=scratch,
        flops=500_000_000,
    )


def body(counts, sample_weights, classes, class_radius):
    shape = rows, columns = counts.shape
    is_odd = (lax.axis_index("row") & 1).astype(F32)
    groups = ((0, 1), (2, 3))
    rim = (REACH, columns)

    def ends(array, width):
        top, bottom = array[:width], array[rows - width :]
        return [jnp.where(is_odd > 0.5, *pair) for pair in ((top, bottom), (bottom, top))]

    sends = [
        number.astype(F32) * weight
        for number, weight in zip(ends(counts, PILOT_RADIUS), ends(sample_weights, PILOT_RADIUS))
    ]
    mass_halo = exchange(*sends, "row")
    wide = (CLASSES + 1) * BAND
    *tables, mass, labels, label_a, label_b = call(
        prepare_kernel,
        [
            ((wide, TILE), BF16),
            ((wide, TILE), BF16),
            ((CLASSES + 1, BAND, 3 * TILE), BF16),
            ((CLASSES + 1, 128, 384), BF16),
            (shape, F32),
            (shape, BF16),
            (rim, jnp.int32),
            (rim, jnp.int32),
        ],
        [class_radius]
        + [
            pltpu.with_memory_space_constraint(field, pltpu.HBM)
            for field in (counts, sample_weights, classes)
        ],
        ins=[SMEM, HBM, HBM, HBM],
        scratch=[
            pltpu.VMEM(shape, jnp.int32),
            pltpu.VMEM(shape, F32),
            pltpu.VMEM(shape, jnp.int32),
            pltpu.SemaphoreType.DMA((3,)),
        ],
        flops=500_000_000,
    )
    label_halo = exchange(label_a, label_b, "row")
    pieces = smooth(mass, mass_halo, None, None, tables, ((CLASSES,),), 1)
    adapted, *sends, first_stat = finish(pieces, [mass], False, True, True, shape)
    halo = exchange(*sends, "row")
    first_total = total_over(first_stat)
    pieces = smooth(adapted, halo, labels, label_halo, tables, groups, 2)
    density_first, adapted, *sends, second_stat = finish(
        pieces, [first_total, first_total, mass], True, True, False, shape
    )
    halo = exchange(*sends, "row")
    second_total = total_over(second_stat)
    pieces = smooth(adapted, halo, labels, label_halo, tables, groups, 2)
    (density_second,) = finish(
        pieces, [second_total, first_total], True, False, False, shape
    )
    return density_first, density_second


def solution(mesh):
    spec = P("row", "col")
    return jax.shard_map(
        body,
        mesh=mesh,
        in_specs=(spec, spec, spec, P()),
        out_specs=(spec, spec),
        check_vma=False,
    )
```

```python
import functools

import jax
import jax.numpy as jnp
from jax import lax
from jax.experimental import pallas as pl
from jax.experimental.pallas import tpu as pltpu
from jax.sharding import PartitionSpec as P


REACH = 64
PILOT_RADIUS = 32
CLASSES = 4
BACKGROUND = 0.5
TILE = 256
BAND = TILE + 2 * REACH
STEP = 64
F32 = jnp.float32
BF16 = jnp.bfloat16
MIB = 1 << 20
HBM = pl.BlockSpec(memory_space=pltpu.HBM)
VMEM = pl.BlockSpec(memory_space=pltpu.VMEM)
SMEM = pl.BlockSpec(memory_space=pltpu.SMEM)


def call(kernel, outs, args, ins=None, out_specs=None, scratch=(), limit=24, flops=100_000_000):
    return pl.pallas_call(
        kernel,
        out_shape=[jax.ShapeDtypeStruct(s, d) for s, d in outs],
        in_specs=ins or [VMEM] * len(args),
        out_specs=out_specs or [VMEM] * len(outs),
        scratch_shapes=scratch,
        compiler_params=pltpu.CompilerParams(vmem_limit_bytes=limit * MIB),
        cost_estimate=pl.CostEstimate(flops=flops, transcendentals=0, bytes_accessed=4 * MIB),
    )(*args)


def iota(shape, dim):
    return lax.broadcasted_iota(jnp.int32, shape, dim)


def split(value):
    high = value.astype(BF16)
    return high, (value - high.astype(F32)).astype(BF16)


def dot(a, b):
    return jnp.dot(a, b, preferred_element_type=F32)


def take(refs, *counts):
    groups = []
    for count in counts:
        groups.append(list(refs[:count]))
        refs = refs[count:]
    return *groups, list(refs)


def chosen(flag, when_set, when_clear):
    return jnp.where(flag > 0.5, when_set, when_clear)


def flags_of(axis):
    index = lax.axis_index(axis)
    last = lax.axis_size(axis) - 1
    values = (index & 1, jnp.minimum(index, 1), jnp.minimum(last - index, 1))
    return [jnp.full((1, 1), value.astype(F32), F32) for value in values]


def fill_bands(slot, radius, high_ref, low_ref, stack_ref, rim_ref):
    radius = jnp.full((1, 1), radius, F32)
    inverse = 1.0 / (2.0 * (0.5 * radius) * (0.5 * radius))

    def shape_of(d):
        return jnp.where(jnp.abs(d) <= radius, jnp.exp(-(d * d) * inverse), 0.0)

    lane = iota((8, 128), 1).astype(F32)
    tap = jnp.where(iota((8, 128), 0) == 0, jnp.where(lane == 0, 1.0, 2.0), 0.0)
    total = jnp.sum(shape_of(lane) * tap, axis=(0, 1), keepdims=True)
    column = iota((128, 128), 1)
    shift = iota((128, 128), 0) - column
    near = split(shape_of((shift - REACH).astype(F32)) / total)
    far = split(shape_of((shift + REACH).astype(F32)) / total)
    zero = jnp.zeros((128, 128), BF16)
    side = column[:REACH] < REACH
    zeros = jnp.zeros((REACH, 128), F32)
    base = slot * BAND
    for part, ref in enumerate((high_ref, low_ref)):
        blocks = ((near[part], zero), (far[part], near[part]), (zero, far[part]))
        for i, pair in enumerate(blocks):
            for k, block in enumerate(pair):
                lanes = slice(k * 128, (k + 1) * 128)
                ref[base + i * 128 : base + (i + 1) * 128, lanes] = block
                places = (0, 2 * TILE) if part == 0 else (TILE,)
                for place in places:
                    shifted = slice(place + k * 128, place + (k + 1) * 128)
                    stack_ref[slot, i * 128 : (i + 1) * 128, shifted] = block
        first = jnp.where(side, far[part][:REACH].astype(F32), zeros).astype(BF16)
        second = jnp.where(side, zeros, near[part][REACH:].astype(F32)).astype(BF16)
        for place in (0, 128) if part == 0 else (256,):
            rim_ref[slot, :REACH, place : place + 128] = first
            rim_ref[slot, REACH:, place : place + 128] = second


CHUNK = 128


def prepare_kernel(*refs):
    (counts_in, weights_in, classes_in), tables, outs, scratch = take(refs, 3, 4, 5)
    mass_ref, mass_a, mass_b, label_a, label_b = outs
    counts, weights, ends, arrived, ended = scratch
    rows = counts.shape[0]
    copies = []
    for n, start in enumerate(range(0, rows, CHUNK)):
        at = slice(start, start + CHUNK)
        pair = [
            pltpu.make_async_copy(counts_in.at[at], counts.at[at], arrived.at[0, n]),
            pltpu.make_async_copy(weights_in.at[at], weights.at[at], arrived.at[1, n]),
        ]
        for copy in pair:
            copy.start()
        copies.append((at, pair))
    end_copies = [
        pltpu.make_async_copy(classes_in.at[0:REACH], ends.at[0], ended.at[0]),
        pltpu.make_async_copy(classes_in.at[rows - REACH : rows], ends.at[1], ended.at[1]),
    ]
    for copy in end_copies:
        copy.start()
    fill_bands(0, F32(PILOT_RADIUS), *tables)
    for at, pair in copies:
        for copy in pair:
            copy.wait()
        mass_ref[at] = counts[at].astype(F32) * weights[at]
    odd = flags_of("row")[0]
    top, bottom = mass_ref[0:PILOT_RADIUS], mass_ref[rows - PILOT_RADIUS :]
    mass_a[...] = chosen(odd, top, bottom)
    mass_b[...] = chosen(odd, bottom, top)
    for copy in end_copies:
        copy.wait()
    label_a[...] = chosen(odd, ends[0], ends[1])
    label_b[...] = chosen(odd, ends[1], ends[0])


def bands_kernel(*refs):
    (radius_ref, classes_in), tables, (label_ref, classes, arrived) = take(refs, 2, 4)
    rows = classes.shape[0]
    copies = []
    for n, start in enumerate(range(0, rows, CHUNK)):
        at = slice(start, start + CHUNK)
        copy = pltpu.make_async_copy(classes_in.at[at], classes.at[at], arrived.at[n])
        copy.start()
        copies.append((at, copy))
    for c in range(CLASSES):
        fill_bands(c, radius_ref[c].astype(F32), *tables)
    for at, copy in copies:
        copy.wait()
        label_ref[at] = classes[at].astype(F32).astype(BF16)


def masked(pieces, labels, c):
    if labels is None:
        return pieces
    keep = labels == c
    return [jnp.where(keep, piece, jnp.zeros_like(piece)) for piece in pieces]


def rows_kernel(*refs, bands, labelled, carried):
    (field_ref,), label_refs, (stack_ref,), plane, (high_ref, low_ref, edge_ref), plane_out, done = (
        take(refs, 1, labelled, 1, carried, 3, carried)
    )
    copies = [pltpu.make_async_copy(*pair) for pair in zip(plane, plane_out, done)]
    for copy in copies:
        copy.start()
    _, columns = field_ref.shape
    for n in range(columns // TILE):
        at = slice(n * TILE, (n + 1) * TILE)
        pieces = split(field_ref[:, at])
        labels = label_refs[0][:, at] if labelled else None
        for slot, c in enumerate(bands):
            high, low = masked(pieces, labels, c)

            def part(t, start):
                own = slice(t * TILE, (t + 1) * TILE)
                right = jnp.concatenate([high[own], high[own], low[own]], axis=0)
                return dot(stack_ref[c, start : start + TILE + REACH, :], right)

            first, second = part(0, REACH), part(1, 0)
            edge_ref[slot, 0:REACH, at] = first[0:REACH]
            edge_ref[slot, REACH:, at] = second[TILE:]
            cut = TILE - REACH
            for target, value in (
                (0, first[REACH:cut]),
                (cut - REACH, first[cut:] + second[: 2 * REACH]),
                (cut + REACH, second[2 * REACH : TILE]),
            ):
                value_high, value_low = split(value)
                high_ref[slot, target : target + value.shape[0], at] = value_high
                low_ref[slot, target : target + value.shape[0], at] = value_low
    for copy in copies:
        copy.wait()


def kept_row(start, rows):
    if start < REACH:
        return rows - 2 * REACH + start
    return start if start >= rows - REACH else start - REACH


def stacked_left(sides, inputs, start, stop, inner):
    refs, edge_ref = sides
    pieces = []
    slot = 0
    for ref in refs:
        for own in range(ref.shape[0]):
            rows = []
            if start < inner:
                rows.append(ref[own, start : min(stop, inner), inputs])
            if stop > inner:
                rows.append(edge_ref[slot, max(start, inner) - inner : stop - inner, inputs])
            pieces.append(rows[0] if len(rows) == 1 else jnp.concatenate(rows))
            slot += 1
    return jnp.concatenate(pieces, axis=1)


def swept(highs, lows, bands, band_refs, inputs, taps, outputs, start, stop, inner):
    right_high, right_low = (
        jnp.concatenate([ref[c * BAND + taps.start : c * BAND + taps.stop, outputs] for c in bands])
        for ref in band_refs
    )
    high = stacked_left(highs, inputs, start, stop, inner)
    low = stacked_left(lows, inputs, start, stop, inner)
    return dot(high, right_high) + dot(high, right_low) + dot(low, right_high)


def edges_kernel(*refs, groups, labelled):
    count = len(groups)
    halo, labels_in, partials, highs, lows, (rim_ref, *band_refs), outs = take(
        refs, 2, 2 * labelled, count, count, count, 3
    )
    edge_high, edge_low, left_ref, right_ref, send_a, send_b = outs
    bands = [c for group in groups for c in group]
    sources = [(ref, own) for ref in partials for own in range(ref.shape[0])]
    columns = halo[0].shape[1]
    odd_row, has_top, has_bottom = flags_of("row")
    odd_column = flags_of("col")[0]
    for n in range(columns // TILE):
        at = slice(n * TILE, (n + 1) * TILE)

        def joined(pair):
            first, second = pair[0][:, at].astype(F32), pair[1][:, at].astype(F32)
            top = chosen(has_top, chosen(odd_row, first, second), 0.0)
            bottom = chosen(has_bottom, chosen(odd_row, second, first), 0.0)
            missing = REACH - first.shape[0]
            if missing:
                zeros = jnp.zeros((missing, TILE), F32)
                return jnp.concatenate([zeros, top, bottom, zeros])
            return jnp.concatenate([top, bottom])

        pieces = split(joined(halo))
        labels = joined(labels_in).astype(BF16) if labelled else None
        for slot, c in enumerate(bands):
            high, low = masked(pieces, labels, c)
            right = jnp.concatenate([high, low, high], axis=0)
            source, own = sources[slot]
            value = source[own, :, at] + dot(rim_ref[c], right)
            edge_high[slot, :, at], edge_low[slot, :, at] = split(value)
    rows = left_ref.shape[0]
    inner = rows - 2 * REACH
    sides = (
        (left_ref, slice(0, TILE), slice(128, BAND), slice(0, TILE)),
        (right_ref, slice(columns - 128, columns), slice(0, 128), slice(0, 128)),
    )
    for target, *window in sides:
        target[...] = swept(
            (highs, edge_high), (lows, edge_low), bands, band_refs, *window, 0, rows, inner
        )
    half = rows // 2
    lower = iota((half, 128), 1) < REACH
    left = left_ref[:, 0:128]
    left = jnp.where(lower, left[:half], pltpu.roll(left[half:], REACH, 1))
    right = right_ref[...]
    right = jnp.where(lower, pltpu.roll(right[:half], REACH, 1), right[half:])
    send_a[...] = chosen(odd_column, left, right)
    send_b[...] = chosen(odd_column, right, left)


def middle_kernel(*refs, groups, start):
    count = len(groups)
    highs, lows, (edge_high, edge_low), band_refs, (out_ref,) = take(refs, count, count, 2, 2)
    bands = [c for group in groups for c in group]
    inner = highs[0].shape[1]
    stop = start + out_ref.shape[0]
    for j in range(out_ref.shape[1] // TILE):
        inputs = slice(j * TILE + 128, j * TILE + 128 + BAND)
        out_ref[:, j * TILE : (j + 1) * TILE] = swept(
            (highs, edge_high),
            (lows, edge_low),
            bands,
            band_refs,
            inputs,
            slice(0, BAND),
            slice(0, TILE),
            start,
            stop,
            inner,
        )


def gathered(pieces, come, flags, start):
    left_ref, middles, right_ref = pieces
    odd, has_left, has_right = flags
    rows = left_ref.shape[0]
    half = rows // 2
    kept = kept_row(start, rows)
    at = slice(kept, kept + STEP)
    lane = iota((STEP, 128), 1)
    local = slice(kept % half, kept % half + STEP)
    come_left = chosen(has_left, chosen(odd, come[0][local], come[1][local]), 0.0)
    come_right = chosen(has_right, chosen(odd, come[1][local], come[0][local]), 0.0)
    if kept < half:
        come_left = pltpu.roll(come_left, REACH, 1)
    else:
        come_right = pltpu.roll(come_right, REACH, 1)
    first = left_ref[at, 0:128] + jnp.where(lane >= REACH, come_left, 0.0)
    last = right_ref[at, :] + jnp.where(lane < REACH, come_right, 0.0)
    each = middles[0].shape[0]
    middle_ref = middles[kept // each]
    own = slice(kept % each, kept % each + STEP)
    blocks = [first, left_ref[at, 128:256]]
    blocks += [middle_ref[own, k : k + 128] for k in range(0, middle_ref.shape[1], 128)]
    blocks += [last]
    turned = [pltpu.roll(block, REACH, 1) for block in blocks]
    return [jnp.where(lane < REACH, a, b) for a, b in zip(turned[:-1], turned[1:])]


def finish_kernel(*refs, middles, scaled, following, totals):
    leaving = scaled and not following
    (left_ref,), middle_refs, (right_ref,), come, refs = take(refs, 1, middles, 1, 2)
    pieces = (left_ref, middle_refs, right_ref)
    totals_in, mass_in, density_out, refs = take(refs, 2 * scaled, following, scaled)
    adapted_out, refs = take(refs, 4 * following)
    if scaled:
        inverse = jnp.exp(-(totals_in[0][0:1, :] / totals_in[1][1:2, :]))
    staged, done = refs if leaving else (density_out[0] if scaled else None, None)
    rows = left_ref.shape[0]
    column_flags = flags_of("col")
    log_sum = jnp.zeros((8, 128), F32)
    mass_sum = jnp.zeros((8, 128), F32)
    copies = []
    for number, start in enumerate(range(0, rows, STEP)):
        at = slice(start, start + STEP)
        for k, block in enumerate(gathered(pieces, come, column_flags, start)):
            lanes = slice(k * 128, (k + 1) * 128)
            if scaled:
                block = block * inverse
                staged[at, lanes] = block
            if following:
                pilot = block + BACKGROUND
                mass = mass_in[0][at, lanes]
                adapted_out[0][at, lanes] = mass * pilot
                terms = mass * jnp.log(pilot)
                log_sum += jnp.sum(terms.reshape(STEP // 8, 8, 128), axis=0)
                if totals:
                    mass_sum += jnp.sum(mass.reshape(STEP // 8, 8, 128), axis=0)
        if leaving:
            copy = pltpu.make_async_copy(staged.at[at], density_out[0].at[at], done.at[number])
            copy.start()
            copies.append(copy)
    if following:
        adapted_ref, send_a, send_b, stat_ref = adapted_out
        odd_row = flags_of("row")[0]
        top, bottom = adapted_ref[0:REACH], adapted_ref[rows - REACH :]
        send_a[...] = chosen(odd_row, top, bottom)
        send_b[...] = chosen(odd_row, bottom, top)
        log_sum = jnp.sum(log_sum, axis=(0, 1), keepdims=True)
        mass_sum = jnp.sum(mass_sum, axis=(0, 1), keepdims=True)
        row = iota((8, 128), 0)
        stat_ref[...] = jnp.where(row == 0, log_sum, jnp.where(row == 1, mass_sum, 0.0))
    for copy in copies:
        copy.wait()


def exchange(first, second, axis):
    along = 0 if axis == "row" else 1
    sizes = [lax.axis_size("row"), lax.axis_size("col")]
    results = []
    for offset, value in ((0, first), (1, second)):
        pairs = []
        for index in range(sizes[0] * sizes[1]):
            place = [index // sizes[1], index % sizes[1]]
            own = place[along]
            partner = own + 1 if own % 2 == offset else own - 1
            if 0 <= partner < sizes[along]:
                place[along] = partner
            else:
                place[1 - along] ^= 1
            pairs.append((index, place[0] * sizes[1] + place[1]))
        results.append(lax.ppermute(value, ("row", "col"), pairs))
    return results


HOPS = {1: (), 2: (1,), 4: (1, 3), 8: (1, 2, 6), 16: (4, 12, 1, 3)}


def total_over(stat):
    for axis in ("col", "row"):
        for hop in HOPS[lax.axis_size(axis)]:
            pairs = [(i, i ^ hop) for i in range(lax.axis_size(axis))]
            stat = stat + lax.ppermute(stat, axis, pairs)
    return stat


def smooth(field, halo, labels, label_halo, tables, groups, cuts, leaving=()):
    high, low, stack, rim = tables
    rows, columns = field.shape
    labelled = labels is not None
    bands = [c for group in groups for c in group]
    highs, lows, partials = [], [], []
    for number, group in enumerate(groups):
        inner = (len(group), rows - 2 * REACH, columns)
        edge = (len(group), 2 * REACH, columns)
        carried = len(leaving) if number == 0 else 0
        results = call(
            functools.partial(
                rows_kernel, bands=group, labelled=labelled, carried=carried
            ),
            [(inner, BF16), (inner, BF16), (edge, F32)] + [(field.shape, F32)] * carried,
            [field] + ([labels] if labelled else []) + [stack, *leaving[:carried]],
            out_specs=[VMEM] * 3 + [HBM] * carried,
            scratch=[pltpu.SemaphoreType.DMA] * carried,
            flops=len(group) * 1_000_000_000,
        )
        if carried:
            left_behind = results[3]
        for results_of, result in zip((highs, lows, partials), results):
            results_of.append(result)
    edge = (len(bands), 2 * REACH, columns)
    edge_high, edge_low, left, right, send_a, send_b = call(
        functools.partial(edges_kernel, groups=groups, labelled=labelled),
        [(edge, BF16), (edge, BF16), ((rows, TILE), F32), ((rows, 128), F32)]
        + [((rows // 2, 128), F32)] * 2,
        [*halo, *(label_halo if labelled else ()), *partials, *highs, *lows]
        + [rim, high, low],
        flops=len(bands) * 500_000_000,
    )
    come = exchange(send_a, send_b, "col")
    middles = []
    for number in range(cuts):
        middles += call(
            functools.partial(middle_kernel, groups=groups, start=number * (rows // cuts)),
            [((rows // cuts, columns - TILE), F32)],
            [*highs, *lows, edge_high, edge_low, high, low],
            flops=len(bands) * 750_000_000 // cuts,
        )
    pieces = [left, *middles, right, *come]
    return (pieces, left_behind) if leaving else pieces


def finish(pieces, extra, scaled, following, totals, shape):
    plane, rim, stat = (shape, F32), ((REACH, shape[1]), F32), ((8, 128), F32)
    outs = [plane] * scaled + [plane, rim, rim, stat] * following
    scratch = []
    leaving = scaled and not following
    if leaving:
        scratch = [pltpu.VMEM(shape, F32), pltpu.SemaphoreType.DMA((shape[0] // STEP,))]
    return call(
        functools.partial(
            finish_kernel,
            middles=len(pieces) - 4,
            scaled=scaled,
            following=following,
            totals=totals,
        ),
        outs,
        [*pieces, *extra],
        out_specs=[HBM if leaving else VMEM] * scaled + [VMEM] * (4 * following),
        scratch=scratch,
        flops=500_000_000,
    )


def tables_of(count):
    return [
        ((count * BAND, TILE), BF16),
        ((count * BAND, TILE), BF16),
        ((count, BAND, 3 * TILE), BF16),
        ((count, 128, 384), BF16),
    ]


def body(counts, sample_weights, classes, class_radius):
    shape = rows, columns = counts.shape
    groups = ((0, 1), (2, 3))
    rim, slim = (REACH, columns), (PILOT_RADIUS, columns)
    counts, sample_weights, classes = (
        pltpu.with_memory_space_constraint(field, pltpu.HBM)
        for field in (counts, sample_weights, classes)
    )
    chunks = rows // CHUNK
    *pilot_tables, mass, mass_a, mass_b, label_a, label_b = call(
        prepare_kernel,
        tables_of(1)
        + [(shape, F32), (slim, F32), (slim, F32), (rim, jnp.int32), (rim, jnp.int32)],
        [counts, sample_weights, classes],
        ins=[HBM, HBM, HBM],
        scratch=[
            pltpu.VMEM(shape, jnp.int32),
            pltpu.VMEM(shape, F32),
            pltpu.VMEM((2, *rim), jnp.int32),
            pltpu.SemaphoreType.DMA((2, chunks)),
            pltpu.SemaphoreType.DMA((2,)),
        ],
        flops=500_000_000,
    )
    mass_halo = exchange(mass_a, mass_b, "row")
    label_halo = exchange(label_a, label_b, "row")
    *tables, labels = call(
        bands_kernel,
        tables_of(CLASSES) + [(shape, BF16)],
        [class_radius, classes],
        ins=[SMEM, HBM],
        scratch=[pltpu.VMEM(shape, jnp.int32), pltpu.SemaphoreType.DMA((chunks,))],
        flops=500_000_000,
    )
    pieces = smooth(mass, mass_halo, None, None, pilot_tables, ((0,),), 1)
    adapted, *sends, first_stat = finish(pieces, [mass], False, True, True, shape)
    halo = exchange(*sends, "row")
    first_total = total_over(first_stat)
    pieces = smooth(adapted, halo, labels, label_halo, tables, groups, 2)
    density_first, adapted, *sends, second_stat = finish(
        pieces, [first_total, first_total, mass], True, True, False, shape
    )
    halo = exchange(*sends, "row")
    second_total = total_over(second_stat)
    pieces, density_first = smooth(
        adapted, halo, labels, label_halo, tables, groups, 2, (density_first,)
    )
    (density_second,) = finish(
        pieces, [second_total, first_total], True, False, False, shape
    )
    return density_first, density_second


def solution(mesh):
    spec = P("row", "col")
    return jax.shard_map(
        body,
        mesh=mesh,
        in_specs=(spec, spec, spec, P()),
        out_specs=(spec, spec),
        check_vma=False,
    )
```

```python
import functools

import jax
import jax.numpy as jnp
from jax import lax
from jax.experimental import pallas as pl
from jax.experimental.pallas import tpu as pltpu
from jax.sharding import PartitionSpec as P


REACH = 64
PILOT_RADIUS = 32
CLASSES = 4
BACKGROUND = 0.5
TILE = 256
BAND = TILE + 2 * REACH
STEP = 64
F32 = jnp.float32
BF16 = jnp.bfloat16
MIB = 1 << 20
HBM = pl.BlockSpec(memory_space=pltpu.HBM)
VMEM = pl.BlockSpec(memory_space=pltpu.VMEM)
SMEM = pl.BlockSpec(memory_space=pltpu.SMEM)


def call(kernel, outs, args, ins=None, out_specs=None, scratch=(), limit=24, flops=100_000_000):
    return pl.pallas_call(
        kernel,
        out_shape=[jax.ShapeDtypeStruct(s, d) for s, d in outs],
        in_specs=ins or [VMEM] * len(args),
        out_specs=out_specs or [VMEM] * len(outs),
        scratch_shapes=scratch,
        compiler_params=pltpu.CompilerParams(vmem_limit_bytes=limit * MIB),
        cost_estimate=pl.CostEstimate(flops=flops, transcendentals=0, bytes_accessed=4 * MIB),
    )(*args)


def iota(shape, dim):
    return lax.broadcasted_iota(jnp.int32, shape, dim)


def split(value):
    high = value.astype(BF16)
    return high, (value - high.astype(F32)).astype(BF16)


def dot(a, b):
    return jnp.dot(a, b, preferred_element_type=F32)


def take(refs, *counts):
    groups = []
    for count in counts:
        groups.append(list(refs[:count]))
        refs = refs[count:]
    return *groups, list(refs)


def chosen(flag, when_set, when_clear):
    return jnp.where(flag > 0.5, when_set, when_clear)


def flags_of(axis):
    index = lax.axis_index(axis)
    last = lax.axis_size(axis) - 1
    values = (index & 1, jnp.minimum(index, 1), jnp.minimum(last - index, 1))
    return [jnp.full((1, 1), value.astype(F32), F32) for value in values]


def fill_bands(slot, radius, high_ref, low_ref, rim_ref):
    radius = jnp.full((1, 1), radius, F32)
    inverse = 1.0 / (2.0 * (0.5 * radius) * (0.5 * radius))

    def shape_of(d):
        return jnp.where(jnp.abs(d) <= radius, jnp.exp(-(d * d) * inverse), 0.0)

    lane = iota((8, 128), 1).astype(F32)
    tap = jnp.where(iota((8, 128), 0) == 0, jnp.where(lane == 0, 1.0, 2.0), 0.0)
    total = jnp.sum(shape_of(lane) * tap, axis=(0, 1), keepdims=True)
    column = iota((128, 128), 1)
    shift = iota((128, 128), 0) - column
    near = split(shape_of((shift - REACH).astype(F32)) / total)
    far = split(shape_of((shift + REACH).astype(F32)) / total)
    zero = jnp.zeros((128, 128), BF16)
    side = column[:REACH] < REACH
    zeros = jnp.zeros((REACH, 128), F32)
    base = slot * BAND
    for part, ref in enumerate((high_ref, low_ref)):
        blocks = ((near[part], zero), (far[part], near[part]), (zero, far[part]))
        for i, pair in enumerate(blocks):
            for k, block in enumerate(pair):
                lanes = slice(k * 128, (k + 1) * 128)
                ref[base + i * 128 : base + (i + 1) * 128, lanes] = block
        first = jnp.where(side, far[part][:REACH].astype(F32), zeros).astype(BF16)
        second = jnp.where(side, zeros, near[part][REACH:].astype(F32)).astype(BF16)
        for place in (0, 128) if part == 0 else (256,):
            rim_ref[slot, :REACH, place : place + 128] = first
            rim_ref[slot, REACH:, place : place + 128] = second


CHUNK = 128


def prepare_kernel(*refs):
    (counts_in, weights_in, classes_in), tables, outs, scratch = take(refs, 3, 3, 5)
    mass_ref, mass_a, mass_b, label_a, label_b = outs
    counts, weights, ends, arrived, ended = scratch
    rows = counts.shape[0]
    copies = []
    for n, start in enumerate(range(0, rows, CHUNK)):
        at = slice(start, start + CHUNK)
        pair = [
            pltpu.make_async_copy(counts_in.at[at], counts.at[at], arrived.at[0, n]),
            pltpu.make_async_copy(weights_in.at[at], weights.at[at], arrived.at[1, n]),
        ]
        for copy in pair:
            copy.start()
        copies.append((at, pair))
    end_copies = [
        pltpu.make_async_copy(classes_in.at[0:REACH], ends.at[0], ended.at[0]),
        pltpu.make_async_copy(classes_in.at[rows - REACH : rows], ends.at[1], ended.at[1]),
    ]
    for copy in end_copies:
        copy.start()
    fill_bands(0, F32(PILOT_RADIUS), *tables)
    for at, pair in copies:
        for copy in pair:
            copy.wait()
        mass_ref[at] = counts[at].astype(F32) * weights[at]
    odd = flags_of("row")[0]
    top, bottom = mass_ref[0:PILOT_RADIUS], mass_ref[rows - PILOT_RADIUS :]
    mass_a[...] = chosen(odd, top, bottom)
    mass_b[...] = chosen(odd, bottom, top)
    for copy in end_copies:
        copy.wait()
    label_a[...] = chosen(odd, ends[0], ends[1])
    label_b[...] = chosen(odd, ends[1], ends[0])


def bands_kernel(*refs):
    (radius_ref, classes_in), tables, (label_ref, classes, arrived) = take(refs, 2, 3)
    rows = classes.shape[0]
    copies = []
    for n, start in enumerate(range(0, rows, CHUNK)):
        at = slice(start, start + CHUNK)
        copy = pltpu.make_async_copy(classes_in.at[at], classes.at[at], arrived.at[n])
        copy.start()
        copies.append((at, copy))
    for c in range(CLASSES):
        fill_bands(c, radius_ref[c].astype(F32), *tables)
    for at, copy in copies:
        copy.wait()
        label_ref[at] = classes[at].astype(F32).astype(BF16)


def masked(pieces, labels, c):
    if labels is None:
        return pieces
    keep = labels == c
    return [jnp.where(keep, piece, jnp.zeros_like(piece)) for piece in pieces]


def rows_kernel(*refs, bands, labelled, carried):
    (field_ref,), label_refs, (band_high, band_low), plane, outs, plane_out, done = take(
        refs, 1, labelled, 2, carried, 3, carried
    )
    high_ref, low_ref, edge_ref = outs
    copies = [pltpu.make_async_copy(*pair) for pair in zip(plane, plane_out, done)]
    for copy in copies:
        copy.start()
    rows, columns = field_ref.shape
    count = rows // REACH
    for n in range(columns // TILE):
        at = slice(n * TILE, (n + 1) * TILE)
        pieces = split(field_ref[:, at])
        labels = label_refs[0][:, at] if labelled else None
        for slot, c in enumerate(bands):
            high, low = masked(pieces, labels, c)
            sums = [None] * count

            def add(result, first):
                for i in range(result.shape[0] // REACH):
                    piece = result[i * REACH : (i + 1) * REACH]
                    own = sums[first + i]
                    sums[first + i] = piece if own is None else own + piece

            half = band_high[c * BAND : c * BAND + 2 * 128, 0:128]
            twice = jnp.concatenate([half, half], axis=1)
            for block in range(rows // 128):
                own = slice(block * 128, (block + 1) * 128)
                first = max(2 * block - 1, 0)
                last = min(2 * block + 3, count)
                taps = slice((first - 2 * block + 1) * REACH, (last - 2 * block + 1) * REACH)
                add(dot(twice[taps], jnp.concatenate([high[own], low[own]])), first)
            for tile in range(rows // TILE):
                own = slice(tile * TILE, (tile + 1) * TILE)
                first = max(4 * tile - 1, 0)
                last = min(4 * tile + 5, count)
                start = c * BAND + (first - 4 * tile + 1) * REACH
                taps = slice(start, start + (last - first) * REACH)
                add(dot(band_low[taps, :], high[own]), first)
            edge_ref[slot, 0:REACH, at] = sums[0]
            edge_ref[slot, REACH:, at] = sums[-1]
            for i, value in enumerate(sums[1:-1]):
                target = slice(i * REACH, (i + 1) * REACH)
                high_ref[slot, target, at], low_ref[slot, target, at] = split(value)
    for copy in copies:
        copy.wait()


def kept_row(start, rows):
    if start < REACH:
        return rows - 2 * REACH + start
    return start if start >= rows - REACH else start - REACH


def stacked_left(sides, inputs, start, stop, inner):
    refs, edge_ref = sides
    pieces = []
    slot = 0
    for ref in refs:
        for own in range(ref.shape[0]):
            rows = []
            if start < inner:
                rows.append(ref[own, start : min(stop, inner), inputs])
            if stop > inner:
                rows.append(edge_ref[slot, max(start, inner) - inner : stop - inner, inputs])
            pieces.append(rows[0] if len(rows) == 1 else jnp.concatenate(rows))
            slot += 1
    return jnp.concatenate(pieces, axis=1)


def swept(highs, lows, bands, band_refs, block, width, columns, start, stop, inner):
    high_ref, low_ref = band_refs

    def window(first, last):
        here, there = max(first, 0), min(last, columns)
        return slice(here, there), slice(here - first, there - first)

    def rights(refs_and_lanes, taps):
        return jnp.concatenate(
            [
                jnp.concatenate(
                    [ref[c * BAND + taps.start : c * BAND + taps.stop, lanes] for ref, lanes in refs_and_lanes],
                    axis=1,
                )
                for c in bands
            ]
        )

    results = []
    origin = block * TILE - 128
    for part in range(width // 128):
        inputs, taps = window(origin + part * 128, origin + (part + 2) * 128)
        left = stacked_left(highs, inputs, start, stop, inner)
        right = rights(((high_ref, slice(0, 128)), (low_ref, slice(0, 128))), taps)
        both = dot(left, right)
        results.append(both[:, :128] + both[:, 128:])
    inputs, taps = window(origin, origin + width + 128)
    left = stacked_left(lows, inputs, start, stop, inner)
    rest = dot(left, rights(((high_ref, slice(0, width)),), taps))
    return [value + rest[:, k * 128 : (k + 1) * 128] for k, value in enumerate(results)]


def edges_kernel(*refs, groups, labelled):
    count = len(groups)
    halo, labels_in, partials, highs, lows, (rim_ref, *band_refs), outs = take(
        refs, 2, 2 * labelled, count, count, count, 3
    )
    edge_high, edge_low, left_ref, right_ref, send_a, send_b = outs
    bands = [c for group in groups for c in group]
    sources = [(ref, own) for ref in partials for own in range(ref.shape[0])]
    columns = halo[0].shape[1]
    odd_row, has_top, has_bottom = flags_of("row")
    odd_column = flags_of("col")[0]
    for n in range(columns // TILE):
        at = slice(n * TILE, (n + 1) * TILE)

        def joined(pair):
            first, second = pair[0][:, at].astype(F32), pair[1][:, at].astype(F32)
            top = chosen(has_top, chosen(odd_row, first, second), 0.0)
            bottom = chosen(has_bottom, chosen(odd_row, second, first), 0.0)
            missing = REACH - first.shape[0]
            if missing:
                zeros = jnp.zeros((missing, TILE), F32)
                return jnp.concatenate([zeros, top, bottom, zeros])
            return jnp.concatenate([top, bottom])

        pieces = split(joined(halo))
        labels = joined(labels_in).astype(BF16) if labelled else None
        for slot, c in enumerate(bands):
            high, low = masked(pieces, labels, c)
            right = jnp.concatenate([high, low, high], axis=0)
            source, own = sources[slot]
            value = source[own, :, at] + dot(rim_ref[c], right)
            edge_high[slot, :, at], edge_low[slot, :, at] = split(value)
    rows = left_ref.shape[0]
    inner = rows - 2 * REACH
    for target, block in ((left_ref, 0), (right_ref, columns // TILE)):
        results = swept(
            (highs, edge_high),
            (lows, edge_low),
            bands,
            band_refs,
            block,
            target.shape[1],
            columns,
            0,
            rows,
            inner,
        )
        for k, value in enumerate(results):
            target[:, k * 128 : (k + 1) * 128] = value
    half = rows // 2
    lower = iota((half, 128), 1) < REACH
    left = left_ref[:, 0:128]
    left = jnp.where(lower, left[:half], pltpu.roll(left[half:], REACH, 1))
    right = right_ref[...]
    right = jnp.where(lower, pltpu.roll(right[:half], REACH, 1), right[half:])
    send_a[...] = chosen(odd_column, left, right)
    send_b[...] = chosen(odd_column, right, left)


def middle_kernel(*refs, groups, start):
    count = len(groups)
    highs, lows, (edge_high, edge_low), band_refs, (out_ref,) = take(refs, count, count, 2, 2)
    bands = [c for group in groups for c in group]
    inner = highs[0].shape[1]
    for j in range(out_ref.shape[1] // TILE):
        results = swept(
            (highs, edge_high),
            (lows, edge_low),
            bands,
            band_refs,
            j + 1,
            TILE,
            edge_high.shape[2],
            start,
            start + out_ref.shape[0],
            inner,
        )
        for k, value in enumerate(results):
            out_ref[:, j * TILE + k * 128 : j * TILE + (k + 1) * 128] = value


def gathered(pieces, come, flags, start):
    left_ref, middles, right_ref = pieces
    odd, has_left, has_right = flags
    rows = left_ref.shape[0]
    half = rows // 2
    kept = kept_row(start, rows)
    at = slice(kept, kept + STEP)
    lane = iota((STEP, 128), 1)
    local = slice(kept % half, kept % half + STEP)
    come_left = chosen(has_left, chosen(odd, come[0][local], come[1][local]), 0.0)
    come_right = chosen(has_right, chosen(odd, come[1][local], come[0][local]), 0.0)
    if kept < half:
        come_left = pltpu.roll(come_left, REACH, 1)
    else:
        come_right = pltpu.roll(come_right, REACH, 1)
    first = left_ref[at, 0:128] + jnp.where(lane >= REACH, come_left, 0.0)
    last = right_ref[at, :] + jnp.where(lane < REACH, come_right, 0.0)
    own = kept
    for middle_ref in middles:
        if own < middle_ref.shape[0]:
            break
        own -= middle_ref.shape[0]
    own = slice(own, own + STEP)
    blocks = [first, left_ref[at, 128:256]]
    blocks += [middle_ref[own, k : k + 128] for k in range(0, middle_ref.shape[1], 128)]
    blocks += [last]
    turned = [pltpu.roll(block, REACH, 1) for block in blocks]
    return [jnp.where(lane < REACH, a, b) for a, b in zip(turned[:-1], turned[1:])]


def finish_kernel(*refs, middles, scaled, following, totals):
    leaving = scaled and not following
    (left_ref,), middle_refs, (right_ref,), come, refs = take(refs, 1, middles, 1, 2)
    pieces = (left_ref, middle_refs, right_ref)
    totals_in, mass_in, density_out, refs = take(refs, 2 * scaled, following, scaled)
    adapted_out, refs = take(refs, 4 * following)
    if scaled:
        inverse = jnp.exp(-(totals_in[0][0:1, :] / totals_in[1][1:2, :]))
    staged, done = refs if leaving else (density_out[0] if scaled else None, None)
    rows = left_ref.shape[0]
    column_flags = flags_of("col")
    log_sum = jnp.zeros((8, 128), F32)
    mass_sum = jnp.zeros((8, 128), F32)
    copies = []
    for number, start in enumerate(range(0, rows, STEP)):
        at = slice(start, start + STEP)
        for k, block in enumerate(gathered(pieces, come, column_flags, start)):
            lanes = slice(k * 128, (k + 1) * 128)
            if scaled:
                block = block * inverse
                staged[at, lanes] = block
            if following:
                pilot = block + BACKGROUND
                mass = mass_in[0][at, lanes]
                adapted_out[0][at, lanes] = mass * pilot
                terms = mass * jnp.log(pilot)
                log_sum += jnp.sum(terms.reshape(STEP // 8, 8, 128), axis=0)
                if totals:
                    mass_sum += jnp.sum(mass.reshape(STEP // 8, 8, 128), axis=0)
        if leaving:
            copy = pltpu.make_async_copy(staged.at[at], density_out[0].at[at], done.at[number])
            copy.start()
            copies.append(copy)
    if following:
        adapted_ref, send_a, send_b, stat_ref = adapted_out
        odd_row = flags_of("row")[0]
        top, bottom = adapted_ref[0:REACH], adapted_ref[rows - REACH :]
        send_a[...] = chosen(odd_row, top, bottom)
        send_b[...] = chosen(odd_row, bottom, top)
        log_sum = jnp.sum(log_sum, axis=(0, 1), keepdims=True)
        mass_sum = jnp.sum(mass_sum, axis=(0, 1), keepdims=True)
        row = iota((8, 128), 0)
        stat_ref[...] = jnp.where(row == 0, log_sum, jnp.where(row == 1, mass_sum, 0.0))
    for copy in copies:
        copy.wait()


def exchange(first, second, axis):
    along = 0 if axis == "row" else 1
    sizes = [lax.axis_size("row"), lax.axis_size("col")]
    results = []
    for offset, value in ((0, first), (1, second)):
        pairs = []
        for index in range(sizes[0] * sizes[1]):
            place = [index // sizes[1], index % sizes[1]]
            own = place[along]
            partner = own + 1 if own % 2 == offset else own - 1
            if 0 <= partner < sizes[along]:
                place[along] = partner
            else:
                place[1 - along] ^= 1
            pairs.append((index, place[0] * sizes[1] + place[1]))
        results.append(lax.ppermute(value, ("row", "col"), pairs))
    return results


HOPS = (
    ("col", 2, 8),
    ("col", 6, 8),
    ("row", 12, 16),
    ("row", 4, 16),
    ("row", 3, 4),
    ("row", 1, 2),
    ("col", 1, 2),
)


def total_over(stat):
    for axis, hop, least in HOPS:
        if lax.axis_size(axis) >= least:
            pairs = [(i, i ^ hop) for i in range(lax.axis_size(axis))]
            stat = stat + lax.ppermute(stat, axis, pairs)
    return stat


def smooth(field, halo, labels, label_halo, tables, groups, cuts, leaving=()):
    high, low, rim = tables
    rows, columns = field.shape
    labelled = labels is not None
    bands = [c for group in groups for c in group]
    highs, lows, partials = [], [], []
    for number, group in enumerate(groups):
        inner = (len(group), rows - 2 * REACH, columns)
        edge = (len(group), 2 * REACH, columns)
        carried = len(leaving) if number == 0 else 0
        results = call(
            functools.partial(
                rows_kernel, bands=group, labelled=labelled, carried=carried
            ),
            [(inner, BF16), (inner, BF16), (edge, F32)] + [(field.shape, F32)] * carried,
            [field] + ([labels] if labelled else []) + [high, low, *leaving[:carried]],
            out_specs=[VMEM] * 3 + [HBM] * carried,
            scratch=[pltpu.SemaphoreType.DMA] * carried,
            flops=len(group) * 1_000_000_000,
        )
        if carried:
            left_behind = results[3]
        for results_of, result in zip((highs, lows, partials), results):
            results_of.append(result)
    edge = (len(bands), 2 * REACH, columns)
    edge_high, edge_low, left, right, send_a, send_b = call(
        functools.partial(edges_kernel, groups=groups, labelled=labelled),
        [(edge, BF16), (edge, BF16), ((rows, TILE), F32), ((rows, 128), F32)]
        + [((rows // 2, 128), F32)] * 2,
        [*halo, *(label_halo if labelled else ()), *partials, *highs, *lows]
        + [rim, high, low],
        flops=len(bands) * 500_000_000,
    )
    come = exchange(send_a, send_b, "col")
    middles = []
    start = 0
    for count in cuts:
        middles += call(
            functools.partial(middle_kernel, groups=groups, start=start),
            [((count, columns - TILE), F32)],
            [*highs, *lows, edge_high, edge_low, high, low],
            flops=len(bands) * 750_000_000 * count // rows,
        )
        start += count
    pieces = [left, *middles, right, *come]
    return (pieces, left_behind) if leaving else pieces


def finish(pieces, extra, scaled, following, totals, shape):
    plane, rim, stat = (shape, F32), ((REACH, shape[1]), F32), ((8, 128), F32)
    outs = [plane] * scaled + [plane, rim, rim, stat] * following
    scratch = []
    leaving = scaled and not following
    if leaving:
        scratch = [pltpu.VMEM(shape, F32), pltpu.SemaphoreType.DMA((shape[0] // STEP,))]
    return call(
        functools.partial(
            finish_kernel,
            middles=len(pieces) - 4,
            scaled=scaled,
            following=following,
            totals=totals,
        ),
        outs,
        [*pieces, *extra],
        out_specs=[HBM if leaving else VMEM] * scaled + [VMEM] * (4 * following),
        scratch=scratch,
        flops=500_000_000,
    )


def tables_of(count):
    return [
        ((count * BAND, TILE), BF16),
        ((count * BAND, TILE), BF16),
        ((count, 128, 384), BF16),
    ]


def body(counts, sample_weights, classes, class_radius):
    shape = rows, columns = counts.shape
    groups = ((0, 1), (2, 3))
    cuts = (rows - 192, 192)
    rim, slim = (REACH, columns), (PILOT_RADIUS, columns)
    counts, sample_weights, classes = (
        pltpu.with_memory_space_constraint(field, pltpu.HBM)
        for field in (counts, sample_weights, classes)
    )
    chunks = rows // CHUNK
    *pilot_tables, mass, mass_a, mass_b, label_a, label_b = call(
        prepare_kernel,
        tables_of(1)
        + [(shape, F32), (slim, F32), (slim, F32), (rim, jnp.int32), (rim, jnp.int32)],
        [counts, sample_weights, classes],
        ins=[HBM, HBM, HBM],
        scratch=[
            pltpu.VMEM(shape, jnp.int32),
            pltpu.VMEM(shape, F32),
            pltpu.VMEM((2, *rim), jnp.int32),
            pltpu.SemaphoreType.DMA((2, chunks)),
            pltpu.SemaphoreType.DMA((2,)),
        ],
        flops=500_000_000,
    )
    mass_halo = exchange(mass_a, mass_b, "row")
    label_halo = exchange(label_a, label_b, "row")
    *tables, labels = call(
        bands_kernel,
        tables_of(CLASSES) + [(shape, BF16)],
        [class_radius, classes],
        ins=[SMEM, HBM],
        scratch=[pltpu.VMEM(shape, jnp.int32), pltpu.SemaphoreType.DMA((chunks,))],
        flops=500_000_000,
    )
    pieces = smooth(mass, mass_halo, None, None, pilot_tables, ((0,),), (rows,))
    adapted, *sends, first_stat = finish(pieces, [mass], False, True, True, shape)
    halo = exchange(*sends, "row")
    first_total = total_over(first_stat)
    pieces = smooth(adapted, halo, labels, label_halo, tables, groups, cuts)
    density_first, adapted, *sends, second_stat = finish(
        pieces, [first_total, first_total, mass], True, True, False, shape
    )
    halo = exchange(*sends, "row")
    second_total = total_over(second_stat)
    pieces, density_first = smooth(
        adapted, halo, labels, label_halo, tables, groups, cuts, (density_first,)
    )
    (density_second,) = finish(
        pieces, [second_total, first_total], True, False, False, shape
    )
    return density_first, density_second


def solution(mesh):
    spec = P("row", "col")
    return jax.shard_map(
        body,
        mesh=mesh,
        in_specs=(spec, spec, spec, P()),
        out_specs=(spec, spec),
        check_vma=False,
    )
```

```python
import functools

import jax
import jax.numpy as jnp
from jax import lax
from jax.experimental import pallas as pl
from jax.experimental.pallas import tpu as pltpu
from jax.sharding import PartitionSpec as P


REACH = 64
PILOT_RADIUS = 32
CLASSES = 4
BACKGROUND = 0.5
TILE = 256
BAND = TILE + 2 * REACH
STEP = 64
F32 = jnp.float32
BF16 = jnp.bfloat16
MIB = 1 << 20
HBM = pl.BlockSpec(memory_space=pltpu.HBM)
VMEM = pl.BlockSpec(memory_space=pltpu.VMEM)
SMEM = pl.BlockSpec(memory_space=pltpu.SMEM)


def call(kernel, outs, args, ins=None, out_specs=None, scratch=(), limit=24, flops=100_000_000):
    return pl.pallas_call(
        kernel,
        out_shape=[jax.ShapeDtypeStruct(s, d) for s, d in outs],
        in_specs=ins or [VMEM] * len(args),
        out_specs=out_specs or [VMEM] * len(outs),
        scratch_shapes=scratch,
        compiler_params=pltpu.CompilerParams(vmem_limit_bytes=limit * MIB),
        cost_estimate=pl.CostEstimate(flops=flops, transcendentals=0, bytes_accessed=4 * MIB),
    )(*args)


def iota(shape, dim):
    return lax.broadcasted_iota(jnp.int32, shape, dim)


def split(value):
    high = value.astype(BF16)
    return high, (value - high.astype(F32)).astype(BF16)


def dot(a, b):
    return jnp.dot(a, b, preferred_element_type=F32)


def take(refs, *counts):
    groups = []
    for count in counts:
        groups.append(list(refs[:count]))
        refs = refs[count:]
    return *groups, list(refs)


def chosen(flag, when_set, when_clear):
    return jnp.where(flag > 0.5, when_set, when_clear)


def flags_of(axis):
    index = lax.axis_index(axis)
    last = lax.axis_size(axis) - 1
    values = (index & 1, jnp.minimum(index, 1), jnp.minimum(last - index, 1))
    return [jnp.full((1, 1), value.astype(F32), F32) for value in values]


def fill_bands(slot, radius, high_ref, low_ref, rim_ref):
    radius = jnp.full((1, 1), radius, F32)
    inverse = 1.0 / (2.0 * (0.5 * radius) * (0.5 * radius))

    def shape_of(d):
        return jnp.where(jnp.abs(d) <= radius, jnp.exp(-(d * d) * inverse), 0.0)

    lane = iota((8, 128), 1).astype(F32)
    tap = jnp.where(iota((8, 128), 0) == 0, jnp.where(lane == 0, 1.0, 2.0), 0.0)
    total = jnp.sum(shape_of(lane) * tap, axis=(0, 1), keepdims=True)
    column = iota((128, 128), 1)
    shift = iota((128, 128), 0) - column
    near = split(shape_of((shift - REACH).astype(F32)) / total)
    far = split(shape_of((shift + REACH).astype(F32)) / total)
    zero = jnp.zeros((128, 128), BF16)
    side = column[:REACH] < REACH
    zeros = jnp.zeros((REACH, 128), F32)
    base = slot * BAND
    for part, ref in enumerate((high_ref, low_ref)):
        blocks = ((near[part], zero), (far[part], near[part]), (zero, far[part]))
        for i, pair in enumerate(blocks):
            for k, block in enumerate(pair):
                lanes = slice(k * 128, (k + 1) * 128)
                ref[base + i * 128 : base + (i + 1) * 128, lanes] = block
        first = jnp.where(side, far[part][:REACH].astype(F32), zeros).astype(BF16)
        second = jnp.where(side, zeros, near[part][REACH:].astype(F32)).astype(BF16)
        for place in (0, 128) if part == 0 else (256,):
            rim_ref[slot, :REACH, place : place + 128] = first
            rim_ref[slot, REACH:, place : place + 128] = second


CHUNK = 128


def prepare_kernel(*refs):
    (counts_in, weights_in, classes_in), tables, outs, scratch = take(refs, 3, 3, 5)
    mass_ref, mass_a, mass_b, label_a, label_b = outs
    counts, weights, ends, arrived, ended = scratch
    rows = counts.shape[0]
    copies = []
    for n, start in enumerate(range(0, rows, CHUNK)):
        at = slice(start, start + CHUNK)
        pair = [
            pltpu.make_async_copy(counts_in.at[at], counts.at[at], arrived.at[0, n]),
            pltpu.make_async_copy(weights_in.at[at], weights.at[at], arrived.at[1, n]),
        ]
        for copy in pair:
            copy.start()
        copies.append((at, pair))
    end_copies = [
        pltpu.make_async_copy(classes_in.at[0:REACH], ends.at[0], ended.at[0]),
        pltpu.make_async_copy(classes_in.at[rows - REACH : rows], ends.at[1], ended.at[1]),
    ]
    for copy in end_copies:
        copy.start()
    fill_bands(0, F32(PILOT_RADIUS), *tables)
    for at, pair in copies:
        for copy in pair:
            copy.wait()
        mass_ref[at] = counts[at].astype(F32) * weights[at]
    odd = flags_of("row")[0]
    top, bottom = mass_ref[0:PILOT_RADIUS], mass_ref[rows - PILOT_RADIUS :]
    mass_a[...] = chosen(odd, top, bottom)
    mass_b[...] = chosen(odd, bottom, top)
    for copy in end_copies:
        copy.wait()
    label_a[...] = chosen(odd, ends[0], ends[1])
    label_b[...] = chosen(odd, ends[1], ends[0])


def bands_kernel(*refs):
    (radius_ref, classes_in), tables, (label_ref, classes, arrived) = take(refs, 2, 3)
    rows = classes.shape[0]
    copies = []
    for n, start in enumerate(range(0, rows, CHUNK)):
        at = slice(start, start + CHUNK)
        copy = pltpu.make_async_copy(classes_in.at[at], classes.at[at], arrived.at[n])
        copy.start()
        copies.append((at, copy))
    for c in range(CLASSES):
        fill_bands(c, radius_ref[c].astype(F32), *tables)
    for at, copy in copies:
        copy.wait()
        label_ref[at] = classes[at].astype(F32).astype(BF16)


def masked(pieces, labels, c):
    if labels is None:
        return pieces
    keep = labels == c
    return [jnp.where(keep, piece, jnp.zeros_like(piece)) for piece in pieces]


def rows_kernel(*refs, bands, labelled, carried):
    (field_ref,), label_refs, (band_high, band_low), plane, outs, plane_out, done = take(
        refs, 1, labelled, 2, carried, 3, carried
    )
    high_ref, low_ref, edge_ref = outs
    rows, columns = field_ref.shape
    copies = []
    for source, target, arrived in zip(plane, plane_out, done):
        for n, start in enumerate(range(0, rows, STEP)):
            at = slice(start, start + STEP)
            copies.append(pltpu.make_async_copy(source.at[at], target.at[at], arrived.at[n]))
    for copy in copies:
        copy.start()
    count = rows // REACH
    for n in range(columns // TILE):
        at = slice(n * TILE, (n + 1) * TILE)
        pieces = split(field_ref[:, at])
        labels = label_refs[0][:, at] if labelled else None
        for slot, c in enumerate(bands):
            high, low = masked(pieces, labels, c)
            sums = [None] * count

            def add(result, first):
                for i in range(result.shape[0] // REACH):
                    piece = result[i * REACH : (i + 1) * REACH]
                    own = sums[first + i]
                    sums[first + i] = piece if own is None else own + piece

            half = band_high[c * BAND : c * BAND + 2 * 128, 0:128]
            twice = jnp.concatenate([half, half], axis=1)
            for block in range(rows // 128):
                own = slice(block * 128, (block + 1) * 128)
                first = max(2 * block - 1, 0)
                last = min(2 * block + 3, count)
                taps = slice((first - 2 * block + 1) * REACH, (last - 2 * block + 1) * REACH)
                add(dot(twice[taps], jnp.concatenate([high[own], low[own]])), first)
            for tile in range(rows // TILE):
                own = slice(tile * TILE, (tile + 1) * TILE)
                first = max(4 * tile - 1, 0)
                last = min(4 * tile + 5, count)
                start = c * BAND + (first - 4 * tile + 1) * REACH
                taps = slice(start, start + (last - first) * REACH)
                add(dot(band_low[taps, :], high[own]), first)
            edge_ref[slot, 0:REACH, at] = sums[0]
            edge_ref[slot, REACH:, at] = sums[-1]
            for i, value in enumerate(sums[1:-1]):
                target = slice(i * REACH, (i + 1) * REACH)
                high_ref[slot, target, at], low_ref[slot, target, at] = split(value)
    for copy in copies:
        copy.wait()


def kept_row(start, rows):
    if start < REACH:
        return rows - 2 * REACH + start
    return start if start >= rows - REACH else start - REACH


def stacked_left(sides, inputs, start, stop, inner):
    refs, edge_ref = sides
    pieces = []
    slot = 0
    for ref in refs:
        for own in range(ref.shape[0]):
            rows = []
            if start < inner:
                rows.append(ref[own, start : min(stop, inner), inputs])
            if stop > inner:
                rows.append(edge_ref[slot, max(start, inner) - inner : stop - inner, inputs])
            pieces.append(rows[0] if len(rows) == 1 else jnp.concatenate(rows))
            slot += 1
    return jnp.concatenate(pieces, axis=1)


def swept(highs, lows, bands, band_refs, block, width, columns, start, stop, inner):
    high_ref, low_ref = band_refs

    def window(first, last):
        here, there = max(first, 0), min(last, columns)
        return slice(here, there), slice(here - first, there - first)

    def rights(refs_and_lanes, taps):
        return jnp.concatenate(
            [
                jnp.concatenate(
                    [ref[c * BAND + taps.start : c * BAND + taps.stop, lanes] for ref, lanes in refs_and_lanes],
                    axis=1,
                )
                for c in bands
            ]
        )

    results = []
    origin = block * TILE - 128
    for part in range(width // 128):
        inputs, taps = window(origin + part * 128, origin + (part + 2) * 128)
        left = stacked_left(highs, inputs, start, stop, inner)
        right = rights(((high_ref, slice(0, 128)), (low_ref, slice(0, 128))), taps)
        both = dot(left, right)
        results.append(both[:, :128] + both[:, 128:])
    inputs, taps = window(origin, origin + width + 128)
    left = stacked_left(lows, inputs, start, stop, inner)
    rest = dot(left, rights(((high_ref, slice(0, width)),), taps))
    return [value + rest[:, k * 128 : (k + 1) * 128] for k, value in enumerate(results)]


def edges_kernel(*refs, groups, labelled):
    count = len(groups)
    halo, labels_in, partials, highs, lows, (rim_ref, *band_refs), outs = take(
        refs, 2, 2 * labelled, count, count, count, 3
    )
    edge_high, edge_low, left_ref, right_ref, send_a, send_b = outs
    bands = [c for group in groups for c in group]
    sources = [(ref, own) for ref in partials for own in range(ref.shape[0])]
    columns = halo[0].shape[1]
    odd_row, has_top, has_bottom = flags_of("row")
    odd_column = flags_of("col")[0]
    for n in range(columns // TILE):
        at = slice(n * TILE, (n + 1) * TILE)

        def joined(pair):
            first, second = pair[0][:, at].astype(F32), pair[1][:, at].astype(F32)
            top = chosen(has_top, chosen(odd_row, first, second), 0.0)
            bottom = chosen(has_bottom, chosen(odd_row, second, first), 0.0)
            missing = REACH - first.shape[0]
            if missing:
                zeros = jnp.zeros((missing, TILE), F32)
                return jnp.concatenate([zeros, top, bottom, zeros])
            return jnp.concatenate([top, bottom])

        pieces = split(joined(halo))
        labels = joined(labels_in).astype(BF16) if labelled else None
        for slot, c in enumerate(bands):
            high, low = masked(pieces, labels, c)
            right = jnp.concatenate([high, low, high], axis=0)
            source, own = sources[slot]
            value = source[own, :, at] + dot(rim_ref[c], right)
            edge_high[slot, :, at], edge_low[slot, :, at] = split(value)
    rows = left_ref.shape[0]
    inner = rows - 2 * REACH
    for target, block in ((left_ref, 0), (right_ref, columns // TILE)):
        results = swept(
            (highs, edge_high),
            (lows, edge_low),
            bands,
            band_refs,
            block,
            target.shape[1],
            columns,
            0,
            rows,
            inner,
        )
        for k, value in enumerate(results):
            target[:, k * 128 : (k + 1) * 128] = value
    half = rows // 2
    lower = iota((half, 128), 1) < REACH
    left = left_ref[:, 0:128]
    left = jnp.where(lower, left[:half], pltpu.roll(left[half:], REACH, 1))
    right = right_ref[...]
    right = jnp.where(lower, pltpu.roll(right[:half], REACH, 1), right[half:])
    send_a[...] = chosen(odd_column, left, right)
    send_b[...] = chosen(odd_column, right, left)


def middle_kernel(*refs, groups, start):
    count = len(groups)
    highs, lows, (edge_high, edge_low), band_refs, (out_ref,) = take(refs, count, count, 2, 2)
    bands = [c for group in groups for c in group]
    inner = highs[0].shape[1]
    for j in range(out_ref.shape[1] // TILE):
        results = swept(
            (highs, edge_high),
            (lows, edge_low),
            bands,
            band_refs,
            j + 1,
            TILE,
            edge_high.shape[2],
            start,
            start + out_ref.shape[0],
            inner,
        )
        for k, value in enumerate(results):
            out_ref[:, j * TILE + k * 128 : j * TILE + (k + 1) * 128] = value


FINE = 16


def gathered(pieces, come, flags, start):
    left_ref, middles, right_ref = pieces
    odd, has_left, has_right = flags
    rows = left_ref.shape[0]
    half = rows // 2
    kept = kept_row(start, rows)
    at = slice(kept, kept + FINE)
    lane = iota((FINE, 128), 1)
    local = slice(kept % half, kept % half + FINE)
    come_left = chosen(has_left, chosen(odd, come[0][local], come[1][local]), 0.0)
    come_right = chosen(has_right, chosen(odd, come[1][local], come[0][local]), 0.0)
    if kept < half:
        come_left = pltpu.roll(come_left, REACH, 1)
    else:
        come_right = pltpu.roll(come_right, REACH, 1)
    first = left_ref[at, 0:128] + jnp.where(lane >= REACH, come_left, 0.0)
    last = right_ref[at, :] + jnp.where(lane < REACH, come_right, 0.0)
    own = kept
    for middle_ref in middles:
        if own < middle_ref.shape[0]:
            break
        own -= middle_ref.shape[0]
    own = slice(own, own + FINE)

    def block_of(k):
        if k == 0:
            return first
        if k == 1:
            return left_ref[at, 128:256]
        if k * 128 < TILE + middle_ref.shape[1]:
            return middle_ref[own, k * 128 - TILE : (k + 1) * 128 - TILE]
        return last

    before = pltpu.roll(block_of(0), REACH, 1)
    for k in range((TILE + middle_ref.shape[1]) // 128):
        after = pltpu.roll(block_of(k + 1), REACH, 1)
        yield jnp.where(lane < REACH, before, after)
        before = after


def finish_kernel(*refs, middles, scaled, following, totals):
    leaving = scaled and not following
    (left_ref,), middle_refs, (right_ref,), come, refs = take(refs, 1, middles, 1, 2)
    pieces = (left_ref, middle_refs, right_ref)
    totals_in, mass_in, density_out, refs = take(refs, 2 * scaled, following, scaled)
    adapted_out, refs = take(refs, 4 * following)
    if scaled:
        inverse = jnp.exp(-(totals_in[0][0:1, :] / totals_in[1][1:2, :]))
    staged, done = refs if leaving else (density_out[0] if scaled else None, None)
    rows = left_ref.shape[0]
    column_flags = flags_of("col")
    columns = TILE + middle_refs[0].shape[1]
    log_sums = [jnp.zeros((8, 128), F32)] * (columns // 128)
    mass_sums = [jnp.zeros((8, 128), F32)] * (columns // 128)
    if following:
        odd_row = flags_of("row")[0]
        adapted_ref, send_a, send_b, stat_ref = adapted_out
    copies = []
    for start in range(0, rows, FINE):
        at = slice(start, start + FINE)
        for k, block in enumerate(gathered(pieces, come, column_flags, start)):
            lanes = slice(k * 128, (k + 1) * 128)
            if scaled:
                block = block * inverse
                staged[at, lanes] = block
            if following:
                pilot = block + BACKGROUND
                mass = mass_in[0][at, lanes]
                adapted_ref[at, lanes] = mass * pilot
                terms = mass * jnp.log(pilot)
                for i in range(0, FINE, 8):
                    log_sums[k] = log_sums[k] + terms[i : i + 8]
                    if totals:
                        mass_sums[k] = mass_sums[k] + mass[i : i + 8]
        if leaving and (start + FINE) % STEP == 0:
            at = slice(start + FINE - STEP, start + FINE)
            copy = pltpu.make_async_copy(
                staged.at[at], density_out[0].at[at], done.at[start // STEP]
            )
            copy.start()
            copies.append(copy)
    if following:
        top, bottom = adapted_ref[0:REACH], adapted_ref[rows - REACH :]
        send_a[...] = chosen(odd_row, top, bottom)
        send_b[...] = chosen(odd_row, bottom, top)
        log_sum = jnp.sum(sum(log_sums), axis=(0, 1), keepdims=True)
        mass_sum = jnp.sum(sum(mass_sums), axis=(0, 1), keepdims=True)
        row = iota((8, 128), 0)
        stat_ref[...] = jnp.where(row == 0, log_sum, jnp.where(row == 1, mass_sum, 0.0))
    for copy in copies:
        copy.wait()


def exchange(first, second, axis):
    along = 0 if axis == "row" else 1
    sizes = [lax.axis_size("row"), lax.axis_size("col")]
    results = []
    for offset, value in ((0, first), (1, second)):
        pairs = []
        for index in range(sizes[0] * sizes[1]):
            place = [index // sizes[1], index % sizes[1]]
            own = place[along]
            partner = own + 1 if own % 2 == offset else own - 1
            if 0 <= partner < sizes[along]:
                place[along] = partner
            else:
                place[1 - along] ^= 1
            pairs.append((index, place[0] * sizes[1] + place[1]))
        results.append(lax.ppermute(value, ("row", "col"), pairs))
    return results


HOPS = (
    (0, 3, (1, 8)),
    (0, 7, (1, 8)),
    (12, 1, (16, 1)),
    (4, 1, (16, 1)),
    (3, 1, (4, 1)),
    (1, 1, (2, 1)),
    (0, 1, (1, 2)),
)


def total_over(stat):
    sizes = (lax.axis_size("row"), lax.axis_size("col"))
    for rows, columns, least in HOPS:
        if sizes[0] >= least[0] and sizes[1] >= least[1]:
            pairs = []
            for index in range(sizes[0] * sizes[1]):
                row, column = divmod(index, sizes[1])
                pairs.append((index, (row ^ rows) * sizes[1] + (column ^ columns)))
            stat = stat + lax.ppermute(stat, ("row", "col"), pairs)
    return stat


def smooth(field, halo, labels, label_halo, tables, groups, cuts, leaving=()):
    high, low, rim = tables
    rows, columns = field.shape
    labelled = labels is not None
    bands = [c for group in groups for c in group]
    highs, lows, partials = [], [], []
    for number, group in enumerate(groups):
        inner = (len(group), rows - 2 * REACH, columns)
        edge = (len(group), 2 * REACH, columns)
        carried = len(leaving) if number == 0 else 0
        results = call(
            functools.partial(
                rows_kernel, bands=group, labelled=labelled, carried=carried
            ),
            [(inner, BF16), (inner, BF16), (edge, F32)] + [(field.shape, F32)] * carried,
            [field] + ([labels] if labelled else []) + [high, low, *leaving[:carried]],
            out_specs=[VMEM] * 3 + [HBM] * carried,
            scratch=[pltpu.SemaphoreType.DMA((rows // STEP,))] * carried,
            flops=len(group) * 1_000_000_000,
        )
        if carried:
            left_behind = results[3]
        for results_of, result in zip((highs, lows, partials), results):
            results_of.append(result)
    edge = (len(bands), 2 * REACH, columns)
    edge_high, edge_low, left, right, send_a, send_b = call(
        functools.partial(edges_kernel, groups=groups, labelled=labelled),
        [(edge, BF16), (edge, BF16), ((rows, TILE), F32), ((rows, 128), F32)]
        + [((rows // 2, 128), F32)] * 2,
        [*halo, *(label_halo if labelled else ()), *partials, *highs, *lows]
        + [rim, high, low],
        flops=len(bands) * 500_000_000,
    )
    come = exchange(send_a, send_b, "col")
    middles = []
    start = 0
    for count in cuts:
        middles += call(
            functools.partial(middle_kernel, groups=groups, start=start),
            [((count, columns - TILE), F32)],
            [*highs, *lows, edge_high, edge_low, high, low],
            flops=len(bands) * 750_000_000 * count // rows,
        )
        start += count
    pieces = [left, *middles, right, *come]
    return (pieces, left_behind) if leaving else pieces


def finish(pieces, extra, scaled, following, totals, shape):
    plane, rim, stat = (shape, F32), ((REACH, shape[1]), F32), ((8, 128), F32)
    outs = [plane] * scaled + [plane, rim, rim, stat] * following
    scratch = []
    leaving = scaled and not following
    if leaving:
        scratch = [pltpu.VMEM(shape, F32), pltpu.SemaphoreType.DMA((shape[0] // STEP,))]
    return call(
        functools.partial(
            finish_kernel,
            middles=len(pieces) - 4,
            scaled=scaled,
            following=following,
            totals=totals,
        ),
        outs,
        [*pieces, *extra],
        out_specs=[HBM if leaving else VMEM] * scaled + [VMEM] * (4 * following),
        scratch=scratch,
        flops=500_000_000,
    )


def tables_of(count):
    return [
        ((count * BAND, TILE), BF16),
        ((count * BAND, TILE), BF16),
        ((count, 128, 384), BF16),
    ]


def body(counts, sample_weights, classes, class_radius):
    shape = rows, columns = counts.shape
    groups = ((0, 1), (2, 3))
    cuts = (rows - 192, 192)
    rim, slim = (REACH, columns), (PILOT_RADIUS, columns)
    counts, sample_weights, classes = (
        pltpu.with_memory_space_constraint(field, pltpu.HBM)
        for field in (counts, sample_weights, classes)
    )
    chunks = rows // CHUNK
    *pilot_tables, mass, mass_a, mass_b, label_a, label_b = call(
        prepare_kernel,
        tables_of(1)
        + [(shape, F32), (slim, F32), (slim, F32), (rim, jnp.int32), (rim, jnp.int32)],
        [counts, sample_weights, classes],
        ins=[HBM, HBM, HBM],
        scratch=[
            pltpu.VMEM(shape, jnp.int32),
            pltpu.VMEM(shape, F32),
            pltpu.VMEM((2, *rim), jnp.int32),
            pltpu.SemaphoreType.DMA((2, chunks)),
            pltpu.SemaphoreType.DMA((2,)),
        ],
        flops=500_000_000,
    )
    mass_halo = exchange(mass_a, mass_b, "row")
    label_halo = exchange(label_a, label_b, "row")
    *tables, labels = call(
        bands_kernel,
        tables_of(CLASSES) + [(shape, BF16)],
        [class_radius, classes],
        ins=[SMEM, HBM],
        scratch=[pltpu.VMEM(shape, jnp.int32), pltpu.SemaphoreType.DMA((chunks,))],
        flops=500_000_000,
    )
    pieces = smooth(mass, mass_halo, None, None, pilot_tables, ((0,),), (rows,))
    adapted, *sends, first_stat = finish(pieces, [mass], False, True, True, shape)
    halo = exchange(*sends, "row")
    first_total = total_over(first_stat)
    pieces = smooth(adapted, halo, labels, label_halo, tables, groups, cuts)
    density_first, adapted, *sends, second_stat = finish(
        pieces, [first_total, first_total, mass], True, True, False, shape
    )
    halo = exchange(*sends, "row")
    second_total = total_over(second_stat)
    pieces, density_first = smooth(
        adapted, halo, labels, label_halo, tables, groups, cuts, (density_first,)
    )
    (density_second,) = finish(
        pieces, [second_total, first_total], True, False, False, shape
    )
    return density_first, density_second


def solution(mesh):
    spec = P("row", "col")
    return jax.shard_map(
        body,
        mesh=mesh,
        in_specs=(spec, spec, spec, P()),
        out_specs=(spec, spec),
        check_vma=False,
    )
```

```python
import functools

import jax
import jax.numpy as jnp
from jax import lax
from jax.experimental import pallas as pl
from jax.experimental.pallas import tpu as pltpu
from jax.sharding import PartitionSpec as P


REACH = 64
PILOT_RADIUS = 32
CLASSES = 4
BACKGROUND = 0.5
TILE = 256
BAND = TILE + 2 * REACH
STEP = 64
F32 = jnp.float32
BF16 = jnp.bfloat16
MIB = 1 << 20
HBM = pl.BlockSpec(memory_space=pltpu.HBM)
VMEM = pl.BlockSpec(memory_space=pltpu.VMEM)
SMEM = pl.BlockSpec(memory_space=pltpu.SMEM)


def call(
    kernel, outs, args, ins=None, out_specs=None, scratch=(), limit=24, flops=0, aliases=None
):
    return pl.pallas_call(
        kernel,
        out_shape=[jax.ShapeDtypeStruct(s, d) for s, d in outs],
        input_output_aliases=aliases or {},
        in_specs=ins or [VMEM] * len(args),
        out_specs=out_specs or [VMEM] * len(outs),
        scratch_shapes=scratch,
        compiler_params=pltpu.CompilerParams(vmem_limit_bytes=limit * MIB),
        cost_estimate=pl.CostEstimate(flops=flops, transcendentals=0, bytes_accessed=4 * MIB),
    )(*args)


def iota(shape, dim):
    return lax.broadcasted_iota(jnp.int32, shape, dim)


def split(value):
    high = value.astype(BF16)
    return high, (value - high.astype(F32)).astype(BF16)


def dot(a, b):
    return jnp.dot(a, b, preferred_element_type=F32)


def take(refs, *counts):
    groups = []
    for count in counts:
        groups.append(list(refs[:count]))
        refs = refs[count:]
    return *groups, list(refs)


def chosen(flag, when_set, when_clear):
    return jnp.where(flag > 0.5, when_set, when_clear)


def flags_of(axis):
    index = lax.axis_index(axis)
    last = lax.axis_size(axis) - 1
    values = (index & 1, jnp.minimum(index, 1), jnp.minimum(last - index, 1))
    return [jnp.full((1, 1), value.astype(F32), F32) for value in values]


def fill_bands(slot, radius, high_ref, low_ref, rim_ref):
    radius = jnp.full((1, 1), radius, F32)
    inverse = 1.0 / (2.0 * (0.5 * radius) * (0.5 * radius))

    def shape_of(d):
        return jnp.where(jnp.abs(d) <= radius, jnp.exp(-(d * d) * inverse), 0.0)

    lane = iota((8, 128), 1).astype(F32)
    tap = jnp.where(iota((8, 128), 0) == 0, jnp.where(lane == 0, 1.0, 2.0), 0.0)
    total = jnp.sum(shape_of(lane) * tap, axis=(0, 1), keepdims=True)
    column = iota((128, 128), 1)
    shift = iota((128, 128), 0) - column
    near = split(shape_of((shift - REACH).astype(F32)) / total)
    far = split(shape_of((shift + REACH).astype(F32)) / total)
    zero = jnp.zeros((128, 128), BF16)
    side = column[:REACH] < REACH
    zeros = jnp.zeros((REACH, 128), F32)
    base = slot * BAND
    for part, ref in enumerate((high_ref, low_ref)):
        blocks = ((near[part], zero), (far[part], near[part]), (zero, far[part]))
        for i, pair in enumerate(blocks):
            for k, block in enumerate(pair):
                lanes = slice(k * 128, (k + 1) * 128)
                ref[base + i * 128 : base + (i + 1) * 128, lanes] = block
        first = jnp.where(side, far[part][:REACH].astype(F32), zeros).astype(BF16)
        second = jnp.where(side, zeros, near[part][REACH:].astype(F32)).astype(BF16)
        for place in (0, 128) if part == 0 else (256,):
            rim_ref[slot, :REACH, place : place + 128] = first
            rim_ref[slot, REACH:, place : place + 128] = second


CHUNK = 128


def prepare_kernel(*refs):
    (counts_in, weights_in, classes_in), tables, outs, scratch = take(refs, 3, 3, 5)
    mass_ref, mass_a, mass_b, label_a, label_b = outs
    counts, weights, ends, arrived, ended = scratch
    rows = counts.shape[0]
    copies = []
    for n, start in enumerate(range(0, rows, CHUNK)):
        at = slice(start, start + CHUNK)
        pair = [
            pltpu.make_async_copy(counts_in.at[at], counts.at[at], arrived.at[0, n]),
            pltpu.make_async_copy(weights_in.at[at], weights.at[at], arrived.at[1, n]),
        ]
        for copy in pair:
            copy.start()
        copies.append((at, pair))
    end_copies = [
        pltpu.make_async_copy(classes_in.at[0:REACH], ends.at[0], ended.at[0]),
        pltpu.make_async_copy(classes_in.at[rows - REACH : rows], ends.at[1], ended.at[1]),
    ]
    for copy in end_copies:
        copy.start()
    fill_bands(0, F32(PILOT_RADIUS), *tables)
    for at, pair in copies:
        for copy in pair:
            copy.wait()
        mass_ref[at] = counts[at].astype(F32) * weights[at]
    odd = flags_of("row")[0]
    top, bottom = mass_ref[0:PILOT_RADIUS], mass_ref[rows - PILOT_RADIUS :]
    mass_a[...] = chosen(odd, top, bottom)
    mass_b[...] = chosen(odd, bottom, top)
    for copy in end_copies:
        copy.wait()
    label_a[...] = chosen(odd, ends[0], ends[1])
    label_b[...] = chosen(odd, ends[1], ends[0])


def bands_kernel(*refs):
    (radius_ref, classes_in), tables, (label_ref, classes, arrived) = take(refs, 2, 3)
    rows = classes.shape[0]
    copies = []
    for n, start in enumerate(range(0, rows, CHUNK)):
        at = slice(start, start + CHUNK)
        copy = pltpu.make_async_copy(classes_in.at[at], classes.at[at], arrived.at[n])
        copy.start()
        copies.append((at, copy))
    for c in range(CLASSES):
        fill_bands(c, radius_ref[c].astype(F32), *tables)
    for at, copy in copies:
        copy.wait()
        label_ref[at] = classes[at].astype(F32).astype(BF16)


def masked(pieces, labels, c):
    if labels is None:
        return pieces
    keep = labels == c
    return [jnp.where(keep, piece, jnp.zeros_like(piece)) for piece in pieces]


def rows_kernel(*refs, bands, labelled, leaving):
    (field_ref,), label_refs, (band_high, band_low), plane, outs, sent = take(
        refs, 1, labelled, 2, (1 + (leaving[0] > 0)) if leaving else 0, 3
    )
    high_ref, low_ref, edge_ref = outs
    rows, columns = field_ref.shape
    copies = []
    if leaving:
        target, done = sent
        for n, start in enumerate(range(*leaving, STEP)):
            at = slice(start, start + STEP)
            copies.append(pltpu.make_async_copy(plane[0].at[at], target.at[at], done.at[n]))
    for copy in copies:
        copy.start()
    count = rows // REACH
    for n in range(columns // TILE):
        at = slice(n * TILE, (n + 1) * TILE)
        pieces = split(field_ref[:, at])
        labels = label_refs[0][:, at] if labelled else None
        for slot, c in enumerate(bands):
            high, low = masked(pieces, labels, c)
            sums = [None] * count

            def add(result, first):
                for i in range(result.shape[0] // REACH):
                    piece = result[i * REACH : (i + 1) * REACH]
                    own = sums[first + i]
                    sums[first + i] = piece if own is None else own + piece

            half = band_high[c * BAND : c * BAND + 2 * 128, 0:128]
            twice = jnp.concatenate([half, half], axis=1)
            for block in range(rows // 128):
                own = slice(block * 128, (block + 1) * 128)
                first = max(2 * block - 1, 0)
                last = min(2 * block + 3, count)
                taps = slice((first - 2 * block + 1) * REACH, (last - 2 * block + 1) * REACH)
                add(dot(twice[taps], jnp.concatenate([high[own], low[own]])), first)
            for tile in range(rows // TILE):
                own = slice(tile * TILE, (tile + 1) * TILE)
                first = max(4 * tile - 1, 0)
                last = min(4 * tile + 5, count)
                start = c * BAND + (first - 4 * tile + 1) * REACH
                taps = slice(start, start + (last - first) * REACH)
                add(dot(band_low[taps, :], high[own]), first)
            edge_ref[slot, 0:REACH, at] = sums[0]
            edge_ref[slot, REACH:, at] = sums[-1]
            for i, value in enumerate(sums[1:-1]):
                target = slice(i * REACH, (i + 1) * REACH)
                high_ref[slot, target, at], low_ref[slot, target, at] = split(value)
    for copy in copies:
        copy.wait()


def kept_row(start, rows):
    if start < REACH:
        return rows - 2 * REACH + start
    return start if start >= rows - REACH else start - REACH


def stacked_left(sides, inputs, start, stop, inner):
    refs, edge_ref = sides
    pieces = []
    slot = 0
    for ref in refs:
        for own in range(ref.shape[0]):
            rows = []
            if start < inner:
                rows.append(ref[own, start : min(stop, inner), inputs])
            if stop > inner:
                rows.append(edge_ref[slot, max(start, inner) - inner : stop - inner, inputs])
            pieces.append(rows[0] if len(rows) == 1 else jnp.concatenate(rows))
            slot += 1
    return jnp.concatenate(pieces, axis=1)


def swept(highs, lows, bands, band_refs, block, width, columns, start, stop, inner):
    high_ref, low_ref = band_refs

    def window(first, last):
        here, there = max(first, 0), min(last, columns)
        return slice(here, there), slice(here - first, there - first)

    def rights(refs_and_lanes, taps):
        return jnp.concatenate(
            [
                jnp.concatenate(
                    [ref[c * BAND + taps.start : c * BAND + taps.stop, lanes] for ref, lanes in refs_and_lanes],
                    axis=1,
                )
                for c in bands
            ]
        )

    results = []
    origin = block * TILE - 128
    for part in range(width // 128):
        inputs, taps = window(origin + part * 128, origin + (part + 2) * 128)
        left = stacked_left(highs, inputs, start, stop, inner)
        right = rights(((high_ref, slice(0, 128)), (low_ref, slice(0, 128))), taps)
        both = dot(left, right)
        results.append(both[:, :128] + both[:, 128:])
    inputs, taps = window(origin, origin + width + 128)
    left = stacked_left(lows, inputs, start, stop, inner)
    rest = dot(left, rights(((high_ref, slice(0, width)),), taps))
    return [value + rest[:, k * 128 : (k + 1) * 128] for k, value in enumerate(results)]


def edges_kernel(*refs, groups, labelled):
    count = len(groups)
    halo, labels_in, partials, highs, lows, (rim_ref, *band_refs), outs = take(
        refs, 2, 2 * labelled, count, count, count, 3
    )
    edge_high, edge_low, left_ref, right_ref, send_a, send_b = outs
    bands = [c for group in groups for c in group]
    sources = [(ref, own) for ref in partials for own in range(ref.shape[0])]
    columns = halo[0].shape[1]
    odd_row, has_top, has_bottom = flags_of("row")
    odd_column = flags_of("col")[0]
    for n in range(columns // TILE):
        at = slice(n * TILE, (n + 1) * TILE)

        def joined(pair):
            first, second = pair[0][:, at].astype(F32), pair[1][:, at].astype(F32)
            top = chosen(has_top, chosen(odd_row, first, second), 0.0)
            bottom = chosen(has_bottom, chosen(odd_row, second, first), 0.0)
            missing = REACH - first.shape[0]
            if missing:
                zeros = jnp.zeros((missing, TILE), F32)
                return jnp.concatenate([zeros, top, bottom, zeros])
            return jnp.concatenate([top, bottom])

        pieces = split(joined(halo))
        labels = joined(labels_in).astype(BF16) if labelled else None
        for slot, c in enumerate(bands):
            high, low = masked(pieces, labels, c)
            right = jnp.concatenate([high, low, high], axis=0)
            source, own = sources[slot]
            value = source[own, :, at] + dot(rim_ref[c], right)
            edge_high[slot, :, at], edge_low[slot, :, at] = split(value)
    rows = left_ref.shape[0]
    inner = rows - 2 * REACH
    for target, block in ((left_ref, 0), (right_ref, columns // TILE)):
        results = swept(
            (highs, edge_high),
            (lows, edge_low),
            bands,
            band_refs,
            block,
            target.shape[1],
            columns,
            0,
            rows,
            inner,
        )
        for k, value in enumerate(results):
            target[:, k * 128 : (k + 1) * 128] = value
    half = rows // 2
    lower = iota((half, 128), 1) < REACH
    left = left_ref[:, 0:128]
    left = jnp.where(lower, left[:half], pltpu.roll(left[half:], REACH, 1))
    right = right_ref[...]
    right = jnp.where(lower, pltpu.roll(right[:half], REACH, 1), right[half:])
    send_a[...] = chosen(odd_column, left, right)
    send_b[...] = chosen(odd_column, right, left)


def middle_kernel(*refs, groups, start):
    count = len(groups)
    highs, lows, (edge_high, edge_low), band_refs, (out_ref,) = take(refs, count, count, 2, 2)
    bands = [c for group in groups for c in group]
    inner = highs[0].shape[1]
    for j in range(out_ref.shape[1] // TILE):
        results = swept(
            (highs, edge_high),
            (lows, edge_low),
            bands,
            band_refs,
            j + 1,
            TILE,
            edge_high.shape[2],
            start,
            start + out_ref.shape[0],
            inner,
        )
        for k, value in enumerate(results):
            out_ref[:, j * TILE + k * 128 : j * TILE + (k + 1) * 128] = value


def gathered(pieces, come, flags, start):
    left_ref, middles, right_ref = pieces
    odd, has_left, has_right = flags
    rows = left_ref.shape[0]
    half = rows // 2
    kept = kept_row(start, rows)
    at = slice(kept, kept + STEP)
    lane = iota((STEP, 128), 1)
    local = slice(kept % half, kept % half + STEP)
    come_left = chosen(has_left, chosen(odd, come[0][local], come[1][local]), 0.0)
    come_right = chosen(has_right, chosen(odd, come[1][local], come[0][local]), 0.0)
    if kept < half:
        come_left = pltpu.roll(come_left, REACH, 1)
    else:
        come_right = pltpu.roll(come_right, REACH, 1)
    first = left_ref[at, 0:128] + jnp.where(lane >= REACH, come_left, 0.0)
    last = right_ref[at, :] + jnp.where(lane < REACH, come_right, 0.0)
    own = kept
    for middle_ref in middles:
        if own < middle_ref.shape[0]:
            break
        own -= middle_ref.shape[0]
    own = slice(own, own + STEP)
    blocks = [first, left_ref[at, 128:256]]
    blocks += [middle_ref[own, k : k + 128] for k in range(0, middle_ref.shape[1], 128)]
    blocks += [last]
    turned = [pltpu.roll(block, REACH, 1) for block in blocks]
    return [jnp.where(lane < REACH, a, b) for a, b in zip(turned[:-1], turned[1:])]


def finish_kernel(*refs, middles, scaled, following, totals):
    leaving = scaled and not following
    (left_ref,), middle_refs, (right_ref,), come, refs = take(refs, 1, middles, 1, 2)
    pieces = (left_ref, middle_refs, right_ref)
    totals_in, mass_in, density_out, refs = take(refs, 2 * scaled, following, scaled)
    adapted_out, refs = take(refs, 4 * following)
    if scaled:
        inverse = jnp.exp(-(totals_in[0][0:1, :] / totals_in[1][1:2, :]))
    staged, done = refs if leaving else (density_out[0] if scaled else None, None)
    rows = left_ref.shape[0]
    column_flags = flags_of("col")
    spans = (TILE + middle_refs[0].shape[1]) // 128
    log_sums = [jnp.zeros((8, 128), F32)] * spans
    mass_sums = [jnp.zeros((8, 128), F32)] * spans
    copies = []
    for number, start in enumerate(range(0, rows, STEP)):
        at = slice(start, start + STEP)
        for k, block in enumerate(gathered(pieces, come, column_flags, start)):
            lanes = slice(k * 128, (k + 1) * 128)
            if scaled:
                block = block * inverse
                staged[at, lanes] = block
            if following:
                pilot = block + BACKGROUND
                mass = mass_in[0][at, lanes]
                adapted_out[0][at, lanes] = mass * pilot
                terms = mass * jnp.log(pilot)
                log_sums[k] += jnp.sum(terms.reshape(STEP // 8, 8, 128), axis=0)
                if totals:
                    mass_sums[k] += jnp.sum(mass.reshape(STEP // 8, 8, 128), axis=0)
        if leaving:
            copy = pltpu.make_async_copy(staged.at[at], density_out[0].at[at], done.at[number])
            copy.start()
            copies.append(copy)
    if following:
        adapted_ref, send_a, send_b, stat_ref = adapted_out
        odd_row = flags_of("row")[0]
        top, bottom = adapted_ref[0:REACH], adapted_ref[rows - REACH :]
        send_a[...] = chosen(odd_row, top, bottom)
        send_b[...] = chosen(odd_row, bottom, top)
        log_sum = jnp.sum(sum(log_sums), axis=(0, 1), keepdims=True)
        mass_sum = jnp.sum(sum(mass_sums), axis=(0, 1), keepdims=True)
        row = iota((8, 128), 0)
        stat_ref[...] = jnp.where(row == 0, log_sum, jnp.where(row == 1, mass_sum, 0.0))
    for copy in copies:
        copy.wait()


def exchange(first, second, axis):
    along = 0 if axis == "row" else 1
    sizes = [lax.axis_size("row"), lax.axis_size("col")]
    results = []
    for offset, value in ((0, first), (1, second)):
        pairs = []
        for index in range(sizes[0] * sizes[1]):
            place = [index // sizes[1], index % sizes[1]]
            own = place[along]
            partner = own + 1 if own % 2 == offset else own - 1
            if 0 <= partner < sizes[along]:
                place[along] = partner
            else:
                place[1 - along] ^= 1
            pairs.append((index, place[0] * sizes[1] + place[1]))
        results.append(lax.ppermute(value, ("row", "col"), pairs))
    return results


HOPS = (
    (0, 3, (1, 8)),
    (0, 7, (1, 8)),
    (12, 1, (16, 1)),
    (4, 1, (16, 1)),
    (3, 1, (4, 1)),
    (1, 1, (2, 1)),
    (0, 1, (1, 2)),
)


def total_over(stat):
    sizes = (lax.axis_size("row"), lax.axis_size("col"))
    for rows, columns, least in HOPS:
        if sizes[0] >= least[0] and sizes[1] >= least[1]:
            pairs = []
            for index in range(sizes[0] * sizes[1]):
                row, column = divmod(index, sizes[1])
                pairs.append((index, (row ^ rows) * sizes[1] + (column ^ columns)))
            stat = stat + lax.ppermute(stat, ("row", "col"), pairs)
    return stat


def smooth(field, halo, labels, label_halo, tables, groups, cuts, plane=None):
    high, low, rim = tables
    rows, columns = field.shape
    labelled = labels is not None
    bands = [c for group in groups for c in group]
    highs, lows, partials = [], [], []
    for number, group in enumerate(groups):
        inner = (len(group), rows - 2 * REACH, columns)
        edge = (len(group), 2 * REACH, columns)
        args = [field] + ([labels] if labelled else []) + [high, low]
        outs = [(inner, BF16), (inner, BF16), (edge, F32)]
        ins, out_specs = [VMEM] * len(args), [VMEM] * len(outs)
        leaving, scratch, aliases = None, [], {}
        if plane is not None:
            part = rows // len(groups)
            leaving = (number * part, (number + 1) * part)
            args, ins = [*args, plane], [*ins, VMEM]
            if number > 0:
                aliases = {len(args): len(outs)}
                args, ins = [*args, plane_out], [*ins, HBM]
            outs, out_specs = [*outs, (field.shape, F32)], [*out_specs, HBM]
            scratch = [pltpu.SemaphoreType.DMA((part // STEP,))]
        results = call(
            functools.partial(rows_kernel, bands=group, labelled=labelled, leaving=leaving),
            outs,
            args,
            ins=ins,
            out_specs=out_specs,
            scratch=scratch,
            flops=len(group) * 1_000_000_000,
            aliases=aliases,
        )
        if plane is not None:
            plane_out = results[3]
        for results_of, result in zip((highs, lows, partials), results):
            results_of.append(result)
    edge = (len(bands), 2 * REACH, columns)
    edge_high, edge_low, left, right, send_a, send_b = call(
        functools.partial(edges_kernel, groups=groups, labelled=labelled),
        [(edge, BF16), (edge, BF16), ((rows, TILE), F32), ((rows, 128), F32)]
        + [((rows // 2, 128), F32)] * 2,
        [*halo, *(label_halo if labelled else ()), *partials, *highs, *lows]
        + [rim, high, low],
        flops=len(bands) * 500_000_000,
    )
    come = exchange(send_a, send_b, "col")
    middles = []
    start = 0
    for count in cuts:
        middles += call(
            functools.partial(middle_kernel, groups=groups, start=start),
            [((count, columns - TILE), F32)],
            [*highs, *lows, edge_high, edge_low, high, low],
            flops=len(bands) * 750_000_000 * count // rows,
        )
        start += count
    pieces = [left, *middles, right, *come]
    return pieces if plane is None else (pieces, plane_out)


def finish(pieces, extra, scaled, following, totals, shape):
    plane, rim, stat = (shape, F32), ((REACH, shape[1]), F32), ((8, 128), F32)
    outs = [plane] * scaled + [plane, rim, rim, stat] * following
    scratch = []
    leaving = scaled and not following
    if leaving:
        scratch = [pltpu.VMEM(shape, F32), pltpu.SemaphoreType.DMA((shape[0] // STEP,))]
    return call(
        functools.partial(
            finish_kernel,
            middles=len(pieces) - 4,
            scaled=scaled,
            following=following,
            totals=totals,
        ),
        outs,
        [*pieces, *extra],
        out_specs=[HBM if leaving else VMEM] * scaled + [VMEM] * (4 * following),
        scratch=scratch,
        flops=500_000_000,
    )


def tables_of(count):
    return [
        ((count * BAND, TILE), BF16),
        ((count * BAND, TILE), BF16),
        ((count, 128, 384), BF16),
    ]


def body(counts, sample_weights, classes, class_radius):
    shape = rows, columns = counts.shape
    groups = ((0, 1), (2, 3))
    cuts = (rows - 192, 192)
    rim, slim = (REACH, columns), (PILOT_RADIUS, columns)
    counts, sample_weights, classes = (
        pltpu.with_memory_space_constraint(field, pltpu.HBM)
        for field in (counts, sample_weights, classes)
    )
    chunks = rows // CHUNK
    *pilot_tables, mass, mass_a, mass_b, label_a, label_b = call(
        prepare_kernel,
        tables_of(1)
        + [(shape, F32), (slim, F32), (slim, F32), (rim, jnp.int32), (rim, jnp.int32)],
        [counts, sample_weights, classes],
        ins=[HBM, HBM, HBM],
        scratch=[
            pltpu.VMEM(shape, jnp.int32),
            pltpu.VMEM(shape, F32),
            pltpu.VMEM((2, *rim), jnp.int32),
            pltpu.SemaphoreType.DMA((2, chunks)),
            pltpu.SemaphoreType.DMA((2,)),
        ],
        flops=500_000_000,
    )
    mass_halo = exchange(mass_a, mass_b, "row")
    label_halo = exchange(label_a, label_b, "row")
    *tables, labels = call(
        bands_kernel,
        tables_of(CLASSES) + [(shape, BF16)],
        [class_radius, classes],
        ins=[SMEM, HBM],
        scratch=[pltpu.VMEM(shape, jnp.int32), pltpu.SemaphoreType.DMA((chunks,))],
        flops=500_000_000,
    )
    pieces = smooth(mass, mass_halo, None, None, pilot_tables, ((0,),), (rows,))
    adapted, *sends, first_stat = finish(pieces, [mass], False, True, True, shape)
    halo = exchange(*sends, "row")
    first_total = total_over(first_stat)
    pieces = smooth(adapted, halo, labels, label_halo, tables, groups, cuts)
    density_first, adapted, *sends, second_stat = finish(
        pieces, [first_total, first_total, mass], True, True, False, shape
    )
    halo = exchange(*sends, "row")
    second_total = total_over(second_stat)
    pieces, density_first = smooth(
        adapted, halo, labels, label_halo, tables, groups, cuts, density_first
    )
    (density_second,) = finish(
        pieces, [second_total, first_total], True, False, False, shape
    )
    return density_first, density_second


def solution(mesh):
    spec = P("row", "col")
    return jax.shard_map(
        body,
        mesh=mesh,
        in_specs=(spec, spec, spec, P()),
        out_specs=(spec, spec),
        check_vma=False,
    )
```

```python
import functools

import jax
import jax.numpy as jnp
from jax import lax
from jax.experimental import pallas as pl
from jax.experimental.pallas import tpu as pltpu
from jax.sharding import PartitionSpec as P


REACH = 64
PILOT_RADIUS = 32
CLASSES = 4
BACKGROUND = 0.5
TILE = 256
BAND = TILE + 2 * REACH
STEP = 64
F32 = jnp.float32
BF16 = jnp.bfloat16
MIB = 1 << 20
HBM = pl.BlockSpec(memory_space=pltpu.HBM)
VMEM = pl.BlockSpec(memory_space=pltpu.VMEM)
SMEM = pl.BlockSpec(memory_space=pltpu.SMEM)


def call(kernel, outs, args, ins=None, out_specs=None, scratch=(), limit=24, flops=0):
    return pl.pallas_call(
        kernel,
        out_shape=[jax.ShapeDtypeStruct(s, d) for s, d in outs],
        in_specs=ins or [VMEM] * len(args),
        out_specs=out_specs or [VMEM] * len(outs),
        scratch_shapes=scratch,
        compiler_params=pltpu.CompilerParams(vmem_limit_bytes=limit * MIB),
        cost_estimate=pl.CostEstimate(flops=flops, transcendentals=0, bytes_accessed=4 * MIB),
    )(*args)


def iota(shape, dim):
    return lax.broadcasted_iota(jnp.int32, shape, dim)


def split(value):
    high = value.astype(BF16)
    return high, (value - high.astype(F32)).astype(BF16)


def dot(a, b):
    return jnp.dot(a, b, preferred_element_type=F32)


def take(refs, *counts):
    groups = []
    for count in counts:
        groups.append(list(refs[:count]))
        refs = refs[count:]
    return *groups, list(refs)


def chosen(flag, when_set, when_clear):
    return jnp.where(flag > 0.5, when_set, when_clear)


def flags_of(axis):
    index = lax.axis_index(axis)
    last = lax.axis_size(axis) - 1
    values = (index & 1, jnp.minimum(index, 1), jnp.minimum(last - index, 1))
    return [jnp.full((1, 1), value.astype(F32), F32) for value in values]


def fill_bands(slot, radius, high_ref, low_ref, rim_ref):
    radius = jnp.full((1, 1), radius, F32)
    inverse = 1.0 / (2.0 * (0.5 * radius) * (0.5 * radius))

    def shape_of(d):
        return jnp.where(jnp.abs(d) <= radius, jnp.exp(-(d * d) * inverse), 0.0)

    lane = iota((8, 128), 1).astype(F32)
    tap = jnp.where(iota((8, 128), 0) == 0, jnp.where(lane == 0, 1.0, 2.0), 0.0)
    total = jnp.sum(shape_of(lane) * tap, axis=(0, 1), keepdims=True)
    column = iota((128, 128), 1)
    shift = iota((128, 128), 0) - column
    near = split(shape_of((shift - REACH).astype(F32)) / total)
    far = split(shape_of((shift + REACH).astype(F32)) / total)
    zero = jnp.zeros((128, 128), BF16)
    side = column[:REACH] < REACH
    zeros = jnp.zeros((REACH, 128), F32)
    base = slot * BAND
    for part, ref in enumerate((high_ref, low_ref)):
        blocks = ((near[part], zero), (far[part], near[part]), (zero, far[part]))
        for i, pair in enumerate(blocks):
            for k, block in enumerate(pair):
                lanes = slice(k * 128, (k + 1) * 128)
                ref[base + i * 128 : base + (i + 1) * 128, lanes] = block
        first = jnp.where(side, far[part][:REACH].astype(F32), zeros).astype(BF16)
        second = jnp.where(side, zeros, near[part][REACH:].astype(F32)).astype(BF16)
        for place in (0, 128) if part == 0 else (256,):
            rim_ref[slot, :REACH, place : place + 128] = first
            rim_ref[slot, REACH:, place : place + 128] = second


CHUNK = 128


def prepare_kernel(*refs):
    (counts_in, weights_in, classes_in), tables, outs, scratch = take(refs, 3, 3, 5)
    mass_ref, mass_a, mass_b, label_a, label_b = outs
    counts, weights, ends, arrived, ended = scratch
    rows = counts.shape[0]
    copies = []
    for n, start in enumerate(range(0, rows, CHUNK)):
        at = slice(start, start + CHUNK)
        pair = [
            pltpu.make_async_copy(counts_in.at[at], counts.at[at], arrived.at[0, n]),
            pltpu.make_async_copy(weights_in.at[at], weights.at[at], arrived.at[1, n]),
        ]
        for copy in pair:
            copy.start()
        copies.append((at, pair))
    end_copies = [
        pltpu.make_async_copy(classes_in.at[0:REACH], ends.at[0], ended.at[0]),
        pltpu.make_async_copy(classes_in.at[rows - REACH : rows], ends.at[1], ended.at[1]),
    ]
    for copy in end_copies:
        copy.start()
    fill_bands(0, F32(PILOT_RADIUS), *tables)
    for at, pair in copies:
        for copy in pair:
            copy.wait()
        mass_ref[at] = counts[at].astype(F32) * weights[at]
    odd = flags_of("row")[0]
    top, bottom = mass_ref[0:PILOT_RADIUS], mass_ref[rows - PILOT_RADIUS :]
    mass_a[...] = chosen(odd, top, bottom)
    mass_b[...] = chosen(odd, bottom, top)
    for copy in end_copies:
        copy.wait()
    label_a[...] = chosen(odd, ends[0], ends[1])
    label_b[...] = chosen(odd, ends[1], ends[0])


def bands_kernel(*refs):
    (radius_ref, classes_in), tables, (label_ref, classes, arrived) = take(refs, 2, 3)
    rows = classes.shape[0]
    copies = []
    for n, start in enumerate(range(0, rows, CHUNK)):
        at = slice(start, start + CHUNK)
        copy = pltpu.make_async_copy(classes_in.at[at], classes.at[at], arrived.at[n])
        copy.start()
        copies.append((at, copy))
    for c in range(CLASSES):
        fill_bands(c, radius_ref[c].astype(F32), *tables)
    for at, copy in copies:
        copy.wait()
        label_ref[at] = classes[at].astype(F32).astype(BF16)


def masked(pieces, labels, c):
    if labels is None:
        return pieces
    keep = labels == c
    return [jnp.where(keep, piece, jnp.zeros_like(piece)) for piece in pieces]


def rows_kernel(*refs, bands, labelled):
    (field_ref,), label_refs, (band_high, band_low, high_ref, low_ref, edge_ref) = take(
        refs, 1, labelled
    )
    rows, columns = field_ref.shape
    count = rows // REACH
    for n in range(columns // TILE):
        at = slice(n * TILE, (n + 1) * TILE)
        pieces = split(field_ref[:, at])
        labels = label_refs[0][:, at] if labelled else None
        for slot, c in enumerate(bands):
            high, low = masked(pieces, labels, c)
            sums = [None] * count

            def add(result, first):
                for i in range(result.shape[0] // REACH):
                    piece = result[i * REACH : (i + 1) * REACH]
                    own = sums[first + i]
                    sums[first + i] = piece if own is None else own + piece

            half = band_high[c * BAND : c * BAND + 2 * 128, 0:128]
            twice = jnp.concatenate([half, half], axis=1)
            for block in range(rows // 128):
                own = slice(block * 128, (block + 1) * 128)
                first = max(2 * block - 1, 0)
                last = min(2 * block + 3, count)
                taps = slice((first - 2 * block + 1) * REACH, (last - 2 * block + 1) * REACH)
                add(dot(twice[taps], jnp.concatenate([high[own], low[own]])), first)
            for tile in range(rows // TILE):
                own = slice(tile * TILE, (tile + 1) * TILE)
                first = max(4 * tile - 1, 0)
                last = min(4 * tile + 5, count)
                start = c * BAND + (first - 4 * tile + 1) * REACH
                taps = slice(start, start + (last - first) * REACH)
                add(dot(band_low[taps, :], high[own]), first)
            edge_ref[slot, 0:REACH, at] = sums[0]
            edge_ref[slot, REACH:, at] = sums[-1]
            for i, value in enumerate(sums[1:-1]):
                target = slice(i * REACH, (i + 1) * REACH)
                high_ref[slot, target, at], low_ref[slot, target, at] = split(value)


def kept_row(start, rows):
    if start < REACH:
        return rows - 2 * REACH + start
    return start if start >= rows - REACH else start - REACH


def stacked_left(sides, inputs, start, stop, inner):
    refs, edge_ref = sides
    pieces = []
    slot = 0
    for ref in refs:
        for own in range(ref.shape[0]):
            rows = []
            if start < inner:
                rows.append(ref[own, start : min(stop, inner), inputs])
            if stop > inner:
                rows.append(edge_ref[slot, max(start, inner) - inner : stop - inner, inputs])
            pieces.append(rows[0] if len(rows) == 1 else jnp.concatenate(rows))
            slot += 1
    return jnp.concatenate(pieces, axis=1)


def swept(highs, lows, bands, band_refs, block, width, columns, start, stop, inner):
    high_ref, low_ref = band_refs

    def window(first, last):
        here, there = max(first, 0), min(last, columns)
        return slice(here, there), slice(here - first, there - first)

    def rights(refs_and_lanes, taps):
        return jnp.concatenate(
            [
                jnp.concatenate(
                    [ref[c * BAND + taps.start : c * BAND + taps.stop, lanes] for ref, lanes in refs_and_lanes],
                    axis=1,
                )
                for c in bands
            ]
        )

    results = []
    origin = block * TILE - 128
    for part in range(width // 128):
        inputs, taps = window(origin + part * 128, origin + (part + 2) * 128)
        left = stacked_left(highs, inputs, start, stop, inner)
        right = rights(((high_ref, slice(0, 128)), (low_ref, slice(0, 128))), taps)
        both = dot(left, right)
        results.append(both[:, :128] + both[:, 128:])
    inputs, taps = window(origin, origin + width + 128)
    left = stacked_left(lows, inputs, start, stop, inner)
    rest = dot(left, rights(((high_ref, slice(0, width)),), taps))
    return [value + rest[:, k * 128 : (k + 1) * 128] for k, value in enumerate(results)]


def edges_kernel(*refs, groups, labelled):
    count = len(groups)
    halo, labels_in, partials, highs, lows, (rim_ref, *band_refs), outs = take(
        refs, 2, 2 * labelled, count, count, count, 3
    )
    edge_high, edge_low, left_ref, right_ref, send_a, send_b = outs
    bands = [c for group in groups for c in group]
    sources = [(ref, own) for ref in partials for own in range(ref.shape[0])]
    columns = halo[0].shape[1]
    odd_row, has_top, has_bottom = flags_of("row")
    odd_column = flags_of("col")[0]
    for n in range(columns // TILE):
        at = slice(n * TILE, (n + 1) * TILE)

        def joined(pair):
            first, second = pair[0][:, at].astype(F32), pair[1][:, at].astype(F32)
            top = chosen(has_top, chosen(odd_row, first, second), 0.0)
            bottom = chosen(has_bottom, chosen(odd_row, second, first), 0.0)
            missing = REACH - first.shape[0]
            if missing:
                zeros = jnp.zeros((missing, TILE), F32)
                return jnp.concatenate([zeros, top, bottom, zeros])
            return jnp.concatenate([top, bottom])

        pieces = split(joined(halo))
        labels = joined(labels_in).astype(BF16) if labelled else None
        for slot, c in enumerate(bands):
            high, low = masked(pieces, labels, c)
            right = jnp.concatenate([high, low, high], axis=0)
            source, own = sources[slot]
            value = source[own, :, at] + dot(rim_ref[c], right)
            edge_high[slot, :, at], edge_low[slot, :, at] = split(value)
    rows = left_ref.shape[0]
    inner = rows - 2 * REACH
    for target, block in ((left_ref, 0), (right_ref, columns // TILE)):
        results = swept(
            (highs, edge_high),
            (lows, edge_low),
            bands,
            band_refs,
            block,
            target.shape[1],
            columns,
            0,
            rows,
            inner,
        )
        for k, value in enumerate(results):
            target[:, k * 128 : (k + 1) * 128] = value
    half = rows // 2
    lower = iota((half, 128), 1) < REACH
    left = left_ref[:, 0:128]
    left = jnp.where(lower, left[:half], pltpu.roll(left[half:], REACH, 1))
    right = right_ref[...]
    right = jnp.where(lower, pltpu.roll(right[:half], REACH, 1), right[half:])
    send_a[...] = chosen(odd_column, left, right)
    send_b[...] = chosen(odd_column, right, left)


def middle_kernel(*refs, groups, start):
    count = len(groups)
    highs, lows, (edge_high, edge_low), band_refs, (left_ref, right_ref), (out_ref,) = take(
        refs, count, count, 2, 2, 2
    )
    bands = [c for group in groups for c in group]
    inner = highs[0].shape[1]
    rows, columns = out_ref.shape
    at = slice(start, start + rows)
    lower = iota((rows, 128), 1) < REACH

    def blocks():
        for k in range(0, TILE, 128):
            yield left_ref[at, k : k + 128]
        for j in range(1, columns // TILE):
            yield from swept(
                (highs, edge_high),
                (lows, edge_low),
                bands,
                band_refs,
                j,
                TILE,
                columns,
                start,
                start + rows,
                inner,
            )
        yield right_ref[at, :]

    before = None
    for k, block in enumerate(blocks()):
        turned = pltpu.roll(block, REACH, 1)
        if before is not None:
            out_ref[:, (k - 1) * 128 : k * 128] = jnp.where(lower, before, turned)
        before = turned


def gathered(middles, come, flags, start):
    odd, has_left, has_right = flags
    rows = sum(ref.shape[0] for ref in middles)
    columns = middles[0].shape[1]
    half = rows // 2
    kept = kept_row(start, rows)
    lane = iota((STEP, 128), 1)
    local = slice(kept % half, kept % half + STEP)
    come_left = chosen(has_left, chosen(odd, come[0][local], come[1][local]), 0.0)
    come_right = chosen(has_right, chosen(odd, come[1][local], come[0][local]), 0.0)
    if kept < half:
        come_right = pltpu.roll(come_right, REACH, 1)
    else:
        come_left = pltpu.roll(come_left, REACH, 1)
    own = kept
    for middle_ref in middles:
        if own < middle_ref.shape[0]:
            break
        own -= middle_ref.shape[0]
    for k in range(0, columns, 128):
        block = middle_ref[own : own + STEP, k : k + 128]
        if k == 0:
            block = block + jnp.where(lane < REACH, come_left, 0.0)
        if k == columns - 128:
            block = block + jnp.where(lane >= REACH, come_right, 0.0)
        yield block


def finish_kernel(*refs, middles, scaled, following, totals):
    middle_refs, come, totals_in, mass_in, density_out, refs = take(
        refs, middles, 2, 2 * scaled, following, scaled
    )
    adapted_out, refs = take(refs, 4 * following)
    rows = sum(ref.shape[0] for ref in middle_refs)
    columns = middle_refs[0].shape[1]
    column_flags = flags_of("col")
    copies = []
    if scaled:
        inverse = jnp.exp(-(totals_in[0][0:1, :] / totals_in[1][1:2, :]))
        staged, done = refs
        for number, start in enumerate(range(0, rows, STEP)):
            at = slice(start, start + STEP)
            for k, block in enumerate(gathered(middle_refs, come, column_flags, start)):
                staged[at, k * 128 : (k + 1) * 128] = block * inverse
            copy = pltpu.make_async_copy(staged.at[at], density_out[0].at[at], done.at[number])
            copy.start()
            copies.append(copy)
    if following:
        adapted_ref, send_a, send_b, stat_ref = adapted_out
        odd_row = flags_of("row")[0]
        log_sums = [jnp.zeros((8, 128), F32)] * (columns // 128)
        mass_sums = [jnp.zeros((8, 128), F32)] * (columns // 128)
        for start in range(0, rows, STEP):
            at = slice(start, start + STEP)
            if scaled:
                blocks = (staged[at, k : k + 128] for k in range(0, columns, 128))
            else:
                blocks = gathered(middle_refs, come, column_flags, start)
            for k, block in enumerate(blocks):
                lanes = slice(k * 128, (k + 1) * 128)
                pilot = block + BACKGROUND
                mass = mass_in[0][at, lanes]
                adapted_ref[at, lanes] = mass * pilot
                terms = mass * jnp.log(pilot)
                log_sums[k] += jnp.sum(terms.reshape(STEP // 8, 8, 128), axis=0)
                if totals:
                    mass_sums[k] += jnp.sum(mass.reshape(STEP // 8, 8, 128), axis=0)
        top, bottom = adapted_ref[0:REACH], adapted_ref[rows - REACH :]
        send_a[...] = chosen(odd_row, top, bottom)
        send_b[...] = chosen(odd_row, bottom, top)
        log_sum = jnp.sum(sum(log_sums), axis=(0, 1), keepdims=True)
        mass_sum = jnp.sum(sum(mass_sums), axis=(0, 1), keepdims=True)
        row = iota((8, 128), 0)
        stat_ref[...] = jnp.where(row == 0, log_sum, jnp.where(row == 1, mass_sum, 0.0))
    for copy in copies:
        copy.wait()


def exchange(first, second, axis):
    along = 0 if axis == "row" else 1
    sizes = [lax.axis_size("row"), lax.axis_size("col")]
    results = []
    for offset, value in ((0, first), (1, second)):
        pairs = []
        for index in range(sizes[0] * sizes[1]):
            place = [index // sizes[1], index % sizes[1]]
            own = place[along]
            partner = own + 1 if own % 2 == offset else own - 1
            if 0 <= partner < sizes[along]:
                place[along] = partner
            else:
                place[1 - along] ^= 1
            pairs.append((index, place[0] * sizes[1] + place[1]))
        results.append(lax.ppermute(value, ("row", "col"), pairs))
    return results


HOPS = (
    (0, 7, (1, 8)),
    (0, 3, (1, 8)),
    (12, 1, (16, 1)),
    (4, 1, (16, 1)),
    (0, 1, (1, 2)),
    (3, 1, (4, 1)),
    (1, 1, (2, 1)),
)


def total_over(stat):
    sizes = (lax.axis_size("row"), lax.axis_size("col"))
    for rows, columns, least in HOPS:
        if sizes[0] >= least[0] and sizes[1] >= least[1]:
            pairs = []
            for index in range(sizes[0] * sizes[1]):
                row, column = divmod(index, sizes[1])
                pairs.append((index, (row ^ rows) * sizes[1] + (column ^ columns)))
            stat = stat + lax.ppermute(stat, ("row", "col"), pairs)
    return stat


def smooth(field, halo, labels, label_halo, tables, groups, cuts):
    high, low, rim = tables
    rows, columns = field.shape
    labelled = labels is not None
    bands = [c for group in groups for c in group]
    highs, lows, partials = [], [], []
    for group in groups:
        inner = (len(group), rows - 2 * REACH, columns)
        edge = (len(group), 2 * REACH, columns)
        results = call(
            functools.partial(rows_kernel, bands=group, labelled=labelled),
            [(inner, BF16), (inner, BF16), (edge, F32)],
            [field] + ([labels] if labelled else []) + [high, low],
            flops=len(group) * 1_000_000_000,
        )
        for results_of, result in zip((highs, lows, partials), results):
            results_of.append(result)
    edge = (len(bands), 2 * REACH, columns)
    edge_high, edge_low, left, right, send_a, send_b = call(
        functools.partial(edges_kernel, groups=groups, labelled=labelled),
        [(edge, BF16), (edge, BF16), ((rows, TILE), F32), ((rows, 128), F32)]
        + [((rows // 2, 128), F32)] * 2,
        [*halo, *(label_halo if labelled else ()), *partials, *highs, *lows]
        + [rim, high, low],
        flops=len(bands) * 500_000_000,
    )
    come = exchange(send_a, send_b, "col")
    middles = []
    start = 0
    for count in cuts:
        middles += call(
            functools.partial(middle_kernel, groups=groups, start=start),
            [((count, columns), F32)],
            [*highs, *lows, edge_high, edge_low, high, low, left, right],
            flops=len(bands) * 750_000_000 * count // rows,
        )
        start += count
    return [*middles, *come]


def finish(pieces, extra, scaled, following, totals, shape):
    plane, rim, stat = (shape, F32), ((REACH, shape[1]), F32), ((8, 128), F32)
    outs = [plane] * scaled + [plane, rim, rim, stat] * following
    scratch = []
    if scaled:
        scratch = [pltpu.VMEM(shape, F32), pltpu.SemaphoreType.DMA((shape[0] // STEP,))]
    return call(
        functools.partial(
            finish_kernel,
            middles=len(pieces) - 2,
            scaled=scaled,
            following=following,
            totals=totals,
        ),
        outs,
        [*pieces, *extra],
        out_specs=[HBM] * scaled + [VMEM] * (4 * following),
        scratch=scratch,
        flops=500_000_000,
    )


def tables_of(count):
    return [
        ((count * BAND, TILE), BF16),
        ((count * BAND, TILE), BF16),
        ((count, 128, 384), BF16),
    ]


def body(counts, sample_weights, classes, class_radius):
    shape = rows, columns = counts.shape
    groups = ((0, 1), (2, 3))
    cuts = (rows - 192, 192)
    rim, slim = (REACH, columns), (PILOT_RADIUS, columns)
    counts, sample_weights, classes = (
        pltpu.with_memory_space_constraint(field, pltpu.HBM)
        for field in (counts, sample_weights, classes)
    )
    chunks = rows // CHUNK
    *pilot_tables, mass, mass_a, mass_b, label_a, label_b = call(
        prepare_kernel,
        tables_of(1)
        + [(shape, F32), (slim, F32), (slim, F32), (rim, jnp.int32), (rim, jnp.int32)],
        [counts, sample_weights, classes],
        ins=[HBM, HBM, HBM],
        scratch=[
            pltpu.VMEM(shape, jnp.int32),
            pltpu.VMEM(shape, F32),
            pltpu.VMEM((2, *rim), jnp.int32),
            pltpu.SemaphoreType.DMA((2, chunks)),
            pltpu.SemaphoreType.DMA((2,)),
        ],
        flops=500_000_000,
    )
    mass_halo = exchange(mass_a, mass_b, "row")
    label_halo = exchange(label_a, label_b, "row")
    *tables, labels = call(
        bands_kernel,
        tables_of(CLASSES) + [(shape, BF16)],
        [class_radius, classes],
        ins=[SMEM, HBM],
        scratch=[pltpu.VMEM(shape, jnp.int32), pltpu.SemaphoreType.DMA((chunks,))],
        flops=500_000_000,
    )
    pieces = smooth(mass, mass_halo, None, None, pilot_tables, ((0,),), (rows,))
    adapted, *sends, first_stat = finish(pieces, [mass], False, True, True, shape)
    halo = exchange(*sends, "row")
    first_total = total_over(first_stat)
    pieces = smooth(adapted, halo, labels, label_halo, tables, groups, cuts)
    density_first, adapted, *sends, second_stat = finish(
        pieces, [first_total, first_total, mass], True, True, False, shape
    )
    halo = exchange(*sends, "row")
    second_total = total_over(second_stat)
    pieces = smooth(adapted, halo, labels, label_halo, tables, groups, cuts)
    (density_second,) = finish(
        pieces, [second_total, first_total], True, False, False, shape
    )
    return density_first, density_second


def solution(mesh):
    spec = P("row", "col")
    return jax.shard_map(
        body,
        mesh=mesh,
        in_specs=(spec, spec, spec, P()),
        out_specs=(spec, spec),
        check_vma=False,
    )
```

```python
import functools

import jax
import jax.numpy as jnp
from jax import lax
from jax.experimental import pallas as pl
from jax.experimental.pallas import tpu as pltpu
from jax.sharding import PartitionSpec as P


REACH = 64
PILOT_RADIUS = 32
CLASSES = 4
BACKGROUND = 0.5
TILE = 256
BAND = TILE + 2 * REACH
STEP = 64
F32 = jnp.float32
BF16 = jnp.bfloat16
MIB = 1 << 20
HBM = pl.BlockSpec(memory_space=pltpu.HBM)
VMEM = pl.BlockSpec(memory_space=pltpu.VMEM)
SMEM = pl.BlockSpec(memory_space=pltpu.SMEM)


def call(kernel, outs, args, ins=None, out_specs=None, scratch=(), limit=24, flops=0):
    return pl.pallas_call(
        kernel,
        out_shape=[jax.ShapeDtypeStruct(s, d) for s, d in outs],
        in_specs=ins or [VMEM] * len(args),
        out_specs=out_specs or [VMEM] * len(outs),
        scratch_shapes=scratch,
        compiler_params=pltpu.CompilerParams(vmem_limit_bytes=limit * MIB),
        cost_estimate=pl.CostEstimate(flops=flops, transcendentals=0, bytes_accessed=4 * MIB),
    )(*args)


def iota(shape, dim):
    return lax.broadcasted_iota(jnp.int32, shape, dim)


def split(value):
    high = value.astype(BF16)
    return high, (value - high.astype(F32)).astype(BF16)


def dot(a, b):
    return jnp.dot(a, b, preferred_element_type=F32)


def take(refs, *counts):
    groups = []
    for count in counts:
        groups.append(list(refs[:count]))
        refs = refs[count:]
    return *groups, list(refs)


def chosen(flag, when_set, when_clear):
    return jnp.where(flag > 0.5, when_set, when_clear)


def flags_of(axis):
    index = lax.axis_index(axis)
    last = lax.axis_size(axis) - 1
    values = (index & 1, jnp.minimum(index, 1), jnp.minimum(last - index, 1))
    return [jnp.full((1, 1), value.astype(F32), F32) for value in values]


def fill_bands(slot, radius, high_ref, low_ref, rim_ref):
    radius = jnp.full((1, 1), radius, F32)
    inverse = 1.0 / (2.0 * (0.5 * radius) * (0.5 * radius))

    def shape_of(d):
        return jnp.where(jnp.abs(d) <= radius, jnp.exp(-(d * d) * inverse), 0.0)

    lane = iota((8, 128), 1).astype(F32)
    tap = jnp.where(iota((8, 128), 0) == 0, jnp.where(lane == 0, 1.0, 2.0), 0.0)
    total = jnp.sum(shape_of(lane) * tap, axis=(0, 1), keepdims=True)
    column = iota((128, 128), 1)
    shift = iota((128, 128), 0) - column
    near = split(shape_of((shift - REACH).astype(F32)) / total)
    far = split(shape_of((shift + REACH).astype(F32)) / total)
    zero = jnp.zeros((128, 128), BF16)
    side = column[:REACH] < REACH
    zeros = jnp.zeros((REACH, 128), F32)
    base = slot * BAND
    for part, ref in enumerate((high_ref, low_ref)):
        blocks = ((near[part], zero), (far[part], near[part]), (zero, far[part]))
        for i, pair in enumerate(blocks):
            for k, block in enumerate(pair):
                lanes = slice(k * 128, (k + 1) * 128)
                ref[base + i * 128 : base + (i + 1) * 128, lanes] = block
        first = jnp.where(side, far[part][:REACH].astype(F32), zeros).astype(BF16)
        second = jnp.where(side, zeros, near[part][REACH:].astype(F32)).astype(BF16)
        for place in (0, 128) if part == 0 else (256,):
            rim_ref[slot, :REACH, place : place + 128] = first
            rim_ref[slot, REACH:, place : place + 128] = second


CHUNK = 128


def prepare_kernel(*refs):
    (counts_in, weights_in, classes_in), tables, outs, scratch = take(refs, 3, 3, 5)
    mass_ref, mass_a, mass_b, label_a, label_b = outs
    counts, weights, ends, arrived, ended = scratch
    rows = counts.shape[0]
    copies = []
    for n, start in enumerate(range(0, rows, CHUNK)):
        at = slice(start, start + CHUNK)
        pair = [
            pltpu.make_async_copy(counts_in.at[at], counts.at[at], arrived.at[0, n]),
            pltpu.make_async_copy(weights_in.at[at], weights.at[at], arrived.at[1, n]),
        ]
        for copy in pair:
            copy.start()
        copies.append((at, pair))
    end_copies = [
        pltpu.make_async_copy(classes_in.at[0:REACH], ends.at[0], ended.at[0]),
        pltpu.make_async_copy(classes_in.at[rows - REACH : rows], ends.at[1], ended.at[1]),
    ]
    for copy in end_copies:
        copy.start()
    fill_bands(0, F32(PILOT_RADIUS), *tables)
    for at, pair in copies:
        for copy in pair:
            copy.wait()
        mass_ref[at] = counts[at].astype(F32) * weights[at]
    odd = flags_of("row")[0]
    top, bottom = mass_ref[0:PILOT_RADIUS], mass_ref[rows - PILOT_RADIUS :]
    mass_a[...] = chosen(odd, top, bottom)
    mass_b[...] = chosen(odd, bottom, top)
    for copy in end_copies:
        copy.wait()
    label_a[...] = chosen(odd, ends[0], ends[1])
    label_b[...] = chosen(odd, ends[1], ends[0])


def bands_kernel(*refs):
    (radius_ref, classes_in), tables, (label_ref, classes, arrived) = take(refs, 2, 3)
    rows = classes.shape[0]
    copies = []
    for n, start in enumerate(range(0, rows, CHUNK)):
        at = slice(start, start + CHUNK)
        copy = pltpu.make_async_copy(classes_in.at[at], classes.at[at], arrived.at[n])
        copy.start()
        copies.append((at, copy))
    for c in range(CLASSES):
        fill_bands(c, radius_ref[c].astype(F32), *tables)
    for at, copy in copies:
        copy.wait()
        label_ref[at] = classes[at].astype(F32).astype(BF16)


def masked(pieces, labels, c):
    if labels is None:
        return pieces
    keep = labels == c
    return [jnp.where(keep, piece, jnp.zeros_like(piece)) for piece in pieces]


def rows_kernel(*refs, bands, labelled):
    (field_ref,), label_refs, (band_high, band_low, high_ref, low_ref, edge_ref) = take(
        refs, 1, labelled
    )
    rows, columns = field_ref.shape
    count = rows // REACH
    for n in range(columns // TILE):
        at = slice(n * TILE, (n + 1) * TILE)
        pieces = split(field_ref[:, at])
        labels = label_refs[0][:, at] if labelled else None
        for slot, c in enumerate(bands):
            high, low = masked(pieces, labels, c)
            sums = [None] * count

            def add(result, first):
                for i in range(result.shape[0] // REACH):
                    piece = result[i * REACH : (i + 1) * REACH]
                    own = sums[first + i]
                    sums[first + i] = piece if own is None else own + piece

            half = band_high[c * BAND : c * BAND + 2 * 128, 0:128]
            twice = jnp.concatenate([half, half], axis=1)
            for block in range(rows // 128):
                own = slice(block * 128, (block + 1) * 128)
                first = max(2 * block - 1, 0)
                last = min(2 * block + 3, count)
                taps = slice((first - 2 * block + 1) * REACH, (last - 2 * block + 1) * REACH)
                add(dot(twice[taps], jnp.concatenate([high[own], low[own]])), first)
            for tile in range(rows // TILE):
                own = slice(tile * TILE, (tile + 1) * TILE)
                first = max(4 * tile - 1, 0)
                last = min(4 * tile + 5, count)
                start = c * BAND + (first - 4 * tile + 1) * REACH
                taps = slice(start, start + (last - first) * REACH)
                add(dot(band_low[taps, :], high[own]), first)
            edge_ref[slot, 0:REACH, at] = sums[0]
            edge_ref[slot, REACH:, at] = sums[-1]
            for i, value in enumerate(sums[1:-1]):
                target = slice(i * REACH, (i + 1) * REACH)
                high_ref[slot, target, at], low_ref[slot, target, at] = split(value)


def kept_row(start, rows):
    if start < REACH:
        return rows - 2 * REACH + start
    return start if start >= rows - REACH else start - REACH


def stacked_left(sides, inputs, start, stop, inner):
    refs, edge_ref = sides
    pieces = []
    slot = 0
    for ref in refs:
        for own in range(ref.shape[0]):
            rows = []
            if start < inner:
                rows.append(ref[own, start : min(stop, inner), inputs])
            if stop > inner:
                rows.append(edge_ref[slot, max(start, inner) - inner : stop - inner, inputs])
            pieces.append(rows[0] if len(rows) == 1 else jnp.concatenate(rows))
            slot += 1
    return jnp.concatenate(pieces, axis=1)


def swept(highs, lows, bands, band_refs, block, width, columns, start, stop, inner):
    high_ref, low_ref = band_refs

    def window(first, last):
        here, there = max(first, 0), min(last, columns)
        return slice(here, there), slice(here - first, there - first)

    def rights(refs_and_lanes, taps):
        return jnp.concatenate(
            [
                jnp.concatenate(
                    [ref[c * BAND + taps.start : c * BAND + taps.stop, lanes] for ref, lanes in refs_and_lanes],
                    axis=1,
                )
                for c in bands
            ]
        )

    results = []
    origin = block * TILE - 128
    for part in range(width // 128):
        inputs, taps = window(origin + part * 128, origin + (part + 2) * 128)
        left = stacked_left(highs, inputs, start, stop, inner)
        right = rights(((high_ref, slice(0, 128)), (low_ref, slice(0, 128))), taps)
        both = dot(left, right)
        results.append(both[:, :128] + both[:, 128:])
    inputs, taps = window(origin, origin + width + 128)
    left = stacked_left(lows, inputs, start, stop, inner)
    rest = dot(left, rights(((high_ref, slice(0, width)),), taps))
    return [value + rest[:, k * 128 : (k + 1) * 128] for k, value in enumerate(results)]


def edges_kernel(*refs, groups, labelled):
    count = len(groups)
    halo, labels_in, partials, highs, lows, (rim_ref, *band_refs), outs = take(
        refs, 2, 2 * labelled, count, count, count, 3
    )
    edge_high, edge_low, left_ref, right_ref, send_a, send_b = outs
    bands = [c for group in groups for c in group]
    sources = [(ref, own) for ref in partials for own in range(ref.shape[0])]
    columns = halo[0].shape[1]
    odd_row, has_top, has_bottom = flags_of("row")
    odd_column = flags_of("col")[0]
    for n in range(columns // TILE):
        at = slice(n * TILE, (n + 1) * TILE)

        def joined(pair):
            first, second = pair[0][:, at].astype(F32), pair[1][:, at].astype(F32)
            top = chosen(has_top, chosen(odd_row, first, second), 0.0)
            bottom = chosen(has_bottom, chosen(odd_row, second, first), 0.0)
            missing = REACH - first.shape[0]
            if missing:
                zeros = jnp.zeros((missing, TILE), F32)
                return jnp.concatenate([zeros, top, bottom, zeros])
            return jnp.concatenate([top, bottom])

        pieces = split(joined(halo))
        labels = joined(labels_in).astype(BF16) if labelled else None
        for slot, c in enumerate(bands):
            high, low = masked(pieces, labels, c)
            right = jnp.concatenate([high, low, high], axis=0)
            source, own = sources[slot]
            value = source[own, :, at] + dot(rim_ref[c], right)
            edge_high[slot, :, at], edge_low[slot, :, at] = split(value)
    rows = left_ref.shape[0]
    inner = rows - 2 * REACH
    for target, block in ((left_ref, 0), (right_ref, columns // TILE)):
        results = swept(
            (highs, edge_high),
            (lows, edge_low),
            bands,
            band_refs,
            block,
            target.shape[1],
            columns,
            0,
            rows,
            inner,
        )
        for k, value in enumerate(results):
            target[:, k * 128 : (k + 1) * 128] = value
    half = rows // 2
    lower = iota((half, 128), 1) < REACH
    left = left_ref[:, 0:128]
    left = jnp.where(lower, left[:half], pltpu.roll(left[half:], REACH, 1))
    right = right_ref[...]
    right = jnp.where(lower, pltpu.roll(right[:half], REACH, 1), right[half:])
    send_a[...] = chosen(odd_column, left, right)
    send_b[...] = chosen(odd_column, right, left)


def middle_kernel(*refs, groups, start):
    count = len(groups)
    highs, lows, (edge_high, edge_low), band_refs, (left_ref, right_ref), (out_ref,) = take(
        refs, count, count, 2, 2, 2
    )
    bands = [c for group in groups for c in group]
    inner = highs[0].shape[1]
    rows, columns = out_ref.shape
    at = slice(start, start + rows)
    lower = iota((rows, 128), 1) < REACH

    def blocks():
        for k in range(0, TILE, 128):
            yield left_ref[at, k : k + 128]
        for j in range(1, columns // TILE):
            yield from swept(
                (highs, edge_high),
                (lows, edge_low),
                bands,
                band_refs,
                j,
                TILE,
                columns,
                start,
                start + rows,
                inner,
            )
        yield right_ref[at, :]

    before = None
    for k, block in enumerate(blocks()):
        turned = pltpu.roll(block, REACH, 1)
        if before is not None:
            out_ref[:, (k - 1) * 128 : k * 128] = jnp.where(lower, before, turned)
        before = turned


def gathered(middles, come, flags, start):
    odd, has_left, has_right = flags
    rows = sum(ref.shape[0] for ref in middles)
    columns = middles[0].shape[1]
    half = rows // 2
    kept = kept_row(start, rows)
    lane = iota((STEP, 128), 1)
    local = slice(kept % half, kept % half + STEP)
    come_left = chosen(has_left, chosen(odd, come[0][local], come[1][local]), 0.0)
    come_right = chosen(has_right, chosen(odd, come[1][local], come[0][local]), 0.0)
    if kept < half:
        come_right = pltpu.roll(come_right, REACH, 1)
    else:
        come_left = pltpu.roll(come_left, REACH, 1)
    own = kept
    for middle_ref in middles:
        if own < middle_ref.shape[0]:
            break
        own -= middle_ref.shape[0]
    for k in range(0, columns, 128):
        block = middle_ref[own : own + STEP, k : k + 128]
        if k == 0:
            block = block + jnp.where(lane < REACH, come_left, 0.0)
        if k == columns - 128:
            block = block + jnp.where(lane >= REACH, come_right, 0.0)
        yield block


def tally_kernel(*refs, middles, scaled, totals):
    middle_refs, come, totals_in, (mass_ref, plane_ref, stat_ref) = take(
        refs, middles, 2, 2 * scaled
    )
    rows, columns = plane_ref.shape
    flags = flags_of("col")
    if scaled:
        inverse = jnp.exp(-(totals_in[0][0:1, :] / totals_in[1][1:2, :]))
    log_sums = [jnp.zeros((8, 128), F32)] * (columns // 128)
    mass_sums = [jnp.zeros((8, 128), F32)] * (columns // 128)
    for start in range(0, rows, STEP):
        at = slice(start, start + STEP)
        for k, block in enumerate(gathered(middle_refs, come, flags, start)):
            lanes = slice(k * 128, (k + 1) * 128)
            if scaled:
                block = block * inverse
            plane_ref[at, lanes] = block
            mass = mass_ref[at, lanes]
            terms = mass * jnp.log(block + BACKGROUND)
            log_sums[k] += jnp.sum(terms.reshape(STEP // 8, 8, 128), axis=0)
            if totals:
                mass_sums[k] += jnp.sum(mass.reshape(STEP // 8, 8, 128), axis=0)
    log_sum = jnp.sum(sum(log_sums), axis=(0, 1), keepdims=True)
    mass_sum = jnp.sum(sum(mass_sums), axis=(0, 1), keepdims=True)
    row = iota((8, 128), 0)
    stat_ref[...] = jnp.where(row == 0, log_sum, jnp.where(row == 1, mass_sum, 0.0))


def adapt_kernel(*refs, kept):
    (plane_ref, mass_ref, adapted_ref, send_a, send_b), density_out, done = take(refs, 5, kept)
    rows = plane_ref.shape[0]
    copies = []
    if kept:
        for number, start in enumerate(range(0, rows, STEP)):
            at = slice(start, start + STEP)
            copies.append(
                pltpu.make_async_copy(
                    plane_ref.at[at], density_out[0].at[at], done[0].at[number]
                )
            )
    for copy in copies:
        copy.start()
    for start in range(0, rows, STEP):
        at = slice(start, start + STEP)
        adapted_ref[at] = mass_ref[at] * (plane_ref[at] + BACKGROUND)
    odd = flags_of("row")[0]
    top, bottom = adapted_ref[0:REACH], adapted_ref[rows - REACH :]
    send_a[...] = chosen(odd, top, bottom)
    send_b[...] = chosen(odd, bottom, top)
    for copy in copies:
        copy.wait()


def finish_kernel(*refs, middles):
    middle_refs, come, totals_in, (density_ref, staged, done) = take(refs, middles, 2, 2)
    rows, _ = staged.shape
    flags = flags_of("col")
    inverse = jnp.exp(-(totals_in[0][0:1, :] / totals_in[1][1:2, :]))
    copies = []
    for number, start in enumerate(range(0, rows, STEP)):
        at = slice(start, start + STEP)
        for k, block in enumerate(gathered(middle_refs, come, flags, start)):
            staged[at, k * 128 : (k + 1) * 128] = block * inverse
        copy = pltpu.make_async_copy(staged.at[at], density_ref.at[at], done.at[number])
        copy.start()
        copies.append(copy)
    for copy in copies:
        copy.wait()


def exchange(first, second, axis):
    along = 0 if axis == "row" else 1
    sizes = [lax.axis_size("row"), lax.axis_size("col")]
    results = []
    for offset, value in ((0, first), (1, second)):
        pairs = []
        for index in range(sizes[0] * sizes[1]):
            place = [index // sizes[1], index % sizes[1]]
            own = place[along]
            partner = own + 1 if own % 2 == offset else own - 1
            if 0 <= partner < sizes[along]:
                place[along] = partner
            else:
                place[1 - along] ^= 1
            pairs.append((index, place[0] * sizes[1] + place[1]))
        results.append(lax.ppermute(value, ("row", "col"), pairs))
    return results


HOPS = (
    (0, 7, (1, 8)),
    (0, 3, (1, 8)),
    (12, 1, (16, 1)),
    (4, 1, (16, 1)),
    (0, 1, (1, 2)),
    (3, 1, (4, 1)),
    (1, 1, (2, 1)),
)


def total_over(stat):
    sizes = (lax.axis_size("row"), lax.axis_size("col"))
    for rows, columns, least in HOPS:
        if sizes[0] >= least[0] and sizes[1] >= least[1]:
            pairs = []
            for index in range(sizes[0] * sizes[1]):
                row, column = divmod(index, sizes[1])
                pairs.append((index, (row ^ rows) * sizes[1] + (column ^ columns)))
            stat = stat + lax.ppermute(stat, ("row", "col"), pairs)
    return stat


def smooth(field, halo, labels, label_halo, tables, groups, cuts):
    high, low, rim = tables
    rows, columns = field.shape
    labelled = labels is not None
    bands = [c for group in groups for c in group]
    highs, lows, partials = [], [], []
    for group in groups:
        inner = (len(group), rows - 2 * REACH, columns)
        edge = (len(group), 2 * REACH, columns)
        results = call(
            functools.partial(rows_kernel, bands=group, labelled=labelled),
            [(inner, BF16), (inner, BF16), (edge, F32)],
            [field] + ([labels] if labelled else []) + [high, low],
            flops=len(group) * 1_000_000_000,
        )
        for results_of, result in zip((highs, lows, partials), results):
            results_of.append(result)
    edge = (len(bands), 2 * REACH, columns)
    edge_high, edge_low, left, right, send_a, send_b = call(
        functools.partial(edges_kernel, groups=groups, labelled=labelled),
        [(edge, BF16), (edge, BF16), ((rows, TILE), F32), ((rows, 128), F32)]
        + [((rows // 2, 128), F32)] * 2,
        [*halo, *(label_halo if labelled else ()), *partials, *highs, *lows]
        + [rim, high, low],
        flops=len(bands) * 500_000_000,
    )
    come = exchange(send_a, send_b, "col")
    middles = []
    start = 0
    for count in cuts:
        middles += call(
            functools.partial(middle_kernel, groups=groups, start=start),
            [((count, columns), F32)],
            [*highs, *lows, edge_high, edge_low, high, low, left, right],
            flops=len(bands) * 750_000_000 * count // rows,
        )
        start += count
    return [*middles, *come]


def leaving(shape):
    return pltpu.SemaphoreType.DMA((shape[0] // STEP,))


def tally(pieces, totals_in, mass):
    shape = mass.shape
    return call(
        functools.partial(
            tally_kernel,
            middles=len(pieces) - 2,
            scaled=bool(totals_in),
            totals=not totals_in,
        ),
        [(shape, F32), ((8, 128), F32)],
        [*pieces, *totals_in, mass],
        flops=500_000_000,
    )


def adapt(plane, mass, kept):
    shape = mass.shape
    rim = (REACH, shape[1])
    return call(
        functools.partial(adapt_kernel, kept=kept),
        [(shape, F32), (rim, F32), (rim, F32)] + [(shape, F32)] * kept,
        [plane, mass],
        out_specs=[VMEM] * 3 + [HBM] * kept,
        scratch=[leaving(shape)] * kept,
        flops=500_000_000,
    )


def finish(pieces, totals_in, shape):
    return call(
        functools.partial(finish_kernel, middles=len(pieces) - 2),
        [(shape, F32)],
        [*pieces, *totals_in],
        out_specs=[HBM],
        scratch=[pltpu.VMEM(shape, F32), leaving(shape)],
        flops=500_000_000,
    )


def tables_of(count):
    return [
        ((count * BAND, TILE), BF16),
        ((count * BAND, TILE), BF16),
        ((count, 128, 384), BF16),
    ]


def body(counts, sample_weights, classes, class_radius):
    shape = rows, columns = counts.shape
    groups = ((0, 1), (2, 3))
    cuts = (rows - 192, 192)
    rim, slim = (REACH, columns), (PILOT_RADIUS, columns)
    counts, sample_weights, classes = (
        pltpu.with_memory_space_constraint(field, pltpu.HBM)
        for field in (counts, sample_weights, classes)
    )
    chunks = rows // CHUNK
    *pilot_tables, mass, mass_a, mass_b, label_a, label_b = call(
        prepare_kernel,
        tables_of(1)
        + [(shape, F32), (slim, F32), (slim, F32), (rim, jnp.int32), (rim, jnp.int32)],
        [counts, sample_weights, classes],
        ins=[HBM, HBM, HBM],
        scratch=[
            pltpu.VMEM(shape, jnp.int32),
            pltpu.VMEM(shape, F32),
            pltpu.VMEM((2, *rim), jnp.int32),
            pltpu.SemaphoreType.DMA((2, chunks)),
            pltpu.SemaphoreType.DMA((2,)),
        ],
        flops=500_000_000,
    )
    mass_halo = exchange(mass_a, mass_b, "row")
    label_halo = exchange(label_a, label_b, "row")
    *tables, labels = call(
        bands_kernel,
        tables_of(CLASSES) + [(shape, BF16)],
        [class_radius, classes],
        ins=[SMEM, HBM],
        scratch=[pltpu.VMEM(shape, jnp.int32), pltpu.SemaphoreType.DMA((chunks,))],
        flops=500_000_000,
    )
    pieces = smooth(mass, mass_halo, None, None, pilot_tables, ((0,),), (rows,))
    plane, stat = tally(pieces, [], mass)
    first_total = total_over(stat)
    adapted, *sends = adapt(plane, mass, False)
    halo = exchange(*sends, "row")
    pieces = smooth(adapted, halo, labels, label_halo, tables, groups, cuts)
    plane, stat = tally(pieces, [first_total, first_total], mass)
    second_total = total_over(stat)
    adapted, *sends, density_first = adapt(plane, mass, True)
    halo = exchange(*sends, "row")
    pieces = smooth(adapted, halo, labels, label_halo, tables, groups, cuts)
    (density_second,) = finish(pieces, [second_total, first_total], shape)
    return density_first, density_second


def solution(mesh):
    spec = P("row", "col")
    return jax.shard_map(
        body,
        mesh=mesh,
        in_specs=(spec, spec, spec, P()),
        out_specs=(spec, spec),
        check_vma=False,
    )
```

```python
import functools

import jax
import jax.numpy as jnp
from jax import lax
from jax.experimental import pallas as pl
from jax.experimental.pallas import tpu as pltpu
from jax.sharding import PartitionSpec as P


REACH = 64
PILOT_RADIUS = 32
CLASSES = 4
BACKGROUND = 0.5
TILE = 256
BAND = TILE + 2 * REACH
STEP = 64
F32 = jnp.float32
BF16 = jnp.bfloat16
MIB = 1 << 20
HBM = pl.BlockSpec(memory_space=pltpu.HBM)
VMEM = pl.BlockSpec(memory_space=pltpu.VMEM)
SMEM = pl.BlockSpec(memory_space=pltpu.SMEM)


def call(kernel, outs, args, ins=None, out_specs=None, scratch=(), limit=24, flops=0):
    return pl.pallas_call(
        kernel,
        out_shape=[jax.ShapeDtypeStruct(s, d) for s, d in outs],
        in_specs=ins or [VMEM] * len(args),
        out_specs=out_specs or [VMEM] * len(outs),
        scratch_shapes=scratch,
        compiler_params=pltpu.CompilerParams(vmem_limit_bytes=limit * MIB),
        cost_estimate=pl.CostEstimate(flops=flops, transcendentals=0, bytes_accessed=4 * MIB),
    )(*args)


def iota(shape, dim):
    return lax.broadcasted_iota(jnp.int32, shape, dim)


def split(value):
    high = value.astype(BF16)
    return high, (value - high.astype(F32)).astype(BF16)


def dot(a, b):
    return jnp.dot(a, b, preferred_element_type=F32)


def take(refs, *counts):
    groups = []
    for count in counts:
        groups.append(list(refs[:count]))
        refs = refs[count:]
    return *groups, list(refs)


def chosen(flag, when_set, when_clear):
    return jnp.where(flag > 0.5, when_set, when_clear)


def flags_of(axis):
    index = lax.axis_index(axis)
    last = lax.axis_size(axis) - 1
    values = (index & 1, jnp.minimum(index, 1), jnp.minimum(last - index, 1))
    return [jnp.full((1, 1), value.astype(F32), F32) for value in values]


def fill_bands(slot, radius, high_ref, low_ref, rim_ref):
    radius = jnp.full((1, 1), radius, F32)
    inverse = 1.0 / (2.0 * (0.5 * radius) * (0.5 * radius))

    def shape_of(d):
        return jnp.where(jnp.abs(d) <= radius, jnp.exp(-(d * d) * inverse), 0.0)

    lane = iota((8, 128), 1).astype(F32)
    tap = jnp.where(iota((8, 128), 0) == 0, jnp.where(lane == 0, 1.0, 2.0), 0.0)
    total = jnp.sum(shape_of(lane) * tap, axis=(0, 1), keepdims=True)
    column = iota((128, 128), 1)
    shift = iota((128, 128), 0) - column
    near = split(shape_of((shift - REACH).astype(F32)) / total)
    far = split(shape_of((shift + REACH).astype(F32)) / total)
    zero = jnp.zeros((128, 128), BF16)
    side = column[:REACH] < REACH
    zeros = jnp.zeros((REACH, 128), F32)
    base = slot * BAND
    for part, ref in enumerate((high_ref, low_ref)):
        blocks = ((near[part], zero), (far[part], near[part]), (zero, far[part]))
        for i, pair in enumerate(blocks):
            for k, block in enumerate(pair):
                lanes = slice(k * 128, (k + 1) * 128)
                ref[base + i * 128 : base + (i + 1) * 128, lanes] = block
        first = jnp.where(side, far[part][:REACH].astype(F32), zeros).astype(BF16)
        second = jnp.where(side, zeros, near[part][REACH:].astype(F32)).astype(BF16)
        for place in (0, 128) if part == 0 else (256,):
            rim_ref[slot, :REACH, place : place + 128] = first
            rim_ref[slot, REACH:, place : place + 128] = second


CHUNK = 128


def prepare_kernel(*refs):
    (counts_in, weights_in, classes_in), tables, outs, scratch = take(refs, 3, 3, 5)
    mass_ref, mass_a, mass_b, label_a, label_b = outs
    counts, weights, ends, arrived, ended = scratch
    rows = counts.shape[0]
    copies = []
    for n, start in enumerate(range(0, rows, CHUNK)):
        at = slice(start, start + CHUNK)
        pair = [
            pltpu.make_async_copy(counts_in.at[at], counts.at[at], arrived.at[0, n]),
            pltpu.make_async_copy(weights_in.at[at], weights.at[at], arrived.at[1, n]),
        ]
        for copy in pair:
            copy.start()
        copies.append((at, pair))
    end_copies = [
        pltpu.make_async_copy(classes_in.at[0:REACH], ends.at[0], ended.at[0]),
        pltpu.make_async_copy(classes_in.at[rows - REACH : rows], ends.at[1], ended.at[1]),
    ]
    for copy in end_copies:
        copy.start()
    fill_bands(0, F32(PILOT_RADIUS), *tables)
    for at, pair in copies:
        for copy in pair:
            copy.wait()
        mass_ref[at] = counts[at].astype(F32) * weights[at]
    odd = flags_of("row")[0]
    top, bottom = mass_ref[0:PILOT_RADIUS], mass_ref[rows - PILOT_RADIUS :]
    mass_a[...] = chosen(odd, top, bottom)
    mass_b[...] = chosen(odd, bottom, top)
    for copy in end_copies:
        copy.wait()
    label_a[...] = chosen(odd, ends[0], ends[1])
    label_b[...] = chosen(odd, ends[1], ends[0])


def bands_kernel(*refs):
    (radius_ref, classes_in), tables, (label_ref, classes, arrived) = take(refs, 2, 3)
    rows = classes.shape[0]
    copies = []
    for n, start in enumerate(range(0, rows, CHUNK)):
        at = slice(start, start + CHUNK)
        copy = pltpu.make_async_copy(classes_in.at[at], classes.at[at], arrived.at[n])
        copy.start()
        copies.append((at, copy))
    for c in range(CLASSES):
        fill_bands(c, radius_ref[c].astype(F32), *tables)
    for at, copy in copies:
        copy.wait()
        label_ref[at] = classes[at].astype(F32).astype(BF16)


def masked(pieces, labels, c):
    if labels is None:
        return pieces
    keep = labels == c
    return [jnp.where(keep, piece, jnp.zeros_like(piece)) for piece in pieces]


def rows_kernel(*refs, bands, labelled):
    (field_ref,), label_refs, (band_high, band_low, high_ref, low_ref, edge_ref) = take(
        refs, 1, labelled
    )
    rows, columns = field_ref.shape
    count = rows // REACH
    for n in range(columns // TILE):
        at = slice(n * TILE, (n + 1) * TILE)
        pieces = split(field_ref[:, at])
        labels = label_refs[0][:, at] if labelled else None
        for slot, c in enumerate(bands):
            high, low = masked(pieces, labels, c)
            sums = [None] * count

            def add(result, first):
                for i in range(result.shape[0] // REACH):
                    piece = result[i * REACH : (i + 1) * REACH]
                    own = sums[first + i]
                    sums[first + i] = piece if own is None else own + piece

            half = band_high[c * BAND : c * BAND + 2 * 128, 0:128]
            twice = jnp.concatenate([half, half], axis=1)
            for block in range(rows // 128):
                own = slice(block * 128, (block + 1) * 128)
                first = max(2 * block - 1, 0)
                last = min(2 * block + 3, count)
                taps = slice((first - 2 * block + 1) * REACH, (last - 2 * block + 1) * REACH)
                add(dot(twice[taps], jnp.concatenate([high[own], low[own]])), first)
            for tile in range(rows // TILE):
                own = slice(tile * TILE, (tile + 1) * TILE)
                first = max(4 * tile - 1, 0)
                last = min(4 * tile + 5, count)
                start = c * BAND + (first - 4 * tile + 1) * REACH
                taps = slice(start, start + (last - first) * REACH)
                add(dot(band_low[taps, :], high[own]), first)
            edge_ref[slot, 0:REACH, at] = sums[0]
            edge_ref[slot, REACH:, at] = sums[-1]
            for i, value in enumerate(sums[1:-1]):
                target = slice(i * REACH, (i + 1) * REACH)
                high_ref[slot, target, at], low_ref[slot, target, at] = split(value)


def kept_row(start, rows):
    if start < REACH:
        return rows - 2 * REACH + start
    return start if start >= rows - REACH else start - REACH


def stacked_left(sides, inputs, start, stop, inner):
    refs, edge_ref = sides
    pieces = []
    slot = 0
    for ref in refs:
        for own in range(ref.shape[0]):
            rows = []
            if start < inner:
                rows.append(ref[own, start : min(stop, inner), inputs])
            if stop > inner:
                rows.append(edge_ref[slot, max(start, inner) - inner : stop - inner, inputs])
            pieces.append(rows[0] if len(rows) == 1 else jnp.concatenate(rows))
            slot += 1
    return jnp.concatenate(pieces, axis=1)


def swept(highs, lows, bands, band_refs, block, width, columns, start, stop, inner):
    high_ref, low_ref = band_refs

    def window(first, last):
        here, there = max(first, 0), min(last, columns)
        return slice(here, there), slice(here - first, there - first)

    def rights(refs_and_lanes, taps):
        return jnp.concatenate(
            [
                jnp.concatenate(
                    [ref[c * BAND + taps.start : c * BAND + taps.stop, lanes] for ref, lanes in refs_and_lanes],
                    axis=1,
                )
                for c in bands
            ]
        )

    results = []
    origin = block * TILE - 128
    for part in range(width // 128):
        inputs, taps = window(origin + part * 128, origin + (part + 2) * 128)
        left = stacked_left(highs, inputs, start, stop, inner)
        right = rights(((high_ref, slice(0, 128)), (low_ref, slice(0, 128))), taps)
        both = dot(left, right)
        results.append(both[:, :128] + both[:, 128:])
    inputs, taps = window(origin, origin + width + 128)
    left = stacked_left(lows, inputs, start, stop, inner)
    rest = dot(left, rights(((high_ref, slice(0, width)),), taps))
    return [value + rest[:, k * 128 : (k + 1) * 128] for k, value in enumerate(results)]


def edges_kernel(*refs, groups, labelled):
    count = len(groups)
    halo, labels_in, partials, highs, lows, (rim_ref, *band_refs), outs = take(
        refs, 2, 2 * labelled, count, count, count, 3
    )
    edge_high, edge_low, left_ref, right_ref, send_a, send_b = outs
    bands = [c for group in groups for c in group]
    sources = [(ref, own) for ref in partials for own in range(ref.shape[0])]
    columns = halo[0].shape[1]
    odd_row, has_top, has_bottom = flags_of("row")
    odd_column = flags_of("col")[0]
    for n in range(columns // TILE):
        at = slice(n * TILE, (n + 1) * TILE)

        def joined(pair):
            first, second = pair[0][:, at].astype(F32), pair[1][:, at].astype(F32)
            top = chosen(has_top, chosen(odd_row, first, second), 0.0)
            bottom = chosen(has_bottom, chosen(odd_row, second, first), 0.0)
            missing = REACH - first.shape[0]
            if missing:
                zeros = jnp.zeros((missing, TILE), F32)
                return jnp.concatenate([zeros, top, bottom, zeros])
            return jnp.concatenate([top, bottom])

        pieces = split(joined(halo))
        labels = joined(labels_in).astype(BF16) if labelled else None
        for slot, c in enumerate(bands):
            high, low = masked(pieces, labels, c)
            right = jnp.concatenate([high, low, high], axis=0)
            source, own = sources[slot]
            value = source[own, :, at] + dot(rim_ref[c], right)
            edge_high[slot, :, at], edge_low[slot, :, at] = split(value)
    rows = left_ref.shape[0]
    inner = rows - 2 * REACH
    for target, block in ((left_ref, 0), (right_ref, columns // TILE)):
        results = swept(
            (highs, edge_high),
            (lows, edge_low),
            bands,
            band_refs,
            block,
            target.shape[1],
            columns,
            0,
            rows,
            inner,
        )
        for k, value in enumerate(results):
            target[:, k * 128 : (k + 1) * 128] = value
    half = rows // 2
    lower = iota((half, 128), 1) < REACH
    left = left_ref[:, 0:128]
    left = jnp.where(lower, left[:half], pltpu.roll(left[half:], REACH, 1))
    right = right_ref[...]
    right = jnp.where(lower, pltpu.roll(right[:half], REACH, 1), right[half:])
    send_a[...] = chosen(odd_column, left, right)
    send_b[...] = chosen(odd_column, right, left)


def middle_kernel(*refs, groups, start, kept):
    count = len(groups)
    highs, lows, (edge_high, edge_low), band_refs, (left_ref, right_ref), refs = take(
        refs, count, count, 2, 2, 2
    )
    plane, (out_ref,), plane_out, done = take(refs, kept, 1, kept)
    copies = []
    for source, target, arrived in zip(plane, plane_out, done):
        for number, first in enumerate(range(0, source.shape[0], STEP)):
            part = slice(first, first + STEP)
            copies.append(
                pltpu.make_async_copy(source.at[part], target.at[part], arrived.at[number])
            )
    for copy in copies:
        copy.start()
    bands = [c for group in groups for c in group]
    inner = highs[0].shape[1]
    rows, columns = out_ref.shape
    at = slice(start, start + rows)
    lower = iota((rows, 128), 1) < REACH

    def blocks():
        for k in range(0, TILE, 128):
            yield left_ref[at, k : k + 128]
        for j in range(1, columns // TILE):
            yield from swept(
                (highs, edge_high),
                (lows, edge_low),
                bands,
                band_refs,
                j,
                TILE,
                columns,
                start,
                start + rows,
                inner,
            )
        yield right_ref[at, :]

    before = None
    for k, block in enumerate(blocks()):
        turned = pltpu.roll(block, REACH, 1)
        if before is not None:
            out_ref[:, (k - 1) * 128 : k * 128] = jnp.where(lower, before, turned)
        before = turned
    for copy in copies:
        copy.wait()


def gathered(middles, come, flags, start):
    odd, has_left, has_right = flags
    rows = sum(ref.shape[0] for ref in middles)
    columns = middles[0].shape[1]
    half = rows // 2
    kept = kept_row(start, rows)
    lane = iota((STEP, 128), 1)
    local = slice(kept % half, kept % half + STEP)
    come_left = chosen(has_left, chosen(odd, come[0][local], come[1][local]), 0.0)
    come_right = chosen(has_right, chosen(odd, come[1][local], come[0][local]), 0.0)
    if kept < half:
        come_right = pltpu.roll(come_right, REACH, 1)
    else:
        come_left = pltpu.roll(come_left, REACH, 1)
    own = kept
    for middle_ref in middles:
        if own < middle_ref.shape[0]:
            break
        own -= middle_ref.shape[0]
    for k in range(0, columns, 128):
        block = middle_ref[own : own + STEP, k : k + 128]
        if k == 0:
            block = block + jnp.where(lane < REACH, come_left, 0.0)
        if k == columns - 128:
            block = block + jnp.where(lane >= REACH, come_right, 0.0)
        yield block


def tally_kernel(*refs, middles, scaled, totals):
    middle_refs, come, totals_in, (mass_ref, plane_ref, stat_ref) = take(
        refs, middles, 2, 2 * scaled
    )
    rows, columns = plane_ref.shape
    flags = flags_of("col")
    if scaled:
        inverse = jnp.exp(-(totals_in[0][0:1, :] / totals_in[1][1:2, :]))
    log_sums = [jnp.zeros((8, 128), F32)] * (columns // 128)
    mass_sums = [jnp.zeros((8, 128), F32)] * (columns // 128)
    for start in range(0, rows, STEP):
        at = slice(start, start + STEP)
        for k, block in enumerate(gathered(middle_refs, come, flags, start)):
            lanes = slice(k * 128, (k + 1) * 128)
            if scaled:
                block = block * inverse
            plane_ref[at, lanes] = block
            mass = mass_ref[at, lanes]
            terms = mass * jnp.log(block + BACKGROUND)
            log_sums[k] += jnp.sum(terms.reshape(STEP // 8, 8, 128), axis=0)
            if totals:
                mass_sums[k] += jnp.sum(mass.reshape(STEP // 8, 8, 128), axis=0)
    log_sum = jnp.sum(sum(log_sums), axis=(0, 1), keepdims=True)
    mass_sum = jnp.sum(sum(mass_sums), axis=(0, 1), keepdims=True)
    row = iota((8, 128), 0)
    stat_ref[...] = jnp.where(row == 0, log_sum, jnp.where(row == 1, mass_sum, 0.0))


def adapt_kernel(*refs, kept):
    (plane_ref, mass_ref, adapted_ref, send_a, send_b), density_out, done = take(refs, 5, kept)
    rows = plane_ref.shape[0]
    copies = []
    if kept:
        for number, start in enumerate(range(0, rows, STEP)):
            at = slice(start, start + STEP)
            copies.append(
                pltpu.make_async_copy(
                    plane_ref.at[at], density_out[0].at[at], done[0].at[number]
                )
            )
    for copy in copies:
        copy.start()
    for start in range(0, rows, STEP):
        at = slice(start, start + STEP)
        adapted_ref[at] = mass_ref[at] * (plane_ref[at] + BACKGROUND)
    odd = flags_of("row")[0]
    top, bottom = adapted_ref[0:REACH], adapted_ref[rows - REACH :]
    send_a[...] = chosen(odd, top, bottom)
    send_b[...] = chosen(odd, bottom, top)
    for copy in copies:
        copy.wait()


def finish_kernel(*refs, middles):
    middle_refs, come, totals_in, (density_ref, staged, done) = take(refs, middles, 2, 2)
    rows, _ = staged.shape
    flags = flags_of("col")
    inverse = jnp.exp(-(totals_in[0][0:1, :] / totals_in[1][1:2, :]))
    copies = []
    for number, start in enumerate(range(0, rows, STEP)):
        at = slice(start, start + STEP)
        for k, block in enumerate(gathered(middle_refs, come, flags, start)):
            staged[at, k * 128 : (k + 1) * 128] = block * inverse
        copy = pltpu.make_async_copy(staged.at[at], density_ref.at[at], done.at[number])
        copy.start()
        copies.append(copy)
    for copy in copies:
        copy.wait()


def exchange(first, second, axis):
    along = 0 if axis == "row" else 1
    sizes = [lax.axis_size("row"), lax.axis_size("col")]
    results = []
    for offset, value in ((0, first), (1, second)):
        pairs = []
        for index in range(sizes[0] * sizes[1]):
            place = [index // sizes[1], index % sizes[1]]
            own = place[along]
            partner = own + 1 if own % 2 == offset else own - 1
            if 0 <= partner < sizes[along]:
                place[along] = partner
            else:
                place[1 - along] ^= 1
            pairs.append((index, place[0] * sizes[1] + place[1]))
        results.append(lax.ppermute(value, ("row", "col"), pairs))
    return results


HOPS = (
    (0, 7, (1, 8)),
    (0, 3, (1, 8)),
    (12, 1, (16, 1)),
    (4, 1, (16, 1)),
    (0, 1, (1, 2)),
    (3, 1, (4, 1)),
    (1, 1, (2, 1)),
)


def total_over(stat):
    sizes = (lax.axis_size("row"), lax.axis_size("col"))
    for rows, columns, least in HOPS:
        if sizes[0] >= least[0] and sizes[1] >= least[1]:
            pairs = []
            for index in range(sizes[0] * sizes[1]):
                row, column = divmod(index, sizes[1])
                pairs.append((index, (row ^ rows) * sizes[1] + (column ^ columns)))
            stat = stat + lax.ppermute(stat, ("row", "col"), pairs)
    return stat


def smooth(field, halo, labels, label_halo, tables, groups, cuts, plane=None):
    high, low, rim = tables
    rows, columns = field.shape
    labelled = labels is not None
    bands = [c for group in groups for c in group]
    highs, lows, partials = [], [], []
    for group in groups:
        inner = (len(group), rows - 2 * REACH, columns)
        edge = (len(group), 2 * REACH, columns)
        results = call(
            functools.partial(rows_kernel, bands=group, labelled=labelled),
            [(inner, BF16), (inner, BF16), (edge, F32)],
            [field] + ([labels] if labelled else []) + [high, low],
            flops=len(group) * 1_000_000_000,
        )
        for results_of, result in zip((highs, lows, partials), results):
            results_of.append(result)
    edge = (len(bands), 2 * REACH, columns)
    edge_high, edge_low, left, right, send_a, send_b = call(
        functools.partial(edges_kernel, groups=groups, labelled=labelled),
        [(edge, BF16), (edge, BF16), ((rows, TILE), F32), ((rows, 128), F32)]
        + [((rows // 2, 128), F32)] * 2,
        [*halo, *(label_halo if labelled else ()), *partials, *highs, *lows]
        + [rim, high, low],
        flops=len(bands) * 500_000_000,
    )
    come = exchange(send_a, send_b, "col")
    middles = []
    start = 0
    for number, count in enumerate(cuts):
        kept = int(plane is not None and number == len(cuts) - 1)
        middle, *gone = call(
            functools.partial(middle_kernel, groups=groups, start=start, kept=kept),
            [((count, columns), F32)] + [(field.shape, F32)] * kept,
            [*highs, *lows, edge_high, edge_low, high, low, left, right] + [plane] * kept,
            out_specs=[VMEM] + [HBM] * kept,
            scratch=[leaving(field.shape)] * kept,
            flops=len(bands) * 750_000_000 * count // rows,
        )
        middles.append(middle)
        start += count
    pieces = [*middles, *come]
    return pieces if plane is None else (pieces, *gone)


def leaving(shape):
    return pltpu.SemaphoreType.DMA((shape[0] // STEP,))


def tally(pieces, totals_in, mass):
    shape = mass.shape
    return call(
        functools.partial(
            tally_kernel,
            middles=len(pieces) - 2,
            scaled=bool(totals_in),
            totals=not totals_in,
        ),
        [(shape, F32), ((8, 128), F32)],
        [*pieces, *totals_in, mass],
        flops=500_000_000,
    )


def adapt(plane, mass, kept):
    shape = mass.shape
    rim = (REACH, shape[1])
    return call(
        functools.partial(adapt_kernel, kept=kept),
        [(shape, F32), (rim, F32), (rim, F32)] + [(shape, F32)] * kept,
        [plane, mass],
        out_specs=[VMEM] * 3 + [HBM] * kept,
        scratch=[leaving(shape)] * kept,
        flops=500_000_000,
    )


def finish(pieces, totals_in, shape):
    return call(
        functools.partial(finish_kernel, middles=len(pieces) - 2),
        [(shape, F32)],
        [*pieces, *totals_in],
        out_specs=[HBM],
        scratch=[pltpu.VMEM(shape, F32), leaving(shape)],
        flops=500_000_000,
    )


def tables_of(count):
    return [
        ((count * BAND, TILE), BF16),
        ((count * BAND, TILE), BF16),
        ((count, 128, 384), BF16),
    ]


def body(counts, sample_weights, classes, class_radius):
    shape = rows, columns = counts.shape
    groups = ((0, 1), (2, 3))
    cuts = (rows - 192, 192)
    rim, slim = (REACH, columns), (PILOT_RADIUS, columns)
    counts, sample_weights, classes = (
        pltpu.with_memory_space_constraint(field, pltpu.HBM)
        for field in (counts, sample_weights, classes)
    )
    chunks = rows // CHUNK
    *pilot_tables, mass, mass_a, mass_b, label_a, label_b = call(
        prepare_kernel,
        tables_of(1)
        + [(shape, F32), (slim, F32), (slim, F32), (rim, jnp.int32), (rim, jnp.int32)],
        [counts, sample_weights, classes],
        ins=[HBM, HBM, HBM],
        scratch=[
            pltpu.VMEM(shape, jnp.int32),
            pltpu.VMEM(shape, F32),
            pltpu.VMEM((2, *rim), jnp.int32),
            pltpu.SemaphoreType.DMA((2, chunks)),
            pltpu.SemaphoreType.DMA((2,)),
        ],
        flops=500_000_000,
    )
    mass_halo = exchange(mass_a, mass_b, "row")
    label_halo = exchange(label_a, label_b, "row")
    *tables, labels = call(
        bands_kernel,
        tables_of(CLASSES) + [(shape, BF16)],
        [class_radius, classes],
        ins=[SMEM, HBM],
        scratch=[pltpu.VMEM(shape, jnp.int32), pltpu.SemaphoreType.DMA((chunks,))],
        flops=500_000_000,
    )
    pieces = smooth(mass, mass_halo, None, None, pilot_tables, ((0,),), (rows,))
    plane, stat = tally(pieces, [], mass)
    first_total = total_over(stat)
    adapted, *sends = adapt(plane, mass, False)
    halo = exchange(*sends, "row")
    pieces = smooth(adapted, halo, labels, label_halo, tables, groups, cuts)
    plane, stat = tally(pieces, [first_total, first_total], mass)
    second_total = total_over(stat)
    adapted, *sends = adapt(plane, mass, False)
    halo = exchange(*sends, "row")
    pieces, density_first = smooth(adapted, halo, labels, label_halo, tables, groups, cuts, plane)
    (density_second,) = finish(pieces, [second_total, first_total], shape)
    return density_first, density_second


def solution(mesh):
    spec = P("row", "col")
    return jax.shard_map(
        body,
        mesh=mesh,
        in_specs=(spec, spec, spec, P()),
        out_specs=(spec, spec),
        check_vma=False,
    )
```
